8 devices in a mesh: tp: 2 (over z, y), dp: 4 (over x, core).
Axes of the slice: x: 2, y: 2, z: 1, core: 2. Of those that a mesh axis runs over, the one named last changes fastest.
Arguments:
- x: bfloat16 [8192, 5120], P(('dp', 'tp'))
- w_gate: bfloat16 [5120, 14336], P('dp', 'tp')
- w_up: bfloat16 [5120, 14336], P('dp', 'tp')
- w_down: bfloat16 [14336, 5120], P('tp', 'dp')
Outputs:
- output: bfloat16 [8192, 5120], P(('dp', 'tp'))
All inputs are finite; a program needn't handle non-finite values.
Results may differ from the reference program's by a relative error of at most 0.0130042.
Values are sent between devices in bfloat16 or wider.
A program may use at most 1 GiB of HBM per device.

```python
import jax
import jax.numpy as jnp
from jax import lax

D = 5120
FF = 14336
TOKENS_DEV = 1024
ROWS = 8192

NBLK = ROWS // TOKENS_DEV


def setup_inputs(seed: int = 0) -> dict:
    k = jax.random.split(jax.random.key(seed), 4)
    x = jax.random.normal(k[0], (ROWS, D), jnp.float32)
    wg = jax.random.normal(k[1], (D, FF), jnp.float32) * D ** -0.5
    wu = jax.random.normal(k[2], (D, FF), jnp.float32) * D ** -0.5
    wd = jax.random.normal(k[3], (FF, D), jnp.float32) * FF ** -0.5
    return {"x": x.astype(jnp.bfloat16), "w_gate": wg.astype(jnp.bfloat16), "w_up": wu.astype(jnp.bfloat16), "w_down": wd.astype(jnp.bfloat16)}


def reference(x, w_gate, w_up, w_down):
    def blk(xb):
        a = jnp.dot(xb, w_gate, preferred_element_type=jnp.float32)
        b = jnp.dot(xb, w_up, preferred_element_type=jnp.float32)
        h = (jax.nn.silu(a) * b).astype(jnp.bfloat16)
        o = jnp.dot(h, w_down, preferred_element_type=jnp.float32)
        return (xb.astype(jnp.float32) + o).astype(jnp.bfloat16)
    y = lax.map(blk, x.reshape(NBLK, TOKENS_DEV, D))
    return y.reshape(ROWS, D)
```

```python
import jax
import jax.numpy as jnp
from jax import lax
from jax.sharding import PartitionSpec as P

COLS = 1792
STRIP = 256


def solution(mesh):
    nt = mesh.shape["tp"]
    nd = mesh.shape["dp"]
    swap = [(i, (i + 1) % nt) for i in range(nt)]

    def body(x, wg, wu, wd):
        r, d = x.shape
        f = wg.shape[1]
        dc = wd.shape[1]
        xc = jnp.concatenate([x, lax.ppermute(x, "tp", swap)], axis=0)
        hs = []
        for s in range(0, f, COLS):
            g = lax.all_gather(wg[:, s:s + COLS], "dp", axis=0, tiled=True)
            u = lax.all_gather(wu[:, s:s + COLS], "dp", axis=0, tiled=True)
            a = jnp.dot(xc, g, preferred_element_type=jnp.float32)
            b = jnp.dot(xc, u, preferred_element_type=jnp.float32)
            hs.append((jax.nn.silu(a) * b).astype(jnp.bfloat16))
        h = jnp.concatenate(hs, axis=1)
        outs = []
        for s in range(0, dc, STRIP):
            w = lax.all_gather(wd[:, s:s + STRIP], "dp", axis=0, tiled=False)
            p = [jnp.dot(h, w[i], preferred_element_type=jnp.float32).astype(jnp.bfloat16) for i in range(nd)]
            mine = jnp.stack([q[:r] for q in p])
            theirs = lax.ppermute(jnp.stack([q[r:] for q in p]), "tp", swap)
            outs.append(mine.astype(jnp.float32) + theirs.astype(jnp.float32))
        o = jnp.stack(outs)
        o = o.transpose(2, 1, 0, 3).reshape(r, d)
        return (x.astype(jnp.float32) + o).astype(jnp.bfloat16)

    return jax.shard_map(body, mesh=mesh, in_specs=(P(("dp", "tp"), None), P("dp", "tp"), P("dp", "tp"), P("tp", "dp")), out_specs=P(("dp", "tp"), None), check_vma=False)
```

```python
import functools

import jax
import jax.numpy as jnp
from jax import lax
from jax.experimental import pallas as pl
from jax.experimental.pallas import tpu as pltpu
from jax.sharding import PartitionSpec as P

CW = 256


def kernel(x, wg, wu, wd, y, w1, w2, w3, db, hb, po, rdi, r1i, yxi,
           xb, wv, hst, s_loc, s_xs, s_ws, s_xx, s_xy, s_xd, s_w1, s_w2, s_w3, s_d1, s_d2, s_d3,
           s_wv, s_h, s_po, s_rs, s_rd, s_r1, s_yx, s_ys, s_ld, s_out):
    rows, dim = x.shape
    dk = dim // 4
    fq = wg.shape[1] // 2
    nch = fq // CW
    first = nch // 2
    ns = dk // CW
    f32, bf16 = jnp.float32, jnp.bfloat16

    t = lax.axis_index("tp")
    d = lax.axis_index("dp")
    side = d // 2
    core = d % 2
    mate = d + 1 - 2 * core
    quarter = [d, mate, (d + 2) % 4, (mate + 2) % 4]
    to_mate = {"dp": mate}
    to_x = {"dp": (d + 2) % 4}
    to_y = {"tp": 1 - t}

    def col(v, size=128):
        return pl.multiple_of(v, size)

    def send(src, dst, send_sem, recv_sem, where):
        pltpu.make_async_remote_copy(
            src_ref=src, dst_ref=dst, send_sem=send_sem, recv_sem=recv_sem,
            device_id=where, device_id_type=pl.DeviceIdType.MESH).start()

    def wait(ref, sem):
        pltpu.make_async_copy(ref, ref, sem).wait()

    def block(b):
        return pl.ds(b * rows, rows)

    def slot(s):
        return pl.ds(s * dk, dk)

    barrier = pltpu.get_barrier_semaphore()
    for where in (to_mate, to_x, to_y):
        pl.semaphore_signal(barrier, inc=1, device_id=where, device_id_type=pl.DeviceIdType.MESH)
    pl.semaphore_wait(barrier, 3)

    for s in range(4):
        src = x.at[:, pl.ds(col(quarter[s] * dk), dk)]
        send(src, xb.at[block(2), slot(s ^ 2)], s_xs.at[0], s_xx.at[s ^ 2], to_x)
        send(src, xb.at[block(1), slot(s)], s_xs.at[1], s_xy.at[s], to_y)
    for s in range(4):
        src = x.at[:, pl.ds(col(quarter[s] * dk), dk)]
        pltpu.make_async_copy(src, xb.at[block(0), slot(s)], s_loc).start()

    def send_chunk(j, _):
        for m, w in enumerate((wg, wu)):
            away = w.at[:, pl.ds(col((1 - side) * fq + j * CW), CW)]
            here = w.at[:, pl.ds(col(side * fq + j * CW), CW)]
            send(away, w2.at[j, :, pl.ds(m * CW, CW)], s_ws.at[1], s_w2.at[j], to_x)
            send(here, w1.at[j, :, pl.ds(m * CW, CW)], s_ws.at[0], s_w1.at[j], to_mate)
        return 0

    lax.fori_loop(0, nch, send_chunk, 0)

    def send_strip(k, _):
        cols = pl.ds(col(k * CW), CW)
        send(wd.at[pl.ds(col((1 - side) * fq), fq), cols], db.at[1, k], s_ws.at[3], s_d2.at[k], to_x)
        send(wd.at[pl.ds(col(side * fq), fq), cols], db.at[0, k], s_ws.at[2], s_d1.at[k], to_mate)
        return 0

    lax.fori_loop(0, ns, send_strip, 0)

    for s in (2, 3, 0, 1):
        piece = xb.at[block(2), slot(s)]
        wait(piece, s_xx.at[s])
        send(piece, xb.at[block(3), slot(s)], s_xs.at[2], s_xd.at[s], to_y)

    def forward_chunk(j):
        wait(w2.at[j], s_w2.at[j])
        send(w2.at[j], w3.at[j], s_ws.at[4], s_w3.at[j], to_mate)

    def load_chunk(j, p):
        for m, w in enumerate((wg, wu)):
            here = w.at[:, pl.ds(col(side * fq + j * CW), CW)]
            pltpu.make_async_copy(here, wv.at[p, slot(0), pl.ds(m * CW, CW)], s_wv.at[p]).start()
        for s, w in ((1, w1), (2, w2), (3, w3)):
            pltpu.make_async_copy(w.at[j], wv.at[p, slot(s)], s_wv.at[p]).start()

    def arrive_chunk(j):
        wait(w1.at[j], s_w1.at[j])
        wait(w3.at[j], s_w3.at[j])

    def hcopy(b, j, q):
        return pltpu.make_async_copy(
            hst.at[q], hb.at[block(b), pl.ds(col(j * CW), CW)], s_h.at[q])

    def gate(b, j, p, q, used=True):
        ab = jnp.dot(xb[block(b), :], wv[p], preferred_element_type=f32)
        a = ab[:, :CW]
        h = (a * jax.nn.sigmoid(a) * ab[:, CW:]).astype(bf16)

        @pl.when(used)
        def _():
            hcopy(b, j, q).wait()

        hst[q] = h
        hcopy(b, j, q).start()

    forward_chunk(0)
    arrive_chunk(0)
    load_chunk(0, 0)
    wait(xb.at[block(0), :], s_loc)
    for s in range(4):
        wait(xb.at[block(1), slot(s)], s_xy.at[s])

    def pass_one(j, _):
        p = j % 2
        wait(wv.at[p], s_wv.at[p])
        gate(0, j, p, 0, j > 0)
        gate(1, j, p, 1, j > 0)

        @pl.when(j + 1 < first)
        def _():
            forward_chunk(j + 1)

        gate(2, j, p, 0)

        @pl.when(j + 1 < first)
        def _():
            arrive_chunk(j + 1)
            load_chunk(j + 1, 1 - p)

        return 0

    lax.fori_loop(0, first, pass_one, 0)

    load_chunk(0, 0)
    for s in range(4):
        wait(xb.at[block(3), slot(s)], s_xd.at[s])

    def pass_diag(j, _):
        p = j % 2

        @pl.when(j + 1 < first)
        def _():
            load_chunk(j + 1, 1 - p)

        wait(wv.at[p], s_wv.at[p])
        gate(3, j, p, 1)
        return 0

    lax.fori_loop(0, first, pass_diag, 0)

    forward_chunk(first)
    arrive_chunk(first)
    load_chunk(first, first % 2)

    def pass_two(j, _):
        p = j % 2
        wait(wv.at[p], s_wv.at[p])
        gate(3, j, p, 0)
        gate(1, j, p, 1)

        @pl.when(j + 1 < nch)
        def _():
            forward_chunk(j + 1)

        gate(2, j, p, 0)

        @pl.when(j + 1 < nch)
        def _():
            arrive_chunk(j + 1)
            load_chunk(j + 1, 1 - p)

        gate(0, j, p, 1)
        return 0

    lax.fori_loop(first, nch, pass_two, 0)
    for q in range(2):
        hcopy(0, 0, q).wait()

    wait(xb.at[block(2), :], s_xs.at[2])
    hcols = pl.ds(0, fq)
    for b in (3, 1, 2, 0):
        pltpu.make_async_copy(hb.at[block(b), :], xb.at[block(b), hcols], s_ld.at[b]).start()

    def tile(b, c):
        return xb.at[block(b), pl.ds(col(fq + c * CW), CW)]

    def strip_slot(i):
        late = i - 2 * ns
        return (jnp.where(i < 2 * ns, i // ns, 2 + late % 2),
                jnp.where(i < 2 * ns, i % ns, late // 2))

    def load_strip(i, p):
        dst = wv.at[p, pl.ds(0, fq), pl.ds(0, CW)]
        late = i - 2 * ns

        @pl.when(i < ns)
        def _():
            src = wd.at[pl.ds(col(side * fq), fq), pl.ds(col(i * CW), CW)]
            pltpu.make_async_copy(src, dst, s_wv.at[p]).start()

        @pl.when((i >= ns) & (i < 2 * ns))
        def _():
            k = i - ns
            wait(db.at[0, k], s_d1.at[k])
            pltpu.make_async_copy(db.at[0, k], dst, s_wv.at[p]).start()

        @pl.when((i >= 2 * ns) & (late % 2 == 0))
        def _():
            k = late // 2
            wait(db.at[1, k], s_d2.at[k])
            send(db.at[1, k], db.at[2, k], s_ws.at[5], s_d3.at[k], to_mate)
            pltpu.make_async_copy(db.at[1, k], dst, s_wv.at[p]).start()

        @pl.when((i >= 2 * ns) & (late % 2 == 1))
        def _():
            k = late // 2
            wait(db.at[2, k], s_d3.at[k])
            pltpu.make_async_copy(db.at[2, k], dst, s_wv.at[p]).start()

    def put(b, i, p):
        return pltpu.make_async_copy(tile(b, p), po.at[b, i], s_po.at[b])

    def down(b, i, p):
        strip = wv[p, pl.ds(0, fq), pl.ds(0, CW)]
        o = jnp.dot(xb[block(b), hcols], strip, preferred_element_type=f32)
        xb[block(b), pl.ds(col(fq + p * CW), CW)] = o.astype(bf16)
        put(b, i, p).start()

    load_strip(0, 0)
    for b in (3, 1, 2, 0):
        wait(xb.at[block(b), hcols], s_ld.at[b])

    def partial(i, _):
        p = i % 2
        wait(wv.at[p, pl.ds(0, fq), pl.ds(0, CW)], s_wv.at[p])
        down(3, i, p)
        down(1, i, p)
        put(3, i, p).wait()
        send(po.at[3, i], rdi.at[i], s_rs.at[0], s_rd.at[i], to_y)

        @pl.when(i + 1 < 4 * ns)
        def _():
            load_strip(i + 1, 1 - p)

        down(2, i, p)
        put(1, i, p).wait()
        send(po.at[1, i], r1i.at[i], s_rs.at[1], s_r1.at[i], to_y)
        down(0, i, p)
        put(2, i, p).wait()
        put(0, i, p).wait()
        return 0

    lax.fori_loop(0, 4 * ns, partial, 0)

    def relay(i):
        q = i % 2
        pltpu.make_async_copy(po.at[2, i], tile(0, 0), s_ld.at[0]).start()
        wait(rdi.at[i], s_rd.at[i])
        pltpu.make_async_copy(rdi.at[i], tile(0, 1), s_ld.at[1]).start()
        wait(tile(0, 0), s_ld.at[0])
        wait(tile(0, 1), s_ld.at[1])

        @pl.when(i >= 2)
        def _():
            wait(tile(1, q), s_ys.at[q])

        o = xb[block(0), pl.ds(fq, CW)].astype(f32) + xb[block(0), pl.ds(fq + CW, CW)].astype(f32)
        xb[block(1), pl.ds(col(fq + q * CW), CW)] = o.astype(bf16)
        s, k = strip_slot(i)
        there = jnp.where(s < 2, 2 * ns + 2 * k + s, (s - 2) * ns + k)
        send(tile(1, q), yxi.at[there], s_ys.at[q], s_yx.at[there], to_x)

    def place(s, k):
        q = jnp.where(s == 0, quarter[0], jnp.where(s == 1, quarter[1], jnp.where(s == 2, quarter[2], quarter[3])))
        return pl.ds(col(q * dk + k * CW), CW)

    def finish(i, q, used):
        s, k = strip_slot(i)
        cols = place(s, k)
        pltpu.make_async_copy(po.at[0, i], tile(2, 0), s_ld.at[0]).start()
        pltpu.make_async_copy(x.at[:, cols], tile(2, 1), s_ld.at[1]).start()
        wait(r1i.at[i], s_r1.at[i])
        pltpu.make_async_copy(r1i.at[i], tile(2, 2), s_ld.at[2]).start()
        wait(yxi.at[i], s_yx.at[i])
        pltpu.make_async_copy(yxi.at[i], tile(2, 3), s_ld.at[3]).start()
        for c in range(4):
            wait(tile(2, c), s_ld.at[c])
        o = xb[block(2), pl.ds(fq, CW)].astype(f32)
        for c in range(1, 4):
            o = o + xb[block(2), pl.ds(fq + c * CW, CW)].astype(f32)
        out = pltpu.make_async_copy(tile(3, q), y.at[:, cols], s_out.at[q])

        @pl.when(used)
        def _():
            out.wait()

        xb[block(3), pl.ds(fq + q * CW, CW)] = o.astype(bf16)
        out.start()

    def tail(n, _):
        @pl.when(n < 4 * ns)
        def _():
            relay(n)

        @pl.when(n > 2 * ns)
        def _():
            m = n - 1
            late = m - 2 * ns
            finish(m, 0, late > 0)
            finish((late % 2) * ns + late // 2, 1, late > 0)

        return 0

    lax.fori_loop(0, 4 * ns + 1, tail, 0)

    for q in range(2):
        wait(tile(3, q), s_out.at[q])
        wait(tile(1, q), s_ys.at[q])
    wait(x, s_xs.at[0])
    wait(x, s_xs.at[1])
    wait(w1, s_ws.at[0])
    wait(w2, s_ws.at[1])
    wait(db.at[0], s_ws.at[2])
    wait(db.at[1], s_ws.at[3])
    wait(w3, s_ws.at[4])
    wait(db.at[2], s_ws.at[5])
    wait(rdi, s_rs.at[0])
    wait(r1i, s_rs.at[1])


def solution(mesh):
    def body(x, wg, wu, wd):
        rows, dim = x.shape
        dk = dim // 4
        fq = wg.shape[1] // 2
        nch = fq // CW
        ns = dk // CW
        bf16 = jnp.bfloat16
        dma = pltpu.SemaphoreType.DMA
        shapes = [
            (rows, dim),
            (nch, dk, 2 * CW), (nch, dk, 2 * CW), (nch, dk, 2 * CW),
            (3, ns, fq, CW),
            (4 * rows, fq),
            (4, 4 * ns, rows, CW),
            (4 * ns, rows, CW), (4 * ns, rows, CW), (4 * ns, rows, CW),
        ]
        outs = pl.pallas_call(
            kernel,
            out_shape=[jax.ShapeDtypeStruct(s, bf16) for s in shapes],
            in_specs=[pl.BlockSpec(memory_space=pl.ANY)] * 4,
            out_specs=[pl.BlockSpec(memory_space=pl.ANY)] * len(shapes),
            scratch_shapes=[
                pltpu.VMEM((4 * rows, dim), bf16),
                pltpu.VMEM((2, dim, 2 * CW), bf16),
                pltpu.VMEM((2, rows, CW), bf16),
                dma, dma((3,)), dma((6,)), dma((4,)), dma((4,)), dma((4,)),
                dma((nch,)), dma((nch,)), dma((nch,)), dma((ns,)), dma((ns,)), dma((ns,)),
                dma((2,)), dma((2,)), dma((4,)), dma((2,)),
                dma((4 * ns,)), dma((4 * ns,)), dma((4 * ns,)), dma((2,)), dma((4,)), dma((2,)),
            ],
            compiler_params=pltpu.CompilerParams(
                collective_id=0, has_side_effects=True, vmem_limit_bytes=67043328),
            cost_estimate=pl.CostEstimate(
                flops=6 * rows * 4 * dim * fq, bytes_accessed=4 * rows * dim * 2, transcendentals=0),
        )(x, wg, wu, wd)
        return outs[0]

    return jax.shard_map(body, mesh=mesh, in_specs=(P(("dp", "tp"), None), P("dp", "tp"), P("dp", "tp"), P("tp", "dp")), out_specs=P(("dp", "tp"), None), check_vma=False)
```

```python
import functools

import jax
import jax.numpy as jnp
from jax import lax
from jax.experimental import pallas as pl
from jax.experimental.pallas import tpu as pltpu
from jax.sharding import PartitionSpec as P

CW = 256


def kernel(x, wg, wu, wd, y, w1, w2, w3, db, hb, po, rdi, r1i, yxi,
           xb, wv, hst, s_loc, s_xs, s_ws, s_xx, s_xy, s_xd, s_w1, s_w2, s_w3, s_d1, s_d2, s_d3,
           s_wv, s_h, s_po, s_rs, s_rd, s_r1, s_yx, s_ys, s_ld, s_out):
    rows, dim = x.shape
    dk = dim // 4
    fq = wg.shape[1] // 2
    nch = fq // CW
    first = nch // 2
    ns = dk // CW
    f32, bf16 = jnp.float32, jnp.bfloat16

    t = lax.axis_index("tp")
    d = lax.axis_index("dp")
    side = d // 2
    core = d % 2
    mate = d + 1 - 2 * core
    quarter = [d, mate, (d + 2) % 4, (mate + 2) % 4]
    to_mate = {"dp": mate}
    to_x = {"dp": (d + 2) % 4}
    to_y = {"tp": 1 - t}

    def col(v, size=128):
        return v if isinstance(v, int) else pl.multiple_of(v, size)

    def send(src, dst, send_sem, recv_sem, where):
        pltpu.make_async_remote_copy(
            src_ref=src, dst_ref=dst, send_sem=send_sem, recv_sem=recv_sem,
            device_id=where, device_id_type=pl.DeviceIdType.MESH).start()

    def wait(ref, sem, name="w"):
        with jax.named_scope(name):
            pltpu.make_async_copy(ref, ref, sem).wait()

    def block(b):
        return pl.ds(col(b * rows, rows), rows)

    def slot(s):
        return pl.ds(s * dk, dk)

    barrier = pltpu.get_barrier_semaphore()
    for where in (to_mate, to_x, to_y):
        pl.semaphore_signal(barrier, inc=1, device_id=where, device_id_type=pl.DeviceIdType.MESH)
    pl.semaphore_wait(barrier, 3)

    for s in range(4):
        src = x.at[:, pl.ds(col(quarter[s] * dk), dk)]
        send(src, xb.at[block(2), slot(s ^ 2)], s_xs.at[0], s_xx.at[s ^ 2], to_x)
        send(src, xb.at[block(1), slot(s)], s_xs.at[1], s_xy.at[s], to_y)
    for s in range(4):
        src = x.at[:, pl.ds(col(quarter[s] * dk), dk)]
        pltpu.make_async_copy(src, xb.at[block(0), slot(s)], s_loc).start()

    def send_chunk(j, _):
        for m, w in enumerate((wg, wu)):
            away = w.at[:, pl.ds(col((1 - side) * fq + j * CW), CW)]
            here = w.at[:, pl.ds(col(side * fq + j * CW), CW)]
            send(away, w2.at[j, :, pl.ds(m * CW, CW)], s_ws.at[1], s_w2.at[j], to_x)
            send(here, w1.at[j, :, pl.ds(m * CW, CW)], s_ws.at[0], s_w1.at[j], to_mate)
        return 0

    lax.fori_loop(0, nch, send_chunk, 0)

    def send_strip(k, _):
        cols = pl.ds(col(k * CW), CW)
        send(wd.at[pl.ds(col((1 - side) * fq), fq), cols], db.at[1, k], s_ws.at[3], s_d2.at[k], to_x)
        send(wd.at[pl.ds(col(side * fq), fq), cols], db.at[0, k], s_ws.at[2], s_d1.at[k], to_mate)
        return 0

    lax.fori_loop(0, ns, send_strip, 0)

    for s in (2, 3, 0, 1):
        piece = xb.at[block(2), slot(s)]
        wait(piece, s_xx.at[s], "xx")
        send(piece, xb.at[block(3), slot(s)], s_xs.at[2], s_xd.at[s], to_y)

    def load_chunk(j, p):
        for m, w in enumerate((wg, wu)):
            here = w.at[:, pl.ds(col(side * fq + j * CW), CW)]
            pltpu.make_async_copy(here, wv.at[p, slot(0), pl.ds(m * CW, CW)], s_wv.at[p]).start()
        for s, w in ((1, w1), (2, w2), (3, w3)):
            pltpu.make_async_copy(w.at[j], wv.at[p, slot(s)], s_wv.at[p]).start()

    def fetch_chunk(j):
        wait(w2.at[j], s_w2.at[j], "w2")
        send(w2.at[j], w3.at[j], s_ws.at[4], s_w3.at[j], to_mate)
        wait(w1.at[j], s_w1.at[j], "w1")
        wait(w3.at[j], s_w3.at[j], "w3")
        load_chunk(j, 0)

    def hcopy(b, j, q):
        return pltpu.make_async_copy(hst.at[q], hb.at[block(b), pl.ds(col(j * CW), CW)], s_h.at[q])

    def gate(b, j, p, q, used=True):
        @pl.when(used)
        def _():
            hcopy(b, j, q).wait()

        ab = jnp.dot(xb[block(b), :], wv[p], preferred_element_type=f32)
        a = ab[:, :CW]
        hst[q] = (a * jax.nn.sigmoid(a) * ab[:, CW:]).astype(bf16)
        hcopy(b, j, q).start()

    wait(xb.at[block(0), :], s_loc, "loc")
    for s in range(4):
        wait(xb.at[block(1), slot(s)], s_xy.at[s], "xy")

    def chunk(j, _):
        fetch_chunk(j)

        @pl.when(j == first)
        def _():
            for s in range(4):
                wait(xb.at[block(3), slot(s)], s_xd.at[s], "xd")

        @pl.when(j >= first)
        def _():
            load_chunk(j - first, 1)

        wait(wv.at[0], s_wv.at[0], "wv")

        def rows_of(n, _):
            g = 3 * j + n
            gate((n + 1) % 3, j, 0, g % 2, g >= 2)
            return 0

        lax.fori_loop(0, 3, rows_of, 0)

        @pl.when(j >= first)
        def _():
            wait(wv.at[1], s_wv.at[1], "wv")
            gate(3, j - first, 1, 2, j > first)

        return 0

    last = nch - 1
    lax.fori_loop(0, last, chunk, 0)

    hcols = pl.ds(0, fq)

    def load_h(b):
        pltpu.make_async_copy(hb.at[block(b), :], xb.at[block(b), hcols], s_ld.at[b]).start()

    def wait_h(b):
        wait(xb.at[block(b), hcols], s_ld.at[b], "ld")

    def tile(b, c, n=1):
        return xb.at[block(b), pl.ds(fq + c * CW, n * CW)]

    def load_pair(half, k, p):
        left = pl.ds(0, CW)
        right = pl.ds(CW, CW)
        if half == 0:
            src = (wd.at[pl.ds(col(side * fq), fq), pl.ds(col(k * CW), CW)], db.at[0, k])
        else:
            src = (db.at[1, k], db.at[2, k])
        pltpu.make_async_copy(src[0], wv.at[p, hcols, left], s_wv.at[p]).start()
        pltpu.make_async_copy(src[1], wv.at[p, hcols, right], s_wv.at[p]).start()

    def wait_pair(p):
        wait(wv.at[p, hcols, :], s_wv.at[p], "wv")

    def down(b, u, p):
        o = jnp.dot(xb[block(b), hcols], wv[p, hcols, :], preferred_element_type=f32)
        xb[block(b), pl.ds(fq, 2 * CW)] = o.astype(bf16)
        for m in range(2):
            pltpu.make_async_copy(tile(b, m), po.at[b, u, m], s_po).start()
        wait(tile(b, 0, 2), s_po, "po")

    def ship_d(u):
        for m in range(2):
            send(po.at[3, u, m], rdi.at[u, m], s_rs.at[0], s_rd.at[2 * u + m], to_y)

    def ship_1(u):
        for m in range(2):
            send(po.at[1, u, m], r1i.at[u, m], s_rs.at[1], s_r1.at[2 * u + m], to_y)

    wait(db.at[0, 0], s_d1.at[0], "d1")
    load_pair(0, 0, 2)
    fetch_chunk(last)
    wait(wv.at[0], s_wv.at[0], "wv")
    q = (3 * last) % 2
    gate(1, last, 0, q)
    hcopy(1, last, q).wait()
    load_h(1)
    gate(0, last, 0, 1 - q)
    wait_h(1)

    def early(k, _):
        p = 2 - k % 2

        @pl.when(k + 1 < ns)
        def _():
            wait(db.at[0, k + 1], s_d1.at[k + 1], "d1")
            load_pair(0, k + 1, 3 - p)

        wait_pair(p)
        down(1, k, p)
        ship_1(k)
        return 0

    lax.fori_loop(0, ns, early, 0)

    done = last - first
    load_chunk(done, 1)
    gate(2, last, 0, q, False)
    hcopy(0, last, 1 - q).wait()
    hcopy(2, last, q).wait()
    wait(xb.at[block(2), :], s_xs.at[2], "xs")
    load_h(0)
    load_h(2)

    def diagonal(j, _):
        i = j - done
        p = jnp.where(j == last, 0, 1 + i % 2)

        @pl.when(j + 1 < last)
        def _():
            load_chunk(j + 1, 2 - i % 2)

        @pl.when(j < last)
        def _():
            wait(wv.at[p], s_wv.at[p], "wv")

        gate(3, j, p, 2)
        return 0

    lax.fori_loop(done, nch, diagonal, 0)
    load_pair(0, 0, 1)
    hcopy(3, last, 2).wait()
    load_h(3)
    for b in (0, 2, 3):
        wait_h(b)

    def own_half(k, _):
        p = 1 + k % 2

        @pl.when(k + 1 < ns)
        def _():
            load_pair(0, k + 1, 3 - p)

        wait_pair(p)

        def rows_of(n, _):
            down(jnp.where(n == 0, 3, jnp.where(n == 1, 2, 0)), k, p)

            @pl.when(n == 0)
            def _():
                ship_d(k)

            return 0

        lax.fori_loop(0, 3, rows_of, 0)
        return 0

    def fetch_pair(k, p):
        wait(db.at[1, k], s_d2.at[k], "d2")
        send(db.at[1, k], db.at[2, k], s_ws.at[5], s_d3.at[k], to_mate)
        wait(db.at[2, k], s_d3.at[k], "d3")
        load_pair(1, k, p)

    lax.fori_loop(0, ns, own_half, 0)

    def relay(half, k, m, used):
        u = half * ns + k
        pltpu.make_async_copy(po.at[2, u, m], tile(0, 4), s_ld.at[0]).start()
        wait(rdi.at[u, m], s_rd.at[2 * u + m], "rd")
        pltpu.make_async_copy(rdi.at[u, m], tile(0, 5), s_ld.at[1]).start()

        @pl.when(used)
        def _():
            wait(tile(1, 4 + m), s_ys.at[m], "ys")

        wait(tile(0, 4), s_ld.at[0], "ld")
        wait(tile(0, 5), s_ld.at[1], "ld")
        o = xb[block(0), pl.ds(fq + 4 * CW, CW)].astype(f32) + xb[block(0), pl.ds(fq + 5 * CW, CW)].astype(f32)
        xb[block(1), pl.ds(fq + (4 + m) * CW, CW)] = o.astype(bf16)
        v = (1 - half) * ns + k
        send(tile(1, 4 + m), yxi.at[v, m], s_ys.at[m], s_yx.at[2 * v + m], to_x)

    def other_half(k, _):
        p = k % 3
        u = ns + k
        wait_pair(p)

        def rows_of(n, _):
            down(jnp.where(n == 0, 3, jnp.where(n == 1, 1, jnp.where(n == 2, 2, 0))), u, p)

            @pl.when(n == 0)
            def _():
                ship_d(u)

            @pl.when(n == 1)
            def _():
                ship_1(u)

            @pl.when((n == 1) & (k + 1 < ns))
            def _():
                fetch_pair(k + 1, (k + 1) % 3)

            return 0

        lax.fori_loop(0, 4, rows_of, 0)
        for m in range(2):
            relay(0, k, m, k > 0)
        return 0

    fetch_pair(0, 0)
    lax.fori_loop(0, ns, other_half, 0)

    def finish(half, k, m, used):
        u = half * ns + k
        n = 2 * half + m
        cols = pl.ds(col(quarter[n] * dk + k * CW), CW)
        pltpu.make_async_copy(po.at[0, u, m], tile(2, 2), s_ld.at[0]).start()
        pltpu.make_async_copy(x.at[:, cols], tile(2, 3), s_ld.at[1]).start()
        wait(r1i.at[u, m], s_r1.at[2 * u + m], "r1")
        pltpu.make_async_copy(r1i.at[u, m], tile(2, 4), s_ld.at[2]).start()
        wait(yxi.at[u, m], s_yx.at[2 * u + m], "yx")
        pltpu.make_async_copy(yxi.at[u, m], tile(2, 5), s_ld.at[3]).start()
        for c in range(4):
            wait(tile(2, 2 + c), s_ld.at[c], "ld")
        out = pltpu.make_async_copy(tile(3, 2 + n), y.at[:, cols], s_out.at[n])

        @pl.when(used)
        def _():
            out.wait()

        o = xb[block(2), pl.ds(fq + 2 * CW, CW)].astype(f32)
        for c in range(3, 6):
            o = o + xb[block(2), pl.ds(fq + c * CW, CW)].astype(f32)
        xb[block(3), pl.ds(fq + (2 + n) * CW, CW)] = o.astype(bf16)
        out.start()

    def tail(k, _):
        @pl.when(k < ns)
        def _():
            for m in range(2):
                relay(1, k, m, True)

        @pl.when(k > 0)
        def _():
            for half in range(2):
                for m in range(2):
                    finish(half, k - 1, m, k > 1)

        return 0

    lax.fori_loop(0, ns + 1, tail, 0)

    for n in range(4):
        wait(tile(3, 2 + n), s_out.at[n], "out")
    for m in range(2):
        wait(tile(1, 4 + m), s_ys.at[m], "ys")
    wait(x, s_xs.at[0], "xs")
    wait(x, s_xs.at[1], "xs")
    wait(w1, s_ws.at[0], "ws")
    wait(w2, s_ws.at[1], "ws")
    wait(db.at[0], s_ws.at[2], "ws")
    wait(db.at[1], s_ws.at[3], "ws")
    wait(w3, s_ws.at[4], "ws")
    wait(db.at[2], s_ws.at[5], "ws")
    wait(rdi, s_rs.at[0], "rs")
    wait(r1i, s_rs.at[1], "rs")


def solution(mesh):
    def body(x, wg, wu, wd):
        rows, dim = x.shape
        dk = dim // 4
        fq = wg.shape[1] // 2
        nch = fq // CW
        ns = dk // CW
        bf16 = jnp.bfloat16
        dma = pltpu.SemaphoreType.DMA
        shapes = [
            (rows, dim),
            (nch, dk, 2 * CW), (nch, dk, 2 * CW), (nch, dk, 2 * CW),
            (3, ns, fq, CW),
            (4 * rows, fq),
            (4, 2 * ns, 2, rows, CW),
            (2 * ns, 2, rows, CW), (2 * ns, 2, rows, CW), (2 * ns, 2, rows, CW),
        ]
        outs = pl.pallas_call(
            kernel,
            out_shape=[jax.ShapeDtypeStruct(s, bf16) for s in shapes],
            in_specs=[pl.BlockSpec(memory_space=pl.ANY)] * 4,
            out_specs=[pl.BlockSpec(memory_space=pl.ANY)] * len(shapes),
            scratch_shapes=[
                pltpu.VMEM((4 * rows, dim), bf16),
                pltpu.VMEM((3, dim, 2 * CW), bf16),
                pltpu.VMEM((3, rows, CW), bf16),
                dma, dma((3,)), dma((6,)), dma((4,)), dma((4,)), dma((4,)),
                dma((nch,)), dma((nch,)), dma((nch,)), dma((ns,)), dma((ns,)), dma((ns,)),
                dma((3,)), dma((3,)), dma, dma((2,)),
                dma((4 * ns,)), dma((4 * ns,)), dma((4 * ns,)), dma((2,)), dma((4,)), dma((4,)),
            ],
            compiler_params=pltpu.CompilerParams(
                collective_id=0, has_side_effects=True, vmem_limit_bytes=67043328),
            cost_estimate=pl.CostEstimate(
                flops=6 * rows * 4 * dim * fq, bytes_accessed=4 * rows * dim * 2, transcendentals=0),
        )(x, wg, wu, wd)
        return outs[0]

    return jax.shard_map(body, mesh=mesh, in_specs=(P(("dp", "tp"), None), P("dp", "tp"), P("dp", "tp"), P("tp", "dp")), out_specs=P(("dp", "tp"), None), check_vma=False)
```

```python
import functools

import jax
import jax.numpy as jnp
from jax import lax
from jax.experimental import pallas as pl
from jax.experimental.pallas import tpu as pltpu
from jax.sharding import PartitionSpec as P

CW = 256


def kernel(x, wg, wu, wd, y, w1, w2, w3, db, hb, po, rdi, r1i, yxi, bxi,
           xb, wv, hst, s_loc, s_xs, s_ws, s_xx, s_xy, s_xd, s_w1, s_w2, s_w3, s_d1, s_d2, s_d3,
           s_wv, s_h, s_po, s_rs, s_rd, s_r1, s_yx, s_bx, s_ys, s_yb, s_ld, s_out):
    rows, dim = x.shape
    dk = dim // 4
    fq = wg.shape[1] // 2
    nch = fq // CW
    first = nch // 2
    ns = dk // CW
    f32, bf16 = jnp.float32, jnp.bfloat16

    t = lax.axis_index("tp")
    d = lax.axis_index("dp")
    side = d // 2
    core = d % 2
    mate = d + 1 - 2 * core
    quarter = [d, mate, (d + 2) % 4, (mate + 2) % 4]
    to_mate = {"dp": mate}
    to_x = {"dp": (d + 2) % 4}
    to_y = {"tp": 1 - t}

    def col(v, size=128):
        return v if isinstance(v, int) else pl.multiple_of(v, size)

    def send(src, dst, send_sem, recv_sem, where):
        pltpu.make_async_remote_copy(
            src_ref=src, dst_ref=dst, send_sem=send_sem, recv_sem=recv_sem,
            device_id=where, device_id_type=pl.DeviceIdType.MESH).start()

    def wait(ref, sem, name="w"):
        with jax.named_scope(name):
            pltpu.make_async_copy(ref, ref, sem).wait()

    def block(b):
        return pl.ds(col(b * rows, rows), rows)

    def slot(s):
        return pl.ds(s * dk, dk)

    barrier = pltpu.get_barrier_semaphore()
    for where in (to_mate, to_x, to_y):
        pl.semaphore_signal(barrier, inc=1, device_id=where, device_id_type=pl.DeviceIdType.MESH)
    pl.semaphore_wait(barrier, 3)

    for s in range(4):
        src = x.at[:, pl.ds(col(quarter[s] * dk), dk)]
        send(src, xb.at[block(2), slot(s ^ 2)], s_xs.at[0], s_xx.at[s ^ 2], to_x)
        send(src, xb.at[block(1), slot(s)], s_xs.at[1], s_xy.at[s], to_y)
    for s in range(4):
        src = x.at[:, pl.ds(col(quarter[s] * dk), dk)]
        pltpu.make_async_copy(src, xb.at[block(0), slot(s)], s_loc).start()

    def send_chunk(j, _):
        for m, w in enumerate((wg, wu)):
            away = w.at[:, pl.ds(col((1 - side) * fq + j * CW), CW)]
            here = w.at[:, pl.ds(col(side * fq + j * CW), CW)]
            send(away, w2.at[j, :, pl.ds(m * CW, CW)], s_ws.at[1], s_w2.at[j], to_x)
            send(here, w1.at[j, :, pl.ds(m * CW, CW)], s_ws.at[0], s_w1.at[j], to_mate)
        return 0

    lax.fori_loop(0, nch, send_chunk, 0)

    def send_strip(k, _):
        cols = pl.ds(col(k * CW), CW)
        send(wd.at[pl.ds(col((1 - side) * fq), fq), cols], db.at[1, k], s_ws.at[3], s_d2.at[k], to_x)
        send(wd.at[pl.ds(col(side * fq), fq), cols], db.at[0, k], s_ws.at[2], s_d1.at[k], to_mate)
        return 0

    lax.fori_loop(0, ns, send_strip, 0)

    for s in (2, 3, 0, 1):
        piece = xb.at[block(2), slot(s)]
        wait(piece, s_xx.at[s], "xx")
        send(piece, xb.at[block(3), slot(s)], s_xs.at[2], s_xd.at[s], to_y)

    def load_here(j, p):
        for m, w in enumerate((wg, wu)):
            here = w.at[:, pl.ds(col(side * fq + j * CW), CW)]
            pltpu.make_async_copy(here, wv.at[p, slot(0), pl.ds(m * CW, CW)], s_wv.at[p]).start()

    def load_slot(w, j, n, p):
        pltpu.make_async_copy(w.at[j], wv.at[p, slot(n)], s_wv.at[p]).start()

    def load_chunk(j, p):
        load_here(j, p)
        for n, w in ((1, w1), (2, w2), (3, w3)):
            load_slot(w, j, n, p)

    def fetch_chunk(j):
        load_here(j, 0)
        wait(w1.at[j], s_w1.at[j], "w1")
        load_slot(w1, j, 1, 0)
        wait(w2.at[j], s_w2.at[j], "w2")
        send(w2.at[j], w3.at[j], s_ws.at[4], s_w3.at[j], to_mate)
        load_slot(w2, j, 2, 0)
        wait(w3.at[j], s_w3.at[j], "w3")
        load_slot(w3, j, 3, 0)

    def hcopy(b, j, q):
        return pltpu.make_async_copy(hst.at[q], hb.at[block(b), pl.ds(col(j * CW), CW)], s_h.at[q])

    def gated(b, p):
        ab = jnp.dot(xb[block(b), :], wv[p], preferred_element_type=f32)
        a = ab[:, :CW]
        return (a * jax.nn.sigmoid(a) * ab[:, CW:]).astype(bf16)

    def gate(b, j, p, q, used=True, to=None):
        to = b if to is None else to

        @pl.when(used)
        def _():
            hcopy(to, j, q).wait()

        hst[q] = gated(b, p)
        hcopy(to, j, q).start()

    wait(xb.at[block(0), :], s_loc, "loc")
    for s in range(4):
        wait(xb.at[block(1), slot(s)], s_xy.at[s], "xy")

    def chunk(j, _):
        fetch_chunk(j)

        @pl.when(j == first)
        def _():
            for s in range(4):
                wait(xb.at[block(3), slot(s)], s_xd.at[s], "xd")

        @pl.when(j >= first)
        def _():
            load_chunk(j - first, 1)

        wait(wv.at[0], s_wv.at[0], "wv")

        def rows_of(n, _):
            g = 3 * j + n
            gate((n + 1) % 3, j, 0, g % 2, g >= 2)
            return 0

        lax.fori_loop(0, 3, rows_of, 0)

        @pl.when(j >= first)
        def _():
            wait(wv.at[1], s_wv.at[1], "wv")
            gate(3, j - first, 1, 2, j > first)

        return 0

    last = nch - 1
    lax.fori_loop(0, last, chunk, 0)

    hcols = pl.ds(0, fq)

    def load_h(b, to):
        pltpu.make_async_copy(hb.at[block(b), :], xb.at[block(to), hcols], s_ld.at[to]).start()

    def wait_h(to):
        wait(xb.at[block(to), hcols], s_ld.at[to], "ld")

    def tile(b, c, n=1):
        return xb.at[block(b), pl.ds(fq + c * CW, n * CW)]

    def load_pair(half, k, p):
        left = pl.ds(0, CW)
        right = pl.ds(CW, CW)
        if half == 0:
            src = (wd.at[pl.ds(col(side * fq), fq), pl.ds(col(k * CW), CW)], db.at[0, k])
        else:
            src = (db.at[1, k], db.at[2, k])
        pltpu.make_async_copy(src[0], wv.at[p, hcols, left], s_wv.at[p]).start()
        pltpu.make_async_copy(src[1], wv.at[p, hcols, right], s_wv.at[p]).start()

    def wait_pair(p):
        wait(wv.at[p, hcols, :], s_wv.at[p], "wv")

    def down(b, out, u, p, start=0, size=rows):
        here = pl.ds(col(b * rows + start, size), size)
        there = pl.ds(col(start, size), size)
        o = jnp.dot(xb[here, hcols], wv[p, hcols, :], preferred_element_type=f32)
        xb[here, pl.ds(fq, 2 * CW)] = o.astype(bf16)
        for m in range(2):
            pltpu.make_async_copy(xb.at[here, pl.ds(fq + m * CW, CW)], po.at[out, u, m, there, :], s_po).start()
        wait(xb.at[here, pl.ds(fq, 2 * CW)], s_po, "po")

    def ship_d(u):
        for m in range(2):
            send(po.at[3, u, m], rdi.at[u, m], s_rs.at[0], s_rd.at[2 * u + m], to_y)

    def ship_1(u, start=0, size=rows):
        there = pl.ds(col(start, size), size)
        for m in range(2):
            send(po.at[1, u, m, there, :], r1i.at[u, m, there, :], s_rs.at[1], s_r1.at[2 * u + m], to_y)

    q = (3 * last) % 2
    for n in range(2):
        hcopy(0, 0, n).wait()
    early_cols = pl.ds(0, last * CW)
    pltpu.make_async_copy(hb.at[block(1), early_cols], xb.at[block(0), early_cols], s_ld.at[0]).start()
    wait(db.at[0, 0], s_d1.at[0], "d1")
    load_pair(0, 0, 2)
    fetch_chunk(last)
    wait(wv.at[0], s_wv.at[0], "wv")
    xb[block(0), pl.ds(last * CW, CW)] = gated(1, 0)
    for s in range(4):
        src = x.at[:, pl.ds(col(quarter[s] * dk), dk)]
        pltpu.make_async_copy(src, xb.at[block(1), slot(s)], s_loc).start()
    wait(xb.at[block(0), early_cols], s_ld.at[0], "ld")
    part = rows // 2

    def early(i, _):
        k = i // 2
        r = i % 2
        p = 2 - k % 2

        @pl.when((r == 0) & (k + 1 < ns))
        def _():
            wait(db.at[0, k + 1], s_d1.at[k + 1], "d1")
            load_pair(0, k + 1, 3 - p)

        @pl.when(r == 0)
        def _():
            wait_pair(p)

        down(0, 1, k, p, r * part, part)
        ship_1(k, r * part, part)
        return 0

    lax.fori_loop(0, 2 * ns, early, 0)

    done = last - first
    load_chunk(done, 1)
    wait(xb.at[block(1), :], s_loc, "loc")
    gate(2, last, 0, q, False)
    gate(1, last, 0, 1 - q, False, 0)
    hcopy(2, last, q).wait()
    hcopy(0, last, 1 - q).wait()
    wait(xb.at[block(2), :], s_xs.at[2], "xs")
    load_h(2, 2)
    load_h(0, 1)

    def diagonal(j, _):
        i = j - done
        p = jnp.where(j == last, 0, 1 + i % 2)

        @pl.when(j + 1 < last)
        def _():
            load_chunk(j + 1, 2 - i % 2)

        @pl.when(j < last)
        def _():
            wait(wv.at[p], s_wv.at[p], "wv")

        gate(3, j, p, 2)
        return 0

    lax.fori_loop(done, nch, diagonal, 0)
    load_pair(0, 0, 1)
    hcopy(3, last, 2).wait()
    load_h(3, 3)
    for b in (1, 2, 3):
        wait_h(b)

    def own_half(k, _):
        p = 1 + k % 2

        @pl.when(k + 1 < ns)
        def _():
            load_pair(0, k + 1, 3 - p)

        wait_pair(p)

        def rows_of(n, _):
            b = 3 - n
            down(b, jnp.where(b == 1, 0, b), k, p)

            @pl.when((n == 0) & (k + 1 < ns))
            def _():
                ship_d(k)

            @pl.when((n == 0) & (k + 1 == ns))
            def _():
                for m in range(2):
                    send(po.at[3, ns - 1, m], bxi.at[m], s_rs.at[2], s_bx.at[m], to_x)

            @pl.when((n == 1) & (k + 1 == ns))
            def _():
                v = 2 * ns - 1
                for m in range(2):
                    send(po.at[2, ns - 1, m], yxi.at[v, m], s_rs.at[3], s_yx.at[2 * v + m], to_x)

            return 0

        lax.fori_loop(0, 3, rows_of, 0)
        return 0

    def fetch_pair(k, p):
        wait(db.at[1, k], s_d2.at[k], "d2")
        send(db.at[1, k], db.at[2, k], s_ws.at[5], s_d3.at[k], to_mate)
        wait(db.at[2, k], s_d3.at[k], "d3")
        load_pair(1, k, p)

    lax.fori_loop(0, ns, own_half, 0)

    def total(tiles):
        o = xb[block(tiles[0][0]), pl.ds(fq + tiles[0][1] * CW, CW)].astype(f32)
        for b, c in tiles[1:]:
            o = o + xb[block(b), pl.ds(fq + c * CW, CW)].astype(f32)
        return o.astype(bf16)

    def relay(half, k, m, turn):
        u = half * ns + k
        pltpu.make_async_copy(po.at[2, u, m], tile(0, 2), s_ld.at[0]).start()
        wait(rdi.at[u, m], s_rd.at[2 * u + m], "rd")
        pltpu.make_async_copy(rdi.at[u, m], tile(0, 3), s_ld.at[1]).start()
        ring = turn % 4

        @pl.when(turn >= 4)
        def _():
            wait(tile(ring, 4 + m), s_ys.at[2 * ring + m], "ys")

        wait(tile(0, 2), s_ld.at[0], "ld")
        wait(tile(0, 3), s_ld.at[1], "ld")
        xb[block(ring), pl.ds(fq + (4 + m) * CW, CW)] = total(((0, 2), (0, 3)))
        v = (1 - half) * ns + k
        send(tile(ring, 4 + m), yxi.at[v, m], s_ys.at[2 * ring + m], s_yx.at[2 * v + m], to_x)

    def other_half(k, _):
        p = k % 3
        u = ns + k
        wait_pair(p)

        def rows_of(n, _):
            b = jnp.where(n == 0, 3, jnp.where(n == 1, 0, jnp.where(n == 2, 2, 1)))
            out = jnp.where(n == 0, 3, jnp.where(n == 1, 1, jnp.where(n == 2, 2, 0)))
            down(b, out, u, p)

            @pl.when(n == 0)
            def _():
                ship_d(u)

            @pl.when((n == 1) & (k > 0))
            def _():
                ship_1(u - 1)

            @pl.when((n == 1) & (k + 1 < ns))
            def _():
                fetch_pair(k + 1, (k + 1) % 3)

            return 0

        lax.fori_loop(0, 4, rows_of, 0)

        @pl.when(k + 1 < ns)
        def _():
            for m in range(2):
                relay(0, k, m, k)

        return 0

    fetch_pair(0, 0)
    lax.fori_loop(0, ns, other_half, 0)

    v = 2 * ns - 1
    for m in range(2):
        pltpu.make_async_copy(po.at[1, v, m], tile(1, 2), s_ld.at[0]).start()
        wait(bxi.at[m], s_bx.at[m], "bx")
        pltpu.make_async_copy(bxi.at[m], tile(1, 3), s_ld.at[1]).start()
        wait(tile(1, 2), s_ld.at[0], "ld")
        wait(tile(1, 3), s_ld.at[1], "ld")
        xb[block(2), pl.ds(fq + m * CW, CW)] = total(((1, 2), (1, 3)))
        send(tile(2, m), r1i.at[v, m], s_yb.at[m], s_r1.at[2 * v + m], to_y)

    parts = ((1, 2), (1, 3), (2, 2), (2, 3))

    def finish(half, k, m, used):
        u = half * ns + k
        n = 2 * half + m
        cols = pl.ds(col(quarter[n] * dk + k * CW), CW)
        pltpu.make_async_copy(po.at[0, u, m], tile(*parts[0]), s_ld.at[0]).start()
        pltpu.make_async_copy(x.at[:, cols], tile(*parts[1]), s_ld.at[1]).start()
        wait(r1i.at[u, m], s_r1.at[2 * u + m], "r1")
        pltpu.make_async_copy(r1i.at[u, m], tile(*parts[2]), s_ld.at[2]).start()
        wait(yxi.at[u, m], s_yx.at[2 * u + m], "yx")
        pltpu.make_async_copy(yxi.at[u, m], tile(*parts[3]), s_ld.at[3]).start()
        for c in range(4):
            wait(tile(*parts[c]), s_ld.at[c], "ld")
        out = pltpu.make_async_copy(tile(3, n), y.at[:, cols], s_out.at[n])

        @pl.when(used)
        def _():
            out.wait()

        xb[block(3), pl.ds(fq + n * CW, CW)] = total(parts)
        out.start()

    def tail(k, _):
        @pl.when(k < ns)
        def _():
            for m in range(2):
                relay(1, k, m, ns - 1 + k)

        @pl.when(k > 0)
        def _():
            for m in range(2):
                for half in (1, 0):
                    finish(half, k - 1, m, k > 1)

        return 0

    lax.fori_loop(0, ns + 1, tail, 0)

    for n in range(4):
        wait(tile(3, n), s_out.at[n], "out")
    for m in range(2):
        wait(tile(2, m), s_yb.at[m], "yb")
        for ring in range(4):
            wait(tile(ring, 4 + m), s_ys.at[2 * ring + m], "ys")
    wait(x, s_xs.at[0], "xs")
    wait(x, s_xs.at[1], "xs")
    wait(w1, s_ws.at[0], "ws")
    wait(w2, s_ws.at[1], "ws")
    wait(db.at[0], s_ws.at[2], "ws")
    wait(db.at[1], s_ws.at[3], "ws")
    wait(w3, s_ws.at[4], "ws")
    wait(db.at[2], s_ws.at[5], "ws")
    wait(rdi.at[pl.ds(0, 2 * ns - 1)], s_rs.at[0], "rs")
    wait(r1i.at[pl.ds(0, 2 * ns - 1)], s_rs.at[1], "rs")
    wait(bxi, s_rs.at[2], "rs")
    wait(bxi, s_rs.at[3], "rs")


def solution(mesh):
    def body(x, wg, wu, wd):
        rows, dim = x.shape
        dk = dim // 4
        fq = wg.shape[1] // 2
        nch = fq // CW
        ns = dk // CW
        bf16 = jnp.bfloat16
        dma = pltpu.SemaphoreType.DMA
        shapes = [
            (rows, dim),
            (nch, dk, 2 * CW), (nch, dk, 2 * CW), (nch, dk, 2 * CW),
            (3, ns, fq, CW),
            (4 * rows, fq),
            (4, 2 * ns, 2, rows, CW),
            (2 * ns, 2, rows, CW), (2 * ns, 2, rows, CW), (2 * ns, 2, rows, CW), (2, rows, CW),
        ]
        outs = pl.pallas_call(
            kernel,
            out_shape=[jax.ShapeDtypeStruct(s, bf16) for s in shapes],
            in_specs=[pl.BlockSpec(memory_space=pl.ANY)] * 4,
            out_specs=[pl.BlockSpec(memory_space=pl.ANY)] * len(shapes),
            scratch_shapes=[
                pltpu.VMEM((4 * rows, dim), bf16),
                pltpu.VMEM((3, dim, 2 * CW), bf16),
                pltpu.VMEM((3, rows, CW), bf16),
                dma, dma((3,)), dma((6,)), dma((4,)), dma((4,)), dma((4,)),
                dma((nch,)), dma((nch,)), dma((nch,)), dma((ns,)), dma((ns,)), dma((ns,)),
                dma((3,)), dma((3,)), dma, dma((4,)),
                dma((4 * ns,)), dma((4 * ns,)), dma((4 * ns,)), dma((2,)), dma((8,)), dma((2,)), dma((4,)), dma((4,)),
            ],
            compiler_params=pltpu.CompilerParams(
                collective_id=0, has_side_effects=True, vmem_limit_bytes=67043328),
            cost_estimate=pl.CostEstimate(
                flops=6 * rows * 4 * dim * fq, bytes_accessed=4 * rows * dim * 2, transcendentals=0),
        )(x, wg, wu, wd)
        return outs[0]

    return jax.shard_map(body, mesh=mesh, in_specs=(P(("dp", "tp"), None), P("dp", "tp"), P("dp", "tp"), P("tp", "dp")), out_specs=P(("dp", "tp"), None), check_vma=False)
```

```python
import functools

import jax
import jax.numpy as jnp
from jax import lax
from jax.experimental import pallas as pl
from jax.experimental.pallas import tpu as pltpu
from jax.sharding import PartitionSpec as P

CW = 256


def kernel(x, wg, wu, wd, y, w1, w2, w3, db, hb, po, rdi, r1i, yxi, bxi,
           xb, wv, hst, acc, s_loc, s_xs, s_ws, s_xx, s_xy, s_xd, s_w1, s_w2, s_w3, s_d1, s_d2, s_d3,
           s_wv, s_h, s_po, s_rs, s_rd, s_r1, s_yx, s_bx, s_ys, s_yb, s_xb, s_ld, s_out):
    rows, dim = x.shape
    dk = dim // 4
    fq = wg.shape[1] // 2
    nch = fq // CW
    first = nch // 2
    ns = dk // CW
    turned = rows * 7 // 8
    f32, bf16 = jnp.float32, jnp.bfloat16

    t = lax.axis_index("tp")
    d = lax.axis_index("dp")
    side = d // 2
    core = d % 2
    mate = d + 1 - 2 * core
    quarter = [d, mate, (d + 2) % 4, (mate + 2) % 4]
    to_mate = {"dp": mate}
    to_x = {"dp": (d + 2) % 4}
    to_y = {"tp": 1 - t}

    def col(v, size=128):
        return v if isinstance(v, int) else pl.multiple_of(v, size)

    def send(src, dst, send_sem, recv_sem, where):
        pltpu.make_async_remote_copy(
            src_ref=src, dst_ref=dst, send_sem=send_sem, recv_sem=recv_sem,
            device_id=where, device_id_type=pl.DeviceIdType.MESH).start()

    def wait(ref, sem, name="w"):
        with jax.named_scope(name):
            pltpu.make_async_copy(ref, ref, sem).wait()

    def block(b):
        return pl.ds(col(b * rows, rows), rows)

    def slot(s):
        return pl.ds(s * dk, dk)

    barrier = pltpu.get_barrier_semaphore()
    for where in (to_mate, to_x, to_y):
        pl.semaphore_signal(barrier, inc=1, device_id=where, device_id_type=pl.DeviceIdType.MESH)
    with jax.named_scope("bar"):
        pl.semaphore_wait(barrier, 3)

    for s in range(4):
        src = x.at[:, pl.ds(col(quarter[s] * dk), dk)]
        send(src, xb.at[block(2), slot(s ^ 2)], s_xs.at[0], s_xx.at[s ^ 2], to_x)
        send(src, xb.at[block(1), slot(s)], s_xs.at[1], s_xy.at[s], to_y)
    for s in range(4):
        src = x.at[:, pl.ds(col(quarter[s] * dk), dk)]
        pltpu.make_async_copy(src, xb.at[block(0), slot(s)], s_loc).start()

    def send_chunk(j, _):
        for m, w in enumerate((wg, wu)):
            away = w.at[:, pl.ds(col((1 - side) * fq + j * CW), CW)]
            here = w.at[:, pl.ds(col(side * fq + j * CW), CW)]
            send(away, w2.at[j, :, pl.ds(m * CW, CW)], s_ws.at[1], s_w2.at[j], to_x)
            send(here, w1.at[j, :, pl.ds(m * CW, CW)], s_ws.at[0], s_w1.at[j], to_mate)
        return 0

    lax.fori_loop(0, nch, send_chunk, 0)

    def send_strip(k, _):
        cols = pl.ds(col(k * CW), CW)
        send(wd.at[pl.ds(col((1 - side) * fq), fq), cols], db.at[1, k], s_ws.at[3], s_d2.at[k], to_x)
        send(wd.at[pl.ds(col(side * fq), fq), cols], db.at[0, k], s_ws.at[2], s_d1.at[k], to_mate)
        return 0

    lax.fori_loop(0, ns, send_strip, 0)

    for s in (2, 3, 0, 1):
        piece = xb.at[block(2), slot(s)]
        wait(piece, s_xx.at[s], "xx")
        send(piece, xb.at[block(3), slot(s)], s_xs.at[2], s_xd.at[s], to_y)

    def load_here(j, p, sem=None):
        for m, w in enumerate((wg, wu)):
            here = w.at[:, pl.ds(col(side * fq + j * CW), CW)]
            pltpu.make_async_copy(
                here, wv.at[p, slot(0), pl.ds(m * CW, CW)], s_wv.at[p if sem is None else sem]).start()

    def load_slot(w, j, n, p, sem=None):
        pltpu.make_async_copy(w.at[j], wv.at[p, slot(n)], s_wv.at[p if sem is None else sem]).start()

    def load_chunk(j, p):
        load_here(j, p)
        for n, w in ((1, w1), (2, w2), (3, w3)):
            load_slot(w, j, n, p)

    def fetch_rest(j):
        wait(w2.at[j], s_w2.at[j], "w2")
        send(w2.at[j], w3.at[j], s_ws.at[4], s_w3.at[j], to_mate)
        load_slot(w2, j, 2, 0)
        wait(w3.at[j], s_w3.at[j], "w3")
        load_slot(w3, j, 3, 0)

    def fetch_chunk(j):
        load_here(j, 0)
        wait(w1.at[j], s_w1.at[j], "w1")
        load_slot(w1, j, 1, 0)
        fetch_rest(j)

    def hcopy(b, j, q):
        return pltpu.make_async_copy(hst.at[q], hb.at[block(b), pl.ds(col(j * CW), CW)], s_h.at[q])

    def gated(b, p):
        return act(jnp.dot(xb[block(b), :], wv[p], preferred_element_type=f32))

    def act(ab):
        a = ab[:, :CW]
        return (a * jax.nn.sigmoid(a) * ab[:, CW:]).astype(bf16)

    def gate(b, j, p, q, used=True, to=None):
        to = b if to is None else to

        @pl.when(used)
        def _():
            hcopy(to, j, q).wait()

        hst[q] = gated(b, p)
        hcopy(to, j, q).start()

    wait(xb.at[block(0), :], s_loc, "loc")
    for s in range(4):
        wait(xb.at[block(1), slot(s)], s_xy.at[s], "xy")

    def chunk(j, _):
        fetch_chunk(j)

        @pl.when(j == first)
        def _():
            for s in range(4):
                wait(xb.at[block(3), slot(s)], s_xd.at[s], "xd")

        @pl.when(j >= first)
        def _():
            load_chunk(j - first, 1)

        wait(wv.at[0], s_wv.at[0], "wv")

        def rows_of(n, _):
            g = 3 * j + n
            gate((n + 1) % 3, j, 0, g % 2, g >= 2)
            return 0

        lax.fori_loop(0, 3, rows_of, 0)

        @pl.when(j >= first)
        def _():
            wait(wv.at[1], s_wv.at[1], "wv")
            gate(3, j - first, 1, 2, j > first)

        return 0

    last = nch - 1
    lax.fori_loop(0, last, chunk, 0)

    hcols = pl.ds(0, fq)

    def load_h(b, to):
        pltpu.make_async_copy(hb.at[block(b), :], xb.at[block(to), hcols], s_ld.at[to]).start()

    def wait_h(to):
        wait(xb.at[block(to), hcols], s_ld.at[to], "ld")

    def tile(b, c, n=1):
        return xb.at[block(b), pl.ds(fq + c * CW, n * CW)]

    def load_pair(half, k, p):
        left = pl.ds(0, CW)
        right = pl.ds(CW, CW)
        if half == 0:
            src = (wd.at[pl.ds(col(side * fq), fq), pl.ds(col(k * CW), CW)], db.at[0, k])
        else:
            src = (db.at[1, k], db.at[2, k])
        pltpu.make_async_copy(src[0], wv.at[p, hcols, left], s_wv.at[p]).start()
        pltpu.make_async_copy(src[1], wv.at[p, hcols, right], s_wv.at[p]).start()

    def wait_pair(p):
        wait(wv.at[p, hcols, :], s_wv.at[p], "wv")

    def down(b, out, u, p, start=0, size=rows):
        here = pl.ds(col(b * rows + start, size), size)
        there = pl.ds(col(start, size), size)
        o = jnp.dot(xb[here, hcols], wv[p, hcols, :], preferred_element_type=f32)
        xb[here, pl.ds(fq, 2 * CW)] = o.astype(bf16)
        for m in range(2):
            pltpu.make_async_copy(xb.at[here, pl.ds(fq + m * CW, CW)], po.at[out, u, m, there, :], s_po).start()
        wait(xb.at[here, pl.ds(fq, 2 * CW)], s_po, "po")

    def ship_d(u):
        for m in range(2):
            send(po.at[3, u, m], rdi.at[u, m], s_rs.at[0], s_rd.at[2 * u + m], to_y)

    def ship_1(u, start=0, size=rows):
        there = pl.ds(col(start, size), size)
        for m in range(2):
            send(po.at[1, u, m, there, :], r1i.at[u, m, there, :], s_rs.at[1], s_r1.at[2 * u + m], to_y)

    q = (3 * last) % 2
    for n in range(2):
        hcopy(0, 0, n).wait()
    early_cols = pl.ds(0, last * CW)
    pltpu.make_async_copy(hb.at[block(1), early_cols], xb.at[block(0), early_cols], s_ld.at[0]).start()
    wait(db.at[0, 0], s_d1.at[0], "d1")
    load_pair(0, 0, 2)
    at_hand, to_come = pl.ds(0, 2 * dk), pl.ds(2 * dk, 2 * dk)
    load_here(last, 0, 3)
    wait(w1.at[last], s_w1.at[last], "w1")
    load_slot(w1, last, 1, 0, 3)
    wait(wv.at[0, at_hand, :], s_wv.at[3], "wv")
    acc[...] = jnp.dot(xb[block(1), at_hand], wv[0, at_hand, :], preferred_element_type=f32)
    fetch_rest(last)
    wait(wv.at[0, to_come, :], s_wv.at[0], "wv")
    ab = acc[...] + jnp.dot(xb[block(1), to_come], wv[0, to_come, :], preferred_element_type=f32)
    xb[block(0), pl.ds(last * CW, CW)] = act(ab)
    for s in range(4):
        src = x.at[:, pl.ds(col(quarter[s] * dk), dk)]
        pltpu.make_async_copy(src, xb.at[block(1), slot(s)], s_loc).start()
    wait(xb.at[block(0), early_cols], s_ld.at[0], "ld")
    part = rows // 2

    def early(i, _):
        k = i // 2
        r = i % 2
        p = 2 - k % 2

        @pl.when((r == 0) & (k + 1 < ns))
        def _():
            wait(db.at[0, k + 1], s_d1.at[k + 1], "d1")
            load_pair(0, k + 1, 3 - p)

        @pl.when(r == 0)
        def _():
            wait_pair(p)

        down(0, 1, k, p, r * part, part)
        ship_1(k, r * part, part)
        return 0

    lax.fori_loop(0, 2 * ns, early, 0)

    done = last - first
    load_chunk(done, 1)
    wait(xb.at[block(1), :], s_loc, "loc")
    gate(2, last, 0, q, False)
    gate(1, last, 0, 1 - q, False, 0)
    hcopy(2, last, q).wait()
    hcopy(0, last, 1 - q).wait()
    wait(xb.at[block(2), :], s_xs.at[2], "xs")
    load_h(2, 2)
    load_h(0, 1)

    def diagonal(j, _):
        i = j - done
        p = jnp.where(j == last, 0, 1 + i % 2)

        @pl.when(j + 1 < last)
        def _():
            load_chunk(j + 1, 2 - i % 2)

        @pl.when(j < last)
        def _():
            wait(wv.at[p], s_wv.at[p], "wv")

        gate(3, j, p, 2)
        return 0

    lax.fori_loop(done, nch, diagonal, 0)
    load_pair(0, 0, 1)
    hcopy(3, last, 2).wait()
    load_h(3, 3)
    for b in (1, 2, 3):
        wait_h(b)

    u, v = ns - 1, 2 * ns - 1
    over, under = pl.ds(0, turned), pl.ds(turned, rows - turned)

    def own_half(k, _):
        p = 1 + k % 2

        @pl.when(k + 1 < ns)
        def _():
            load_pair(0, k + 1, 3 - p)

        wait_pair(p)

        def rows_of(n, _):
            b = 3 - n
            down(b, jnp.where(b == 1, 0, b), k, p)

            @pl.when((n == 0) & (k + 1 < ns))
            def _():
                ship_d(k)

            @pl.when((n == 0) & (k + 1 == ns))
            def _():
                for m in range(2):
                    send(po.at[3, u, m, over, :], bxi.at[m], s_rs.at[2], s_bx.at[m], to_x)
                    send(po.at[3, u, m, under, :], rdi.at[u, m, under, :], s_rs.at[4], s_rd.at[2 * u + m], to_y)

            @pl.when((n == 1) & (k + 1 == ns))
            def _():
                for m in range(2):
                    send(po.at[2, u, m, over, :], yxi.at[v, m, over, :], s_rs.at[3], s_yx.at[2 * v + m], to_x)

            return 0

        lax.fori_loop(0, 3, rows_of, 0)
        return 0

    def fetch_pair(k, p):
        wait(db.at[1, k], s_d2.at[k], "d2")
        send(db.at[1, k], db.at[2, k], s_ws.at[5], s_d3.at[k], to_mate)
        wait(db.at[2, k], s_d3.at[k], "d3")
        load_pair(1, k, p)

    lax.fori_loop(0, ns, own_half, 0)

    def total(tiles):
        o = xb[block(tiles[0][0]), pl.ds(fq + tiles[0][1] * CW, CW)].astype(f32)
        for b, c in tiles[1:]:
            o = o + xb[block(b), pl.ds(fq + c * CW, CW)].astype(f32)
        return o.astype(bf16)

    def relay(half, k, m, turn):
        u = half * ns + k
        pltpu.make_async_copy(po.at[2, u, m], tile(0, 2), s_ld.at[0]).start()
        wait(rdi.at[u, m], s_rd.at[2 * u + m], "rd")
        pltpu.make_async_copy(rdi.at[u, m], tile(0, 3), s_ld.at[1]).start()
        ring = turn % 4

        @pl.when(turn >= 4)
        def _():
            wait(tile(ring, 4 + m), s_ys.at[2 * ring + m], "ys")

        wait(tile(0, 2), s_ld.at[0], "ld")
        wait(tile(0, 3), s_ld.at[1], "ld")
        xb[block(ring), pl.ds(fq + (4 + m) * CW, CW)] = total(((0, 2), (0, 3)))
        v = (1 - half) * ns + k
        send(tile(ring, 4 + m), yxi.at[v, m], s_ys.at[2 * ring + m], s_yx.at[2 * v + m], to_x)

    def other_half(k, _):
        p = k % 3
        u = ns + k
        wait_pair(p)

        def rows_of(n, _):
            b = jnp.where(n == 0, 3, jnp.where(n == 1, 0, jnp.where(n == 2, 2, 1)))
            out = jnp.where(n == 0, 3, jnp.where(n == 1, 1, jnp.where(n == 2, 2, 0)))
            down(b, out, u, p)

            @pl.when(n == 0)
            def _():
                ship_d(u)

            @pl.when((n == 1) & (k > 0))
            def _():
                ship_1(u - 1)

            @pl.when((n == 1) & (k + 1 < ns))
            def _():
                fetch_pair(k + 1, (k + 1) % 3)

            return 0

        lax.fori_loop(0, 4, rows_of, 0)

        @pl.when(k + 1 < ns)
        def _():
            for m in range(2):
                relay(0, k, m, k)

        return 0

    fetch_pair(0, 0)
    lax.fori_loop(0, ns, other_half, 0)

    def rows_in(b, start, size):
        return pl.ds(b * rows + start, size)

    for m in range(2):
        one = xb.at[rows_in(1, 0, turned), pl.ds(fq + 2 * CW, CW)]
        two = xb.at[rows_in(1, 0, turned), pl.ds(fq + 3 * CW, CW)]
        pltpu.make_async_copy(po.at[1, v, m, over, :], one, s_ld.at[0]).start()
        wait(bxi.at[m], s_bx.at[m], "bx")
        pltpu.make_async_copy(bxi.at[m], two, s_ld.at[1]).start()
        wait(one, s_ld.at[0], "ld")
        wait(two, s_ld.at[1], "ld")
        here = rows_in(2, 0, turned), pl.ds(fq + m * CW, CW)
        xb[here] = (one[...].astype(f32) + two[...].astype(f32)).astype(bf16)
        send(xb.at[here], r1i.at[v, m, over, :], s_yb.at[m], s_r1.at[2 * v + m], to_y)
        send(po.at[1, v, m, under, :], r1i.at[v, m, under, :], s_rs.at[5], s_r1.at[2 * v + m], to_y)

    for m in range(2):
        one = xb.at[rows_in(1, 0, rows - turned), pl.ds(fq + 2 * CW, CW)]
        two = xb.at[rows_in(1, 0, rows - turned), pl.ds(fq + 3 * CW, CW)]
        pltpu.make_async_copy(po.at[2, u, m, under, :], one, s_ld.at[0]).start()
        wait(rdi.at[u, m, under, :], s_rd.at[2 * u + m], "rd")
        pltpu.make_async_copy(rdi.at[u, m, under, :], two, s_ld.at[1]).start()
        wait(one, s_ld.at[0], "ld")
        wait(two, s_ld.at[1], "ld")
        here = rows_in(0, 0, rows - turned), pl.ds(fq + m * CW, CW)
        xb[here] = (one[...].astype(f32) + two[...].astype(f32)).astype(bf16)
        send(xb.at[here], yxi.at[v, m, under, :], s_xb.at[m], s_yx.at[2 * v + m], to_x)

    parts = ((1, 2), (1, 3), (2, 2), (2, 3))

    def finish(half, k, m, used):
        u = half * ns + k
        n = 2 * half + m
        cols = pl.ds(col(quarter[n] * dk + k * CW), CW)
        pltpu.make_async_copy(po.at[0, u, m], tile(*parts[0]), s_ld.at[0]).start()
        pltpu.make_async_copy(x.at[:, cols], tile(*parts[1]), s_ld.at[1]).start()
        wait(r1i.at[u, m], s_r1.at[2 * u + m], "r1")
        pltpu.make_async_copy(r1i.at[u, m], tile(*parts[2]), s_ld.at[2]).start()
        wait(yxi.at[u, m], s_yx.at[2 * u + m], "yx")
        pltpu.make_async_copy(yxi.at[u, m], tile(*parts[3]), s_ld.at[3]).start()
        for c in range(4):
            wait(tile(*parts[c]), s_ld.at[c], "ld")
        out = pltpu.make_async_copy(tile(3, n), y.at[:, cols], s_out.at[n])

        @pl.when(used)
        def _():
            out.wait()

        xb[block(3), pl.ds(fq + n * CW, CW)] = total(parts)
        out.start()

    def tail(k, _):
        @pl.when(k < ns)
        def _():
            for m in range(2):
                relay(1, k, m, ns - 1 + k)

        @pl.when(k > 0)
        def _():
            for half in (1, 0):
                finish(half, k - 1, 0, k > 1)

            @pl.when(k < ns)
            def _():
                for half in (1, 0):
                    finish(half, k - 1, 1, k > 1)

        return 0

    lax.fori_loop(0, ns + 1, tail, 0)

    for n in range(4):
        wait(tile(3, n), s_out.at[n], "out")
    for m in range(2):
        wait(xb.at[rows_in(2, 0, turned), pl.ds(fq + m * CW, CW)], s_yb.at[m], "yb")
        wait(xb.at[rows_in(0, 0, rows - turned), pl.ds(fq + m * CW, CW)], s_xb.at[m], "xb")
        for ring in range(4):
            wait(tile(ring, 4 + m), s_ys.at[2 * ring + m], "ys")
    wait(x, s_xs.at[0], "xs")
    wait(x, s_xs.at[1], "xs")
    wait(w1, s_ws.at[0], "ws")
    wait(w2, s_ws.at[1], "ws")
    wait(db.at[0], s_ws.at[2], "ws")
    wait(db.at[1], s_ws.at[3], "ws")
    wait(w3, s_ws.at[4], "ws")
    wait(db.at[2], s_ws.at[5], "ws")
    wait(rdi.at[pl.ds(0, 2 * ns - 1)], s_rs.at[0], "rs")
    wait(r1i.at[pl.ds(0, 2 * ns - 1)], s_rs.at[1], "rs")
    wait(bxi, s_rs.at[2], "rs")
    wait(bxi, s_rs.at[3], "rs")
    wait(rdi.at[u, :, under, :], s_rs.at[4], "rs")
    wait(r1i.at[v, :, under, :], s_rs.at[5], "rs")
    for w in (u, v):
        wait(r1i.at[w, 1], s_r1.at[2 * w + 1], "r1")
        wait(yxi.at[w, 1], s_yx.at[2 * w + 1], "yx")


def write(x, part, po, r1i, yxi, y, buf, strip, s_strip, s_in, s_out):
    dk = x.shape[1] // 4
    ns = dk // CW
    n, size = buf.shape[:2]
    d = lax.axis_index("dp")
    mate = d + 1 - 2 * (d % 2)
    cols = [pl.ds(pl.multiple_of(q * dk + (ns - 1) * CW, 128), CW) for q in (mate, (mate + 2) % 4)]
    loads = []
    for half in range(2):
        u = half * ns + ns - 1
        for i, src in enumerate((po.at[0, u, 1], x.at[:, cols[half]], r1i.at[u, 1], yxi.at[u, 1])):
            loads.append(pltpu.make_async_copy(src, strip.at[half, i], s_strip.at[4 * half + i]))
    rows = [pl.ds(i * size, size) for i in range(n)]
    ins = [pltpu.make_async_copy(part.at[rows[i], :], buf.at[i], s_in.at[i]) for i in range(n)]
    outs = [pltpu.make_async_copy(buf.at[i], y.at[rows[i], :], s_out.at[i]) for i in range(n)]
    for copy in loads + ins:
        copy.start()
    for copy in loads:
        copy.wait()
    for i in range(n):
        ins[i].wait()
        for half in range(2):
            o = strip[half, 0, rows[i], :].astype(jnp.float32)
            for c in range(1, 4):
                o = o + strip[half, c, rows[i], :].astype(jnp.float32)
            buf[i, :, cols[half]] = o.astype(buf.dtype)
        outs[i].start()
    for copy in outs:
        copy.wait()


def solution(mesh):
    def body(x, wg, wu, wd):
        rows, dim = x.shape
        dk = dim // 4
        fq = wg.shape[1] // 2
        nch = fq // CW
        ns = dk // CW
        bf16 = jnp.bfloat16
        dma = pltpu.SemaphoreType.DMA
        shapes = [
            (rows, dim),
            (nch, dk, 2 * CW), (nch, dk, 2 * CW), (nch, dk, 2 * CW),
            (3, ns, fq, CW),
            (4 * rows, fq),
            (4, 2 * ns, 2, rows, CW),
            (2 * ns, 2, rows, CW), (2 * ns, 2, rows, CW), (2 * ns, 2, rows, CW), (2, rows * 7 // 8, CW),
        ]
        outs = pl.pallas_call(
            kernel,
            out_shape=[jax.ShapeDtypeStruct(s, bf16) for s in shapes],
            in_specs=[pl.BlockSpec(memory_space=pl.ANY)] * 4,
            out_specs=[pl.BlockSpec(memory_space=pl.ANY)] * len(shapes),
            scratch_shapes=[
                pltpu.VMEM((4 * rows, dim), bf16),
                pltpu.VMEM((3, dim, 2 * CW), bf16),
                pltpu.VMEM((3, rows, CW), bf16),
                pltpu.VMEM((rows, 2 * CW), jnp.float32),
                dma, dma((3,)), dma((6,)), dma((4,)), dma((4,)), dma((4,)),
                dma((nch,)), dma((nch,)), dma((nch,)), dma((ns,)), dma((ns,)), dma((ns,)),
                dma((4,)), dma((3,)), dma, dma((6,)),
                dma((4 * ns,)), dma((4 * ns,)), dma((4 * ns,)), dma((2,)), dma((8,)), dma((2,)), dma((2,)), dma((4,)), dma((4,)),
            ],
            compiler_params=pltpu.CompilerParams(
                collective_id=0, has_side_effects=True, vmem_limit_bytes=67043328),
            cost_estimate=pl.CostEstimate(
                flops=6 * rows * 4 * dim * fq, bytes_accessed=4 * rows * dim * 2, transcendentals=0),
        )(x, wg, wu, wd)
        part, po, r1i, yxi = outs[0], outs[6], outs[8], outs[9]
        n = 8
        any_space = pl.BlockSpec(memory_space=pl.ANY)
        return pl.pallas_call(
            write,
            out_shape=jax.ShapeDtypeStruct((rows, dim), bf16),
            in_specs=[any_space] * 5,
            out_specs=any_space,
            scratch_shapes=[
                pltpu.VMEM((n, rows // n, dim), bf16),
                pltpu.VMEM((2, 4, rows, CW), bf16),
                dma((8,)), dma((n,)), dma((n,)),
            ],
            compiler_params=pltpu.CompilerParams(vmem_limit_bytes=67043328),
        )(x, part, po, r1i, yxi)

    return jax.shard_map(body, mesh=mesh, in_specs=(P(("dp", "tp"), None), P("dp", "tp"), P("dp", "tp"), P("tp", "dp")), out_specs=P(("dp", "tp"), None), check_vma=False)
```

```python
import functools

import jax
import jax.numpy as jnp
from jax import lax
from jax.experimental import pallas as pl
from jax.experimental.pallas import tpu as pltpu
from jax.sharding import PartitionSpec as P

CW = 256


def kernel(x, wg, wu, wd, y, w1, w2, w3, db, hb, po, rdi, r1i, yxi, bxi,
           xb, wv, hst, acc, s_loc, s_xs, s_ws, s_xx, s_xy, s_xd, s_w1, s_w2, s_w3, s_d1, s_d2, s_d3,
           s_wv, s_h, s_po, s_rs, s_rd, s_r1, s_yx, s_bx, s_ys, s_yb, s_xb, s_ld, s_out):
    rows, dim = x.shape
    dk = dim // 4
    fq = wg.shape[1] // 2
    nch = fq // CW
    first = nch // 2
    ns = dk // CW
    turned = rows * 13 // 16
    f32, bf16 = jnp.float32, jnp.bfloat16

    t = lax.axis_index("tp")
    d = lax.axis_index("dp")
    side = d // 2
    core = d % 2
    mate = d + 1 - 2 * core
    quarter = [d, mate, (d + 2) % 4, (mate + 2) % 4]
    to_mate = {"dp": mate}
    to_x = {"dp": (d + 2) % 4}
    to_y = {"tp": 1 - t}

    def col(v, size=128):
        return v if isinstance(v, int) else pl.multiple_of(v, size)

    def send(src, dst, send_sem, recv_sem, where):
        pltpu.make_async_remote_copy(
            src_ref=src, dst_ref=dst, send_sem=send_sem, recv_sem=recv_sem,
            device_id=where, device_id_type=pl.DeviceIdType.MESH).start()

    def wait(ref, sem, name="w"):
        with jax.named_scope(name):
            pltpu.make_async_copy(ref, ref, sem).wait()

    def block(b):
        return pl.ds(col(b * rows, rows), rows)

    def slot(s):
        return pl.ds(s * dk, dk)

    barrier = pltpu.get_barrier_semaphore()
    for where in (to_mate, to_x, to_y):
        pl.semaphore_signal(barrier, inc=1, device_id=where, device_id_type=pl.DeviceIdType.MESH)
    pl.semaphore_wait(barrier, 3)

    for s in range(4):
        src = x.at[:, pl.ds(col(quarter[s] * dk), dk)]
        send(src, xb.at[block(2), slot(s ^ 2)], s_xs.at[0], s_xx.at[s ^ 2], to_x)
        send(src, xb.at[block(1), slot(s)], s_xs.at[1], s_xy, to_y)
    for s in range(4):
        src = x.at[:, pl.ds(col(quarter[s] * dk), dk)]
        pltpu.make_async_copy(src, xb.at[block(0), slot(s)], s_loc).start()

    def send_chunk(j, _):
        for m, w in enumerate((wg, wu)):
            away = w.at[:, pl.ds(col((1 - side) * fq + j * CW), CW)]
            here = w.at[:, pl.ds(col(side * fq + j * CW), CW)]
            send(away, w2.at[j, :, pl.ds(m * CW, CW)], s_ws.at[1], s_w2.at[j], to_x)
            send(here, w1.at[j, :, pl.ds(m * CW, CW)], s_ws.at[0], s_w1, to_mate)
        return 0

    lax.fori_loop(0, nch, send_chunk, 0)

    def send_strip(k, _):
        cols = pl.ds(col(k * CW), CW)
        send(wd.at[pl.ds(col((1 - side) * fq), fq), cols], db.at[1, k], s_ws.at[3], s_d2.at[k], to_x)
        send(wd.at[pl.ds(col(side * fq), fq), cols], db.at[0, k], s_ws.at[2], s_d1, to_mate)
        return 0

    lax.fori_loop(0, ns, send_strip, 0)

    for s in (2, 3, 0, 1):
        piece = xb.at[block(2), slot(s)]
        wait(piece, s_xx.at[s], "xx")
        send(piece, xb.at[block(3), slot(s)], s_xs.at[2], s_xd, to_y)

    def load_here(j, p, sem):
        for m, w in enumerate((wg, wu)):
            here = w.at[:, pl.ds(col(side * fq + j * CW), CW)]
            pltpu.make_async_copy(here, wv.at[p, slot(0), pl.ds(m * CW, CW)], s_wv.at[sem]).start()

    def load_slot(w, j, n, p, sem):
        pltpu.make_async_copy(w.at[j], wv.at[p, slot(n)], s_wv.at[sem]).start()

    def load_chunk(j, p):
        load_here(j, p, p)
        for n, w in ((1, w1), (2, w2), (3, w3)):
            load_slot(w, j, n, p, p)

    def load_local(j):
        load_here(j, 0, 3)
        load_slot(w1, j, 1, 0, 3)

    def fetch_chunk(j, sem):
        wait(w2.at[j], s_w2.at[j], "w2")
        send(w2.at[j], w3.at[j], s_ws.at[4], s_w3.at[j], to_mate)
        load_slot(w2, j, 2, 0, 0)
        wait(w3.at[j], s_w3.at[j], "w3")
        load_slot(w3, j, 3, 0, sem)

    def hcopy(b, j, q):
        return pltpu.make_async_copy(hst.at[q], hb.at[block(b), pl.ds(col(j * CW), CW)], s_h.at[q])

    def gated(b, p):
        return act(jnp.dot(xb[block(b), :], wv[p], preferred_element_type=f32))

    def act(ab):
        a = ab[:, :CW]
        return (a * jax.nn.sigmoid(a) * ab[:, CW:]).astype(bf16)

    def gate(b, j, p, q, used=True, to=None):
        to = b if to is None else to

        @pl.when(used)
        def _():
            hcopy(to, j, q).wait()

        hst[q] = gated(b, p)
        hcopy(to, j, q).start()

    wait(xb.at[block(0), :], s_loc, "loc")
    wait(xb.at[block(1), :], s_xy, "xy")
    wait(w1, s_w1, "w1")
    at_hand, to_come = pl.ds(0, 2 * dk), pl.ds(2 * dk, 2 * dk)
    load_local(0)

    hcols = pl.ds(0, fq)

    def load_h(b, to):
        pltpu.make_async_copy(hb.at[block(b), :], xb.at[block(to), hcols], s_ld.at[to]).start()

    def wait_h(to):
        wait(xb.at[block(to), hcols], s_ld.at[to], "ld")

    def tile(b, c, n=1):
        return xb.at[block(b), pl.ds(fq + c * CW, n * CW)]

    def load_pair(half, k, p):
        left = pl.ds(0, CW)
        right = pl.ds(CW, CW)
        if half == 0:
            src = (wd.at[pl.ds(col(side * fq), fq), pl.ds(col(k * CW), CW)], db.at[0, k])
        else:
            src = (db.at[1, k], db.at[2, k])
        pltpu.make_async_copy(src[0], wv.at[p, hcols, left], s_wv.at[p]).start()
        pltpu.make_async_copy(src[1], wv.at[p, hcols, right], s_wv.at[p]).start()

    def wait_pair(p):
        wait(wv.at[p, hcols, :], s_wv.at[p], "wv")

    def down(b, out, u, p, start=0, size=rows):
        here = pl.ds(col(b * rows + start, size), size)
        there = pl.ds(col(start, size), size)
        o = jnp.dot(xb[here, hcols], wv[p, hcols, :], preferred_element_type=f32)
        xb[here, pl.ds(fq, 2 * CW)] = o.astype(bf16)
        for m in range(2):
            pltpu.make_async_copy(xb.at[here, pl.ds(fq + m * CW, CW)], po.at[out, u, m, there, :], s_po).start()
        wait(xb.at[here, pl.ds(fq, 2 * CW)], s_po, "po")

    def ship_d(u):
        for m in range(2):
            send(po.at[3, u, m], rdi.at[u, m], s_rs.at[0], s_rd.at[2 * u + m], to_y)

    def ship_1(u, start=0, size=rows):
        there = pl.ds(col(start, size), size)
        for m in range(2):
            send(po.at[1, u, m, there, :], r1i.at[u, m, there, :], s_rs.at[1], s_r1.at[2 * u + m], to_y)

    early_cols = pl.ds(0, (nch - 1) * CW)

    last = nch - 1

    def chunk(j, _):
        fetch_chunk(j, 0)

        @pl.when(j == first)
        def _():
            wait(xb.at[block(3), :], s_xd, "xd")

        @pl.when(j >= first)
        def _():
            load_chunk(j - first, 1)

        wait(wv.at[0, at_hand, :], s_wv.at[3], "wv")
        wait(wv.at[0, to_come, :], s_wv.at[0], "wv")

        def rows_of(n, _):
            g = 3 * j + n
            gate((n + 1) % 3, j, 0, g % 2, g >= 2)
            return 0

        lax.fori_loop(0, 3, rows_of, 0)
        load_local(j + 1)

        @pl.when(j + 1 == last)
        def _():
            for n in range(2):
                hcopy(0, 0, n).wait()
            pltpu.make_async_copy(hb.at[block(1), early_cols], xb.at[block(0), early_cols], s_ld.at[0]).start()
            wait(db.at[0], s_d1, "d1")
            load_pair(0, 0, 2)

        @pl.when(j >= first)
        def _():
            wait(wv.at[1], s_wv.at[1], "wv")
            gate(3, j - first, 1, 2, j > first)

        return 0

    lax.fori_loop(0, last, chunk, 0)

    q = (3 * last) % 2
    wait(wv.at[0, at_hand, :], s_wv.at[3], "wv")
    acc[...] = jnp.dot(xb[block(1), at_hand], wv[0, at_hand, :], preferred_element_type=f32)
    fetch_chunk(last, 3)
    wait(wv.at[0, slot(2), :], s_wv.at[0], "wv")
    acc[...] += jnp.dot(xb[block(1), slot(2)], wv[0, slot(2), :], preferred_element_type=f32)
    wait(wv.at[0, slot(3), :], s_wv.at[3], "wv")
    ab = acc[...] + jnp.dot(xb[block(1), slot(3)], wv[0, slot(3), :], preferred_element_type=f32)
    xb[block(0), pl.ds(last * CW, CW)] = act(ab)
    for s in range(4):
        src = x.at[:, pl.ds(col(quarter[s] * dk), dk)]
        pltpu.make_async_copy(src, xb.at[block(1), slot(s)], s_loc).start()
    wait(xb.at[block(0), early_cols], s_ld.at[0], "ld")
    part = rows // 2

    def early(i, _):
        k = i // 2
        r = i % 2
        p = 2 - k % 2

        @pl.when((r == 0) & (k + 1 < ns))
        def _():
            load_pair(0, k + 1, 3 - p)

        @pl.when(r == 0)
        def _():
            wait_pair(p)

        @pl.when(k == 0)
        def _():
            here = pl.ds(col(r * part, part), part)
            o = jnp.dot(xb[here, hcols], wv[p, hcols, :], preferred_element_type=f32)
            xb[here, pl.ds(fq + 4 * CW, 2 * CW)] = o.astype(bf16)
            for m in range(2):
                send(xb.at[here, pl.ds(fq + (4 + m) * CW, CW)], r1i.at[0, m, here, :], s_rs.at[6], s_r1.at[m], to_y)

        @pl.when(k > 0)
        def _():
            down(0, 1, k, p, r * part, part)
            ship_1(k, r * part, part)

        return 0

    lax.fori_loop(0, 2 * ns, early, 0)

    done = last - first
    load_chunk(done, 1)
    wait(xb.at[block(1), :], s_loc, "loc")
    gate(2, last, 0, q, False)
    gate(1, last, 0, 1 - q, False, 0)
    hcopy(2, last, q).wait()
    hcopy(0, last, 1 - q).wait()
    wait(xb.at[block(2), :], s_xs.at[2], "xs")
    load_h(2, 2)
    load_h(0, 1)

    def diagonal(j, _):
        i = j - done
        p = jnp.where(j == last, 0, 1 + i % 2)

        @pl.when(j + 1 < last)
        def _():
            load_chunk(j + 1, 2 - i % 2)

        @pl.when(j < last)
        def _():
            wait(wv.at[p], s_wv.at[p], "wv")

        gate(3, j, p, 2)
        return 0

    lax.fori_loop(done, nch, diagonal, 0)
    load_pair(0, 0, 1)
    hcopy(3, last, 2).wait()
    load_h(3, 3)
    for b in (1, 2, 3):
        wait_h(b)

    u, v = ns - 1, 2 * ns - 1
    over, under = pl.ds(0, turned), pl.ds(turned, rows - turned)

    def own_half(k, _):
        p = 1 + k % 2

        @pl.when(k + 1 < ns)
        def _():
            load_pair(0, k + 1, 3 - p)

        wait_pair(p)

        def rows_of(n, _):
            b = 3 - n
            down(b, jnp.where(b == 1, 0, b), k, p)

            @pl.when((n == 0) & (k + 1 < ns))
            def _():
                ship_d(k)

            @pl.when((n == 0) & (k + 1 == ns))
            def _():
                for m in range(2):
                    send(po.at[3, u, m, over, :], bxi.at[m], s_rs.at[2], s_bx.at[m], to_x)
                    send(po.at[3, u, m, under, :], rdi.at[u, m, under, :], s_rs.at[4], s_rd.at[2 * u + m], to_y)

            @pl.when((n == 1) & (k + 1 == ns))
            def _():
                for m in range(2):
                    send(po.at[2, u, m, over, :], yxi.at[v, m, over, :], s_rs.at[3], s_yx.at[2 * v + m], to_x)

            return 0

        lax.fori_loop(0, 3, rows_of, 0)
        return 0

    def fetch_pair(k, p):
        wait(db.at[1, k], s_d2.at[k], "d2")
        send(db.at[1, k], db.at[2, k], s_ws.at[5], s_d3.at[k], to_mate)
        wait(db.at[2, k], s_d3.at[k], "d3")
        load_pair(1, k, p)

    lax.fori_loop(0, ns, own_half, 0)

    def total(tiles):
        o = xb[block(tiles[0][0]), pl.ds(fq + tiles[0][1] * CW, CW)].astype(f32)
        for b, c in tiles[1:]:
            o = o + xb[block(b), pl.ds(fq + c * CW, CW)].astype(f32)
        return o.astype(bf16)

    def relay(half, k, m, turn):
        u = half * ns + k
        pltpu.make_async_copy(po.at[2, u, m], tile(0, 2), s_ld.at[0]).start()
        wait(rdi.at[u, m], s_rd.at[2 * u + m], "rd")
        pltpu.make_async_copy(rdi.at[u, m], tile(0, 3), s_ld.at[1]).start()
        ring = turn % 4

        @pl.when(turn >= 4)
        def _():
            wait(tile(ring, 4 + m), s_ys.at[2 * ring + m], "ys")

        wait(tile(0, 2), s_ld.at[0], "ld")
        wait(tile(0, 3), s_ld.at[1], "ld")
        xb[block(ring), pl.ds(fq + (4 + m) * CW, CW)] = total(((0, 2), (0, 3)))
        v = (1 - half) * ns + k
        send(tile(ring, 4 + m), yxi.at[v, m], s_ys.at[2 * ring + m], s_yx.at[2 * v + m], to_x)

    def other_half(k, _):
        p = k % 3
        u = ns + k
        wait_pair(p)

        def rows_of(n, _):
            b = jnp.where(n == 0, 3, jnp.where(n == 1, 0, jnp.where(n == 2, 2, 1)))
            out = jnp.where(n == 0, 3, jnp.where(n == 1, 1, jnp.where(n == 2, 2, 0)))
            down(b, out, u, p)

            @pl.when(n == 0)
            def _():
                ship_d(u)

            @pl.when((n == 1) & (k > 0))
            def _():
                ship_1(u - 1)

            @pl.when((n == 1) & (k + 1 < ns))
            def _():
                fetch_pair(k + 1, (k + 1) % 3)

            return 0

        lax.fori_loop(0, 4, rows_of, 0)

        @pl.when(k + 1 < ns)
        def _():
            for m in range(2):
                relay(0, k, m, k)

        return 0

    fetch_pair(0, 0)
    wait(tile(0, 4, 2), s_rs.at[6], "rs")
    lax.fori_loop(0, ns, other_half, 0)

    def rows_in(b, start, size):
        return pl.ds(b * rows + start, size)

    for m in range(2):
        one = xb.at[rows_in(1, 0, turned), pl.ds(fq + 2 * CW, CW)]
        two = xb.at[rows_in(1, 0, turned), pl.ds(fq + 3 * CW, CW)]
        pltpu.make_async_copy(po.at[1, v, m, over, :], one, s_ld.at[0]).start()
        wait(bxi.at[m], s_bx.at[m], "bx")
        pltpu.make_async_copy(bxi.at[m], two, s_ld.at[1]).start()
        wait(one, s_ld.at[0], "ld")
        wait(two, s_ld.at[1], "ld")
        here = rows_in(2, 0, turned), pl.ds(fq + m * CW, CW)
        xb[here] = (one[...].astype(f32) + two[...].astype(f32)).astype(bf16)
        send(xb.at[here], r1i.at[v, m, over, :], s_yb.at[m], s_r1.at[2 * v + m], to_y)
        send(po.at[1, v, m, under, :], r1i.at[v, m, under, :], s_rs.at[5], s_r1.at[2 * v + m], to_y)

    for m in range(2):
        one = xb.at[rows_in(1, 0, rows - turned), pl.ds(fq + 2 * CW, CW)]
        two = xb.at[rows_in(1, 0, rows - turned), pl.ds(fq + 3 * CW, CW)]
        pltpu.make_async_copy(po.at[2, u, m, under, :], one, s_ld.at[0]).start()
        wait(rdi.at[u, m, under, :], s_rd.at[2 * u + m], "rd")
        pltpu.make_async_copy(rdi.at[u, m, under, :], two, s_ld.at[1]).start()
        wait(one, s_ld.at[0], "ld")
        wait(two, s_ld.at[1], "ld")
        here = rows_in(0, 0, rows - turned), pl.ds(fq + m * CW, CW)
        xb[here] = (one[...].astype(f32) + two[...].astype(f32)).astype(bf16)
        send(xb.at[here], yxi.at[v, m, under, :], s_xb.at[m], s_yx.at[2 * v + m], to_x)

    parts = ((1, 2), (1, 3), (2, 2), (2, 3))

    def finish(half, k, m, used):
        u = half * ns + k
        n = 2 * half + m
        cols = pl.ds(col(quarter[n] * dk + k * CW), CW)
        pltpu.make_async_copy(po.at[0, u, m], tile(*parts[0]), s_ld.at[0]).start()
        pltpu.make_async_copy(x.at[:, cols], tile(*parts[1]), s_ld.at[1]).start()
        wait(r1i.at[u, m], s_r1.at[2 * u + m], "r1")
        pltpu.make_async_copy(r1i.at[u, m], tile(*parts[2]), s_ld.at[2]).start()
        wait(yxi.at[u, m], s_yx.at[2 * u + m], "yx")
        pltpu.make_async_copy(yxi.at[u, m], tile(*parts[3]), s_ld.at[3]).start()
        for c in range(4):
            wait(tile(*parts[c]), s_ld.at[c], "ld")
        out = pltpu.make_async_copy(tile(3, n), y.at[:, cols], s_out.at[n])

        @pl.when(used)
        def _():
            out.wait()

        xb[block(3), pl.ds(fq + n * CW, CW)] = total(parts)
        out.start()

    def begin(half):
        w = half * ns + ns - 1
        n = 2 * half + 1
        src, sem = ((r1i, s_r1), (yxi, s_yx))[half]
        cols = pl.ds(col(quarter[n] * dk + (ns - 1) * CW), CW)
        pltpu.make_async_copy(po.at[0, w, 1], tile(*parts[0]), s_ld.at[0]).start()
        wait(src.at[w, 1], sem.at[2 * w + 1])
        pltpu.make_async_copy(src.at[w, 1], tile(*parts[1]), s_ld.at[1]).start()
        wait(tile(*parts[0]), s_ld.at[0], "ld")
        wait(tile(*parts[1]), s_ld.at[1], "ld")
        out = pltpu.make_async_copy(tile(3, n), y.at[:, cols], s_out.at[n])
        out.wait()
        xb[block(3), pl.ds(fq + n * CW, CW)] = total(parts[:2])
        out.start()

    def tail(k, _):
        @pl.when(k < ns)
        def _():
            for m in range(2):
                relay(1, k, m, ns - 1 + k)

        @pl.when(k > 0)
        def _():
            for half in (1, 0):
                finish(half, k - 1, 0, k > 1)

            @pl.when(k < ns)
            def _():
                for half in (1, 0):
                    finish(half, k - 1, 1, k > 1)

            @pl.when(k == ns)
            def _():
                for half in (1, 0):
                    begin(half)

        return 0

    lax.fori_loop(0, ns + 1, tail, 0)

    for n in range(4):
        wait(tile(3, n), s_out.at[n], "out")
    for m in range(2):
        wait(xb.at[rows_in(2, 0, turned), pl.ds(fq + m * CW, CW)], s_yb.at[m], "yb")
        wait(xb.at[rows_in(0, 0, rows - turned), pl.ds(fq + m * CW, CW)], s_xb.at[m], "xb")
        for ring in range(4):
            wait(tile(ring, 4 + m), s_ys.at[2 * ring + m], "ys")
    wait(x, s_xs.at[0], "xs")
    wait(x, s_xs.at[1], "xs")
    wait(w1, s_ws.at[0], "ws")
    wait(w2, s_ws.at[1], "ws")
    wait(db.at[0], s_ws.at[2], "ws")
    wait(db.at[1], s_ws.at[3], "ws")
    wait(w3, s_ws.at[4], "ws")
    wait(db.at[2], s_ws.at[5], "ws")
    wait(rdi.at[pl.ds(0, 2 * ns - 1)], s_rs.at[0], "rs")
    wait(r1i.at[pl.ds(0, 2 * ns - 2)], s_rs.at[1], "rs")
    wait(bxi, s_rs.at[2], "rs")
    wait(bxi, s_rs.at[3], "rs")
    wait(rdi.at[u, :, under, :], s_rs.at[4], "rs")
    wait(r1i.at[v, :, under, :], s_rs.at[5], "rs")
    wait(r1i.at[v, 1], s_r1.at[2 * v + 1], "r1")
    wait(yxi.at[u, 1], s_yx.at[2 * u + 1], "yx")


def write(x, part, r1i, yxi, y, buf, strip, s_strip, s_in, s_out):
    dk = x.shape[1] // 4
    ns = dk // CW
    n, size = buf.shape[:2]
    d = lax.axis_index("dp")
    mate = d + 1 - 2 * (d % 2)
    cols = [pl.ds(pl.multiple_of(q * dk + (ns - 1) * CW, 128), CW) for q in (mate, (mate + 2) % 4)]
    loads = []
    for half, late in enumerate((yxi.at[ns - 1, 1], r1i.at[2 * ns - 1, 1])):
        for i, src in enumerate((x.at[:, cols[half]], late)):
            loads.append(pltpu.make_async_copy(src, strip.at[half, i], s_strip.at[2 * half + i]))
    rows = [pl.ds(i * size, size) for i in range(n)]
    ins = [pltpu.make_async_copy(part.at[rows[i], :], buf.at[i], s_in.at[i]) for i in range(n)]
    outs = [pltpu.make_async_copy(buf.at[i], y.at[rows[i], :], s_out.at[i]) for i in range(n)]
    for copy in loads + ins:
        copy.start()
    for copy in loads:
        copy.wait()
    for i in range(n):
        ins[i].wait()
        for half in range(2):
            o = buf[i, :, cols[half]].astype(jnp.float32) + strip[half, 1, rows[i], :].astype(jnp.float32)
            o = o + strip[half, 0, rows[i], :].astype(jnp.float32)
            buf[i, :, cols[half]] = o.astype(buf.dtype)
        outs[i].start()
    for copy in outs:
        copy.wait()


def solution(mesh):
    def body(x, wg, wu, wd):
        rows, dim = x.shape
        dk = dim // 4
        fq = wg.shape[1] // 2
        nch = fq // CW
        ns = dk // CW
        bf16 = jnp.bfloat16
        dma = pltpu.SemaphoreType.DMA
        shapes = [
            (rows, dim),
            (nch, dk, 2 * CW), (nch, dk, 2 * CW), (nch, dk, 2 * CW),
            (3, ns, fq, CW),
            (4 * rows, fq),
            (4, 2 * ns, 2, rows, CW),
            (2 * ns, 2, rows, CW), (2 * ns, 2, rows, CW), (2 * ns, 2, rows, CW), (2, rows * 13 // 16, CW),
        ]
        outs = pl.pallas_call(
            kernel,
            out_shape=[jax.ShapeDtypeStruct(s, bf16) for s in shapes],
            in_specs=[pl.BlockSpec(memory_space=pl.ANY)] * 4,
            out_specs=[pl.BlockSpec(memory_space=pl.ANY)] * len(shapes),
            scratch_shapes=[
                pltpu.VMEM((4 * rows, dim), bf16),
                pltpu.VMEM((3, dim, 2 * CW), bf16),
                pltpu.VMEM((3, rows, CW), bf16),
                pltpu.VMEM((rows, 2 * CW), jnp.float32),
                dma, dma((3,)), dma((6,)), dma((4,)), dma, dma,
                dma, dma((nch,)), dma((nch,)), dma, dma((ns,)), dma((ns,)),
                dma((4,)), dma((3,)), dma, dma((7,)),
                dma((4 * ns,)), dma((4 * ns,)), dma((4 * ns,)), dma((2,)), dma((8,)), dma((2,)), dma((2,)), dma((4,)), dma((4,)),
            ],
            compiler_params=pltpu.CompilerParams(
                collective_id=0, has_side_effects=True, vmem_limit_bytes=67043328),
            cost_estimate=pl.CostEstimate(
                flops=6 * rows * 4 * dim * fq, bytes_accessed=4 * rows * dim * 2, transcendentals=0),
        )(x, wg, wu, wd)
        part, r1i, yxi = outs[0], outs[8], outs[9]
        n = 8
        any_space = pl.BlockSpec(memory_space=pl.ANY)
        return pl.pallas_call(
            write,
            out_shape=jax.ShapeDtypeStruct((rows, dim), bf16),
            in_specs=[any_space] * 4,
            out_specs=any_space,
            scratch_shapes=[
                pltpu.VMEM((n, rows // n, dim), bf16),
                pltpu.VMEM((2, 2, rows, CW), bf16),
                dma((4,)), dma((n,)), dma((n,)),
            ],
            compiler_params=pltpu.CompilerParams(vmem_limit_bytes=67043328),
        )(x, part, r1i, yxi)

    return jax.shard_map(body, mesh=mesh, in_specs=(P(("dp", "tp"), None), P("dp", "tp"), P("dp", "tp"), P("tp", "dp")), out_specs=P(("dp", "tp"), None), check_vma=False)
```

```python
import functools

import jax
import jax.numpy as jnp
from jax import lax
from jax.experimental import pallas as pl
from jax.experimental.pallas import tpu as pltpu
from jax.sharding import PartitionSpec as P

CW = 256


def kernel(x, wg, wu, wd, y, w1, w2, w3, db, hb, po, rdi, r1i, yxi, bxi,
           xb, wv, hst, acc, s_loc, s_xs, s_ws, s_xx, s_xy, s_xd, s_w1, s_w2, s_w3, s_d1, s_d2, s_d3,
           s_wv, s_h, s_po, s_pr, s_rs, s_rd, s_r1, s_yx, s_bx, s_ys, s_yb, s_xb, s_ld, s_out):
    rows, dim = x.shape
    dk = dim // 4
    fq = wg.shape[1] // 2
    nch = fq // CW
    first = nch // 2
    ns = dk // CW
    turned = rows * 49 // 64
    f32, bf16 = jnp.float32, jnp.bfloat16

    t = lax.axis_index("tp")
    d = lax.axis_index("dp")
    side = d // 2
    core = d % 2
    mate = d + 1 - 2 * core
    quarter = [d, mate, (d + 2) % 4, (mate + 2) % 4]
    to_mate = {"dp": mate}
    to_x = {"dp": (d + 2) % 4}
    to_y = {"tp": 1 - t}

    def col(v, size=128):
        return v if isinstance(v, int) else pl.multiple_of(v, size)

    def send(src, dst, send_sem, recv_sem, where):
        pltpu.make_async_remote_copy(
            src_ref=src, dst_ref=dst, send_sem=send_sem, recv_sem=recv_sem,
            device_id=where, device_id_type=pl.DeviceIdType.MESH).start()

    def wait(ref, sem, name="w"):
        with jax.named_scope(name):
            pltpu.make_async_copy(ref, ref, sem).wait()

    def block(b):
        return pl.ds(col(b * rows, rows), rows)

    def slot(s):
        return pl.ds(s * dk, dk)

    barrier = pltpu.get_barrier_semaphore()
    for where in (to_mate, to_x, to_y):
        pl.semaphore_signal(barrier, inc=1, device_id=where, device_id_type=pl.DeviceIdType.MESH)
    pl.semaphore_wait(barrier, 3)

    for s in range(4):
        src = x.at[:, pl.ds(col(quarter[s] * dk), dk)]
        send(src, xb.at[block(2), slot(s ^ 2)], s_xs.at[0], s_xx.at[s ^ 2], to_x)
        send(src, xb.at[block(1), slot(s)], s_xs.at[1], s_xy, to_y)
    for s in range(4):
        src = x.at[:, pl.ds(col(quarter[s] * dk), dk)]
        pltpu.make_async_copy(src, xb.at[block(0), slot(s)], s_loc).start()

    def send_chunk(j, _):
        for m, w in enumerate((wg, wu)):
            away = w.at[:, pl.ds(col((1 - side) * fq + j * CW), CW)]
            here = w.at[:, pl.ds(col(side * fq + j * CW), CW)]
            send(away, w2.at[j, :, pl.ds(m * CW, CW)], s_ws.at[1], s_w2.at[j], to_x)
            send(here, w1.at[j, :, pl.ds(m * CW, CW)], s_ws.at[0], s_w1, to_mate)
        return 0

    lax.fori_loop(0, nch, send_chunk, 0)

    def send_strip(k, _):
        cols = pl.ds(col(k * CW), CW)
        send(wd.at[pl.ds(col((1 - side) * fq), fq), cols], db.at[1, k], s_ws.at[3], s_d2.at[k], to_x)
        send(wd.at[pl.ds(col(side * fq), fq), cols], db.at[0, k], s_ws.at[2], s_d1, to_mate)
        return 0

    lax.fori_loop(0, ns, send_strip, 0)

    for s in (2, 3, 0, 1):
        piece = xb.at[block(2), slot(s)]
        wait(piece, s_xx.at[s], "xx")
        send(piece, xb.at[block(3), slot(s)], s_xs.at[2], s_xd, to_y)

    def load_here(j, p, sem):
        for m, w in enumerate((wg, wu)):
            here = w.at[:, pl.ds(col(side * fq + j * CW), CW)]
            pltpu.make_async_copy(here, wv.at[p, slot(0), pl.ds(m * CW, CW)], s_wv.at[sem]).start()

    def load_slot(w, j, n, p, sem):
        pltpu.make_async_copy(w.at[j], wv.at[p, slot(n)], s_wv.at[sem]).start()

    def load_chunk(j, p):
        load_here(j, p, p)
        for n, w in ((1, w1), (2, w2), (3, w3)):
            load_slot(w, j, n, p, p)

    def load_local(j):
        load_here(j, 0, 3)
        load_slot(w1, j, 1, 0, 3)

    def fetch_chunk(j, sem):
        wait(w2.at[j], s_w2.at[j], "w2")
        send(w2.at[j], w3.at[j], s_ws.at[4], s_w3.at[j], to_mate)
        load_slot(w2, j, 2, 0, 0)
        wait(w3.at[j], s_w3.at[j], "w3")
        load_slot(w3, j, 3, 0, sem)

    def hcopy(b, j, q):
        return pltpu.make_async_copy(hst.at[q], hb.at[block(b), pl.ds(col(j * CW), CW)], s_h.at[q])

    def gated(b, p):
        return act(jnp.dot(xb[block(b), :], wv[p], preferred_element_type=f32))

    def act(ab):
        a = ab[:, :CW]
        return (a * jax.nn.sigmoid(a) * ab[:, CW:]).astype(bf16)

    def gate(b, j, p, q, used=True, to=None):
        to = b if to is None else to

        @pl.when(used)
        def _():
            hcopy(to, j, q).wait()

        hst[q] = gated(b, p)
        hcopy(to, j, q).start()

    wait(xb.at[block(0), :], s_loc, "loc")
    wait(xb.at[block(1), :], s_xy, "xy")
    wait(w1, s_w1, "w1")
    at_hand, to_come = pl.ds(0, 2 * dk), pl.ds(2 * dk, 2 * dk)
    load_local(0)

    hcols = pl.ds(0, fq)

    def load_h(b, to):
        pltpu.make_async_copy(hb.at[block(b), :], xb.at[block(to), hcols], s_ld.at[to]).start()

    def wait_h(to):
        wait(xb.at[block(to), hcols], s_ld.at[to], "ld")

    def tile(b, c, n=1):
        return xb.at[block(b), pl.ds(fq + c * CW, n * CW)]

    def load_pair(half, k, p):
        left = pl.ds(0, CW)
        right = pl.ds(CW, CW)
        if half == 0:
            src = (wd.at[pl.ds(col(side * fq), fq), pl.ds(col(k * CW), CW)], db.at[0, k])
        else:
            src = (db.at[1, k], db.at[2, k])
        pltpu.make_async_copy(src[0], wv.at[p, hcols, left], s_wv.at[p]).start()
        pltpu.make_async_copy(src[1], wv.at[p, hcols, right], s_wv.at[p]).start()

    def wait_pair(p):
        wait(wv.at[p, hcols, :], s_wv.at[p], "wv")

    def down(b, out, u, p):
        o = jnp.dot(xb[block(b), hcols], wv[p, hcols, :], preferred_element_type=f32)
        xb[block(b), pl.ds(fq, 2 * CW)] = o.astype(bf16)
        for m in range(2):
            pltpu.make_async_copy(tile(b, m), po.at[out, u, m], s_po).start()
        wait(tile(b, 0, 2), s_po, "po")

    def ship_d(u):
        for m in range(2):
            send(po.at[3, u, m], rdi.at[u, m], s_rs.at[0], s_rd.at[2 * u + m], to_y)

    def ship_1(u):
        for m in range(2):
            send(po.at[1, u, m], r1i.at[u, m], s_rs.at[1], s_r1.at[2 * u + m], to_y)

    early_cols = pl.ds(0, (nch - 1) * CW)

    last = nch - 1

    def chunk(j, _):
        fetch_chunk(j, 0)

        @pl.when(j == first)
        def _():
            wait(xb.at[block(3), :], s_xd, "xd")

        spare = (j >= first) & (j + 1 < last)

        @pl.when(spare)
        def _():
            load_chunk(j - first, 1)

        wait(wv.at[0, at_hand, :], s_wv.at[3], "wv")
        wait(wv.at[0, to_come, :], s_wv.at[0], "wv")

        def rows_of(n, _):
            g = 3 * j + n
            gate((n + 1) % 3, j, 0, g % 2, g >= 2)
            return 0

        lax.fori_loop(0, 3, rows_of, 0)
        load_local(j + 1)

        @pl.when(j + 1 == last)
        def _():
            for n in range(2):
                hcopy(0, 0, n).wait()
            pltpu.make_async_copy(hb.at[block(1), early_cols], xb.at[block(0), early_cols], s_ld.at[0]).start()
            wait(db.at[0], s_d1, "d1")
            load_pair(0, 0, 2)

        @pl.when(spare)
        def _():
            wait(wv.at[1], s_wv.at[1], "wv")
            gate(3, j - first, 1, 2, j > first)

        return 0

    lax.fori_loop(0, last, chunk, 0)

    q = (3 * last) % 2
    wait(wv.at[0, at_hand, :], s_wv.at[3], "wv")
    acc[...] = jnp.dot(xb[block(1), at_hand], wv[0, at_hand, :], preferred_element_type=f32)
    fetch_chunk(last, 3)
    wait(wv.at[0, slot(2), :], s_wv.at[0], "wv")
    acc[...] += jnp.dot(xb[block(1), slot(2)], wv[0, slot(2), :], preferred_element_type=f32)
    wait(wv.at[0, slot(3), :], s_wv.at[3], "wv")
    ab = acc[...] + jnp.dot(xb[block(1), slot(3)], wv[0, slot(3), :], preferred_element_type=f32)
    xb[block(0), pl.ds(last * CW, CW)] = act(ab)
    for s in range(4):
        src = x.at[:, pl.ds(col(quarter[s] * dk), dk)]
        pltpu.make_async_copy(src, xb.at[block(1), slot(s)], s_loc).start()
    wait(xb.at[block(0), early_cols], s_ld.at[0], "ld")
    wait_pair(2)
    quart = rows // 4

    def first_pair(i, _):
        here = pl.ds(col(i * quart, quart), quart)
        o = jnp.dot(xb[here, hcols], wv[2, hcols, :], preferred_element_type=f32)
        xb[here, pl.ds(fq + 4 * CW, 2 * CW)] = o.astype(bf16)
        for m in range(2):
            send(xb.at[here, pl.ds(fq + (4 + m) * CW, CW)], r1i.at[0, m, here, :], s_rs.at[6], s_r1.at[m], to_y)
        return 0

    load_pair(0, 1, 1)
    lax.fori_loop(0, 4, first_pair, 0)

    def early(i, _):
        k = i // 2
        r = i % 2
        p = 2 - k % 2
        part = rows // 2

        def place_of(i):
            return i // 2, pl.ds(col((i % 2) * part, part), part)

        def done_with(i):
            k, there = place_of(i)
            wait(xb.at[there, pl.ds(fq, 2 * CW)], s_pr.at[i % 2], "pr")
            for m in range(2):
                send(po.at[1, k, m, there, :], r1i.at[k, m, there, :], s_rs.at[1], s_r1.at[2 * k + m], to_y)

        @pl.when((r == 0) & (k + 1 < ns))
        def _():
            load_pair(0, k + 1, 3 - p)

        @pl.when(r == 0)
        def _():
            wait_pair(p)

        here = place_of(i)[1]
        o = jnp.dot(xb[here, hcols], wv[p, hcols, :], preferred_element_type=f32)

        @pl.when(i > 2)
        def _():
            done_with(i - 1)

        xb[here, pl.ds(fq, 2 * CW)] = o.astype(bf16)
        for m in range(2):
            pltpu.make_async_copy(xb.at[here, pl.ds(fq + m * CW, CW)], po.at[1, k, m, here, :], s_pr.at[r]).start()

        @pl.when(i + 1 == 2 * ns)
        def _():
            done_with(i)

        return 0

    lax.fori_loop(2, 2 * ns, early, 0)

    done = last - 1 - first
    load_chunk(done, 1)
    wait(xb.at[block(1), :], s_loc, "loc")
    gate(2, last, 0, q, False)
    gate(1, last, 0, 1 - q, False, 0)
    hcopy(2, last, q).wait()
    hcopy(0, last, 1 - q).wait()
    wait(xb.at[block(2), :], s_xs.at[2], "xs")
    load_h(2, 2)
    load_h(0, 1)

    def diagonal(j, _):
        i = j - done
        p = jnp.where(j == last, 0, 1 + i % 2)

        @pl.when(j + 1 < last)
        def _():
            load_chunk(j + 1, 2 - i % 2)

        @pl.when(j < last)
        def _():
            wait(wv.at[p], s_wv.at[p], "wv")

        gate(3, j, p, 2)
        return 0

    lax.fori_loop(done, nch, diagonal, 0)
    load_pair(0, 0, 1)
    hcopy(3, last, 2).wait()
    load_h(3, 3)
    for b in (1, 2, 3):
        wait_h(b)

    u, v = ns - 1, 2 * ns - 1
    over, under = pl.ds(0, turned), pl.ds(turned, rows - turned)

    def own_half(k, _):
        p = 1 + k % 2

        @pl.when(k + 1 < ns)
        def _():
            load_pair(0, k + 1, 3 - p)

        wait_pair(p)

        def rows_of(n, _):
            b = 3 - n
            down(b, jnp.where(b == 1, 0, b), k, p)

            @pl.when((n == 0) & (k + 1 < ns))
            def _():
                ship_d(k)

            @pl.when((n == 0) & (k + 1 == ns))
            def _():
                for m in range(2):
                    send(po.at[3, u, m, over, :], bxi.at[m], s_rs.at[2], s_bx.at[m], to_x)
                    send(po.at[3, u, m, under, :], rdi.at[u, m, under, :], s_rs.at[4], s_rd.at[2 * u + m], to_y)

            @pl.when((n == 1) & (k + 1 == ns))
            def _():
                for m in range(2):
                    send(po.at[2, u, m, over, :], yxi.at[v, m, over, :], s_rs.at[3], s_yx.at[2 * v + m], to_x)

            return 0

        lax.fori_loop(0, 3, rows_of, 0)
        return 0

    def fetch_pair(k, p):
        wait(db.at[1, k], s_d2.at[k], "d2")
        send(db.at[1, k], db.at[2, k], s_ws.at[5], s_d3.at[k], to_mate)
        wait(db.at[2, k], s_d3.at[k], "d3")
        load_pair(1, k, p)

    lax.fori_loop(0, ns, own_half, 0)

    def total(tiles):
        o = xb[block(tiles[0][0]), pl.ds(fq + tiles[0][1] * CW, CW)].astype(f32)
        for b, c in tiles[1:]:
            o = o + xb[block(b), pl.ds(fq + c * CW, CW)].astype(f32)
        return o.astype(bf16)

    def relay(half, k, m, turn):
        u = half * ns + k
        pltpu.make_async_copy(po.at[2, u, m], tile(0, 2), s_ld.at[0]).start()
        wait(rdi.at[u, m], s_rd.at[2 * u + m], "rd")
        pltpu.make_async_copy(rdi.at[u, m], tile(0, 3), s_ld.at[1]).start()
        ring = turn % 4

        @pl.when(turn >= 4)
        def _():
            wait(tile(ring, 4 + m), s_ys.at[2 * ring + m], "ys")

        wait(tile(0, 2), s_ld.at[0], "ld")
        wait(tile(0, 3), s_ld.at[1], "ld")
        xb[block(ring), pl.ds(fq + (4 + m) * CW, CW)] = total(((0, 2), (0, 3)))
        v = (1 - half) * ns + k
        send(tile(ring, 4 + m), yxi.at[v, m], s_ys.at[2 * ring + m], s_yx.at[2 * v + m], to_x)

    def other_half(k, _):
        p = k % 3
        u = ns + k
        wait_pair(p)

        def rows_of(n, _):
            b = jnp.where(n == 0, 3, jnp.where(n == 1, 0, jnp.where(n == 2, 2, 1)))
            out = jnp.where(n == 0, 3, jnp.where(n == 1, 1, jnp.where(n == 2, 2, 0)))
            down(b, out, u, p)

            @pl.when(n == 0)
            def _():
                ship_d(u)

            @pl.when((n == 1) & (k > 0))
            def _():
                ship_1(u - 1)

            @pl.when((n == 1) & (k + 1 < ns))
            def _():
                fetch_pair(k + 1, (k + 1) % 3)

            return 0

        lax.fori_loop(0, 4, rows_of, 0)

        @pl.when(k + 1 < ns)
        def _():
            for m in range(2):
                relay(0, k, m, k)

        return 0

    fetch_pair(0, 0)
    wait(tile(0, 4, 2), s_rs.at[6], "rs")
    lax.fori_loop(0, ns, other_half, 0)

    def rows_in(b, start, size):
        return pl.ds(b * rows + start, size)

    for m in range(2):
        one = xb.at[rows_in(1, 0, turned), pl.ds(fq + 2 * CW, CW)]
        two = xb.at[rows_in(1, 0, turned), pl.ds(fq + 3 * CW, CW)]
        pltpu.make_async_copy(po.at[1, v, m, over, :], one, s_ld.at[0]).start()
        wait(bxi.at[m], s_bx.at[m], "bx")
        pltpu.make_async_copy(bxi.at[m], two, s_ld.at[1]).start()
        wait(one, s_ld.at[0], "ld")
        wait(two, s_ld.at[1], "ld")
        here = rows_in(2, 0, turned), pl.ds(fq + m * CW, CW)
        xb[here] = (one[...].astype(f32) + two[...].astype(f32)).astype(bf16)
        send(xb.at[here], r1i.at[v, m, over, :], s_yb.at[m], s_r1.at[2 * v + m], to_y)
        send(po.at[1, v, m, under, :], r1i.at[v, m, under, :], s_rs.at[5], s_r1.at[2 * v + m], to_y)

    for m in range(2):
        one = xb.at[rows_in(1, 0, rows - turned), pl.ds(fq + 2 * CW, CW)]
        two = xb.at[rows_in(1, 0, rows - turned), pl.ds(fq + 3 * CW, CW)]
        pltpu.make_async_copy(po.at[2, u, m, under, :], one, s_ld.at[0]).start()
        wait(rdi.at[u, m, under, :], s_rd.at[2 * u + m], "rd")
        pltpu.make_async_copy(rdi.at[u, m, under, :], two, s_ld.at[1]).start()
        wait(one, s_ld.at[0], "ld")
        wait(two, s_ld.at[1], "ld")
        here = rows_in(0, 0, rows - turned), pl.ds(fq + m * CW, CW)
        xb[here] = (one[...].astype(f32) + two[...].astype(f32)).astype(bf16)
        send(xb.at[here], yxi.at[v, m, under, :], s_xb.at[m], s_yx.at[2 * v + m], to_x)

    parts = ((1, 2), (1, 3), (2, 2), (2, 3))

    def finish(half, k, m, used):
        u = half * ns + k
        n = 2 * half + m
        cols = pl.ds(col(quarter[n] * dk + k * CW), CW)
        pltpu.make_async_copy(po.at[0, u, m], tile(*parts[0]), s_ld.at[0]).start()
        pltpu.make_async_copy(x.at[:, cols], tile(*parts[1]), s_ld.at[1]).start()
        wait(r1i.at[u, m], s_r1.at[2 * u + m], "r1")
        pltpu.make_async_copy(r1i.at[u, m], tile(*parts[2]), s_ld.at[2]).start()
        wait(yxi.at[u, m], s_yx.at[2 * u + m], "yx")
        pltpu.make_async_copy(yxi.at[u, m], tile(*parts[3]), s_ld.at[3]).start()
        for c in range(4):
            wait(tile(*parts[c]), s_ld.at[c], "ld")
        out = pltpu.make_async_copy(tile(3, n), y.at[:, cols], s_out.at[n])

        @pl.when(used)
        def _():
            out.wait()

        xb[block(3), pl.ds(fq + n * CW, CW)] = total(parts)
        out.start()

    def begin(half):
        w = half * ns + ns - 1
        n = 2 * half + 1
        src, sem = ((r1i, s_r1), (yxi, s_yx))[half]
        cols = pl.ds(col(quarter[n] * dk + (ns - 1) * CW), CW)
        pltpu.make_async_copy(po.at[0, w, 1], tile(*parts[0]), s_ld.at[0]).start()
        wait(src.at[w, 1], sem.at[2 * w + 1])
        pltpu.make_async_copy(src.at[w, 1], tile(*parts[1]), s_ld.at[1]).start()
        wait(tile(*parts[0]), s_ld.at[0], "ld")
        wait(tile(*parts[1]), s_ld.at[1], "ld")
        out = pltpu.make_async_copy(tile(3, n), y.at[:, cols], s_out.at[n])
        out.wait()
        xb[block(3), pl.ds(fq + n * CW, CW)] = total(parts[:2])
        out.start()

    def tail(k, _):
        @pl.when(k < ns)
        def _():
            for m in range(2):
                relay(1, k, m, ns - 1 + k)

        @pl.when(k > 0)
        def _():
            for half in (1, 0):
                finish(half, k - 1, 0, k > 1)

            @pl.when(k < ns)
            def _():
                for half in (1, 0):
                    finish(half, k - 1, 1, k > 1)

            @pl.when(k == ns)
            def _():
                for half in (1, 0):
                    begin(half)

        return 0

    lax.fori_loop(0, ns + 1, tail, 0)

    for n in range(4):
        wait(tile(3, n), s_out.at[n], "out")
    for m in range(2):
        wait(xb.at[rows_in(2, 0, turned), pl.ds(fq + m * CW, CW)], s_yb.at[m], "yb")
        wait(xb.at[rows_in(0, 0, rows - turned), pl.ds(fq + m * CW, CW)], s_xb.at[m], "xb")
        for ring in range(4):
            wait(tile(ring, 4 + m), s_ys.at[2 * ring + m], "ys")
    wait(x, s_xs.at[0], "xs")
    wait(x, s_xs.at[1], "xs")
    wait(w1, s_ws.at[0], "ws")
    wait(w2, s_ws.at[1], "ws")
    wait(db.at[0], s_ws.at[2], "ws")
    wait(db.at[1], s_ws.at[3], "ws")
    wait(w3, s_ws.at[4], "ws")
    wait(db.at[2], s_ws.at[5], "ws")
    wait(rdi.at[pl.ds(0, 2 * ns - 1)], s_rs.at[0], "rs")
    wait(r1i.at[pl.ds(0, 2 * ns - 2)], s_rs.at[1], "rs")
    wait(bxi, s_rs.at[2], "rs")
    wait(bxi, s_rs.at[3], "rs")
    wait(rdi.at[u, :, under, :], s_rs.at[4], "rs")
    wait(r1i.at[v, :, under, :], s_rs.at[5], "rs")
    wait(r1i.at[v, 1], s_r1.at[2 * v + 1], "r1")
    wait(yxi.at[u, 1], s_yx.at[2 * u + 1], "yx")


def write(x, part, r1i, yxi, y, buf, strip, s_strip, s_in, s_out):
    dk = x.shape[1] // 4
    ns = dk // CW
    n, size = buf.shape[:2]
    d = lax.axis_index("dp")
    mate = d + 1 - 2 * (d % 2)
    cols = [pl.ds(pl.multiple_of(q * dk + (ns - 1) * CW, 128), CW) for q in (mate, (mate + 2) % 4)]
    loads = []
    for half, late in enumerate((yxi.at[ns - 1, 1], r1i.at[2 * ns - 1, 1])):
        for i, src in enumerate((x.at[:, cols[half]], late)):
            loads.append(pltpu.make_async_copy(src, strip.at[half, i], s_strip.at[2 * half + i]))
    rows = [pl.ds(i * size, size) for i in range(n)]
    ins = [pltpu.make_async_copy(part.at[rows[i], :], buf.at[i], s_in.at[i]) for i in range(n)]
    outs = [pltpu.make_async_copy(buf.at[i], y.at[rows[i], :], s_out.at[i]) for i in range(n)]
    for copy in loads + ins:
        copy.start()
    for copy in loads:
        copy.wait()
    for i in range(n):
        ins[i].wait()
        for half in range(2):
            o = buf[i, :, cols[half]].astype(jnp.float32) + strip[half, 1, rows[i], :].astype(jnp.float32)
            o = o + strip[half, 0, rows[i], :].astype(jnp.float32)
            buf[i, :, cols[half]] = o.astype(buf.dtype)
        outs[i].start()
    for copy in outs:
        copy.wait()


def solution(mesh):
    def body(x, wg, wu, wd):
        rows, dim = x.shape
        dk = dim // 4
        fq = wg.shape[1] // 2
        nch = fq // CW
        ns = dk // CW
        bf16 = jnp.bfloat16
        dma = pltpu.SemaphoreType.DMA
        shapes = [
            (rows, dim),
            (nch, dk, 2 * CW), (nch, dk, 2 * CW), (nch, dk, 2 * CW),
            (3, ns, fq, CW),
            (4 * rows, fq),
            (4, 2 * ns, 2, rows, CW),
            (2 * ns, 2, rows, CW), (2 * ns, 2, rows, CW), (2 * ns, 2, rows, CW), (2, rows * 49 // 64, CW),
        ]
        outs = pl.pallas_call(
            kernel,
            out_shape=[jax.ShapeDtypeStruct(s, bf16) for s in shapes],
            in_specs=[pl.BlockSpec(memory_space=pl.ANY)] * 4,
            out_specs=[pl.BlockSpec(memory_space=pl.ANY)] * len(shapes),
            scratch_shapes=[
                pltpu.VMEM((4 * rows, dim), bf16),
                pltpu.VMEM((3, dim, 2 * CW), bf16),
                pltpu.VMEM((3, rows, CW), bf16),
                pltpu.VMEM((rows, 2 * CW), jnp.float32),
                dma, dma((3,)), dma((6,)), dma((4,)), dma, dma,
                dma, dma((nch,)), dma((nch,)), dma, dma((ns,)), dma((ns,)),
                dma((4,)), dma((3,)), dma, dma((2,)), dma((7,)),
                dma((4 * ns,)), dma((4 * ns,)), dma((4 * ns,)), dma((2,)), dma((8,)), dma((2,)), dma((2,)), dma((4,)), dma((4,)),
            ],
            compiler_params=pltpu.CompilerParams(
                collective_id=0, has_side_effects=True, vmem_limit_bytes=67043328),
            cost_estimate=pl.CostEstimate(
                flops=6 * rows * 4 * dim * fq, bytes_accessed=4 * rows * dim * 2, transcendentals=0),
        )(x, wg, wu, wd)
        part, r1i, yxi = outs[0], outs[8], outs[9]
        n = 8
        any_space = pl.BlockSpec(memory_space=pl.ANY)
        return pl.pallas_call(
            write,
            out_shape=jax.ShapeDtypeStruct((rows, dim), bf16),
            in_specs=[any_space] * 4,
            out_specs=any_space,
            scratch_shapes=[
                pltpu.VMEM((n, rows // n, dim), bf16),
                pltpu.VMEM((2, 2, rows, CW), bf16),
                dma((4,)), dma((n,)), dma((n,)),
            ],
            compiler_params=pltpu.CompilerParams(vmem_limit_bytes=67043328),
        )(x, part, r1i, yxi)

    return jax.shard_map(body, mesh=mesh, in_specs=(P(("dp", "tp"), None), P("dp", "tp"), P("dp", "tp"), P("tp", "dp")), out_specs=P(("dp", "tp"), None), check_vma=False)
```

```python
import functools

import jax
import jax.numpy as jnp
from jax import lax
from jax.experimental import pallas as pl
from jax.experimental.pallas import tpu as pltpu
from jax.sharding import PartitionSpec as P

CW = 256


def kernel(x, wg, wu, wd, y, w1, w2, w3, db, hb, po, rdi, r1i, yxi, bxi,
           xb, wv, hst, acc, s_loc, s_xs, s_ws, s_xx, s_xy, s_xd, s_w1, s_w2, s_w3, s_d1, s_d2, s_d3,
           s_wv, s_h, s_po, s_pr, s_rs, s_rd, s_r1, s_yx, s_bx, s_ys, s_yb, s_xb, s_ld, s_out):
    rows, dim = x.shape
    dk = dim // 4
    fq = wg.shape[1] // 2
    nch = fq // CW
    first = nch // 2
    ns = dk // CW
    turned = rows * 3 // 4
    f32, bf16 = jnp.float32, jnp.bfloat16

    t = lax.axis_index("tp")
    d = lax.axis_index("dp")
    side = d // 2
    core = d % 2
    mate = d + 1 - 2 * core
    quarter = [d, mate, (d + 2) % 4, (mate + 2) % 4]
    to_mate = {"dp": mate}
    to_x = {"dp": (d + 2) % 4}
    to_y = {"tp": 1 - t}

    def col(v, size=128):
        return v if isinstance(v, int) else pl.multiple_of(v, size)

    def send(src, dst, send_sem, recv_sem, where):
        pltpu.make_async_remote_copy(
            src_ref=src, dst_ref=dst, send_sem=send_sem, recv_sem=recv_sem,
            device_id=where, device_id_type=pl.DeviceIdType.MESH).start()

    def wait(ref, sem, name="w"):
        with jax.named_scope(name):
            pltpu.make_async_copy(ref, ref, sem).wait()

    def block(b):
        return pl.ds(col(b * rows, rows), rows)

    def slot(s):
        return pl.ds(s * dk, dk)

    barrier = pltpu.get_barrier_semaphore()
    for where in (to_mate, to_x, to_y):
        pl.semaphore_signal(barrier, inc=1, device_id=where, device_id_type=pl.DeviceIdType.MESH)
    pl.semaphore_wait(barrier, 3)

    for s in range(4):
        src = x.at[:, pl.ds(col(quarter[s] * dk), dk)]
        send(src, xb.at[block(2), slot(s ^ 2)], s_xs.at[0], s_xx.at[s ^ 2], to_x)
        send(src, xb.at[block(1), slot(s)], s_xs.at[1], s_xy, to_y)
    for s in range(4):
        src = x.at[:, pl.ds(col(quarter[s] * dk), dk)]
        pltpu.make_async_copy(src, xb.at[block(0), slot(s)], s_loc).start()

    def send_chunk(j, _):
        for m, w in enumerate((wg, wu)):
            away = w.at[:, pl.ds(col((1 - side) * fq + j * CW), CW)]
            here = w.at[:, pl.ds(col(side * fq + j * CW), CW)]
            send(away, w2.at[j, :, pl.ds(m * CW, CW)], s_ws.at[1], s_w2.at[j], to_x)
            send(here, w1.at[j, :, pl.ds(m * CW, CW)], s_ws.at[0], s_w1, to_mate)
        return 0

    lax.fori_loop(0, nch, send_chunk, 0)

    def send_strip(k, _):
        cols = pl.ds(col(k * CW), CW)
        send(wd.at[pl.ds(col((1 - side) * fq), fq), cols], db.at[1, k], s_ws.at[3], s_d2.at[k], to_x)
        send(wd.at[pl.ds(col(side * fq), fq), cols], db.at[0, k], s_ws.at[2], s_d1, to_mate)
        return 0

    lax.fori_loop(0, ns, send_strip, 0)

    for s in (2, 3, 0, 1):
        piece = xb.at[block(2), slot(s)]
        wait(piece, s_xx.at[s], "xx")
        send(piece, xb.at[block(3), slot(s)], s_xs.at[2], s_xd, to_y)

    def load_here(j, p, sem):
        for m, w in enumerate((wg, wu)):
            here = w.at[:, pl.ds(col(side * fq + j * CW), CW)]
            pltpu.make_async_copy(here, wv.at[p, slot(0), pl.ds(m * CW, CW)], s_wv.at[sem]).start()

    def load_slot(w, j, n, p, sem):
        pltpu.make_async_copy(w.at[j], wv.at[p, slot(n)], s_wv.at[sem]).start()

    def load_chunk(j, p):
        load_here(j, p, p)
        for n, w in ((1, w1), (2, w2), (3, w3)):
            load_slot(w, j, n, p, p)

    def load_local(j):
        load_here(j, 0, 3)
        load_slot(w1, j, 1, 0, 3)

    def fetch_chunk(j, sem):
        wait(w2.at[j], s_w2.at[j], "w2")
        send(w2.at[j], w3.at[j], s_ws.at[4], s_w3.at[j], to_mate)
        load_slot(w2, j, 2, 0, 0)
        wait(w3.at[j], s_w3.at[j], "w3")
        load_slot(w3, j, 3, 0, sem)

    def hcopy(b, j, q):
        return pltpu.make_async_copy(hst.at[q], hb.at[block(b), pl.ds(col(j * CW), CW)], s_h.at[q])

    def gated(b, p):
        return act(jnp.dot(xb[block(b), :], wv[p], preferred_element_type=f32))

    def act(ab):
        a = ab[:, :CW]
        return (a * jax.nn.sigmoid(a) * ab[:, CW:]).astype(bf16)

    def gate(b, j, p, q, used=True, to=None):
        to = b if to is None else to

        @pl.when(used)
        def _():
            hcopy(to, j, q).wait()

        hst[q] = gated(b, p)
        hcopy(to, j, q).start()

    wait(xb.at[block(0), :], s_loc, "loc")
    wait(xb.at[block(1), :], s_xy, "xy")
    wait(w1, s_w1, "w1")
    at_hand, to_come = pl.ds(0, 2 * dk), pl.ds(2 * dk, 2 * dk)
    load_local(0)

    hcols = pl.ds(0, fq)

    def load_h(b, to):
        pltpu.make_async_copy(hb.at[block(b), :], xb.at[block(to), hcols], s_ld.at[to]).start()

    def wait_h(to):
        wait(xb.at[block(to), hcols], s_ld.at[to], "ld")

    def tile(b, c, n=1):
        return xb.at[block(b), pl.ds(fq + c * CW, n * CW)]

    def load_pair(half, k, p):
        left = pl.ds(0, CW)
        right = pl.ds(CW, CW)
        if half == 0:
            src = (wd.at[pl.ds(col(side * fq), fq), pl.ds(col(k * CW), CW)], db.at[0, k])
        else:
            src = (db.at[1, k], db.at[2, k])
        pltpu.make_async_copy(src[0], wv.at[p, hcols, left], s_wv.at[p]).start()
        pltpu.make_async_copy(src[1], wv.at[p, hcols, right], s_wv.at[p]).start()

    def wait_pair(p):
        wait(wv.at[p, hcols, :], s_wv.at[p], "wv")

    def down(b, out, u, p):
        o = jnp.dot(xb[block(b), hcols], wv[p, hcols, :], preferred_element_type=f32)
        xb[block(b), pl.ds(fq, 2 * CW)] = o.astype(bf16)
        for m in range(2):
            pltpu.make_async_copy(tile(b, m), po.at[out, u, m], s_po).start()
        wait(tile(b, 0, 2), s_po, "po")

    def ship_d(u):
        for m in range(2):
            send(po.at[3, u, m], rdi.at[u, m], s_rs.at[0], s_rd.at[u], to_y)

    def ship_1(u):
        for m in range(2):
            send(po.at[1, u, m], r1i.at[u, m], s_rs.at[1], s_r1.at[u], to_y)

    early_cols = pl.ds(0, (nch - 1) * CW)

    last = nch - 1

    def chunk(j, _):
        fetch_chunk(j, 0)

        @pl.when(j == first)
        def _():
            wait(xb.at[block(3), :], s_xd, "xd")

        spare = (j >= first) & (j + 1 < last)

        @pl.when(spare)
        def _():
            load_chunk(j - first, 1)

        wait(wv.at[0, at_hand, :], s_wv.at[3], "wv")
        wait(wv.at[0, to_come, :], s_wv.at[0], "wv")

        def rows_of(n, _):
            g = 3 * j + n
            gate((n + 1) % 3, j, 0, g % 2, g >= 2)
            return 0

        lax.fori_loop(0, 3, rows_of, 0)
        load_local(j + 1)

        @pl.when(j + 1 == last)
        def _():
            for n in range(2):
                hcopy(0, 0, n).wait()
            pltpu.make_async_copy(hb.at[block(1), early_cols], xb.at[block(0), early_cols], s_ld.at[0]).start()
            wait(db.at[0], s_d1, "d1")
            load_pair(0, 0, 2)

        @pl.when(spare)
        def _():
            wait(wv.at[1], s_wv.at[1], "wv")
            gate(3, j - first, 1, 2, j > first)

        return 0

    lax.fori_loop(0, last, chunk, 0)

    q = (3 * last) % 2
    wait(wv.at[0, at_hand, :], s_wv.at[3], "wv")
    acc[...] = jnp.dot(xb[block(1), at_hand], wv[0, at_hand, :], preferred_element_type=f32)
    fetch_chunk(last, 3)
    wait(wv.at[0, slot(2), :], s_wv.at[0], "wv")
    quart = rows // 4

    def first_pair(i, _):
        here = pl.ds(col(i * quart, quart), quart)
        there = pl.ds(col(rows + i * quart, quart), quart)
        ab = acc[here, :] + jnp.dot(xb[there, slot(2)], wv[0, slot(2), :], preferred_element_type=f32)

        @pl.when(i == 0)
        def _():
            wait(wv.at[0, slot(3), :], s_wv.at[3], "wv")
            wait(xb.at[block(0), early_cols], s_ld.at[0], "ld")
            wait_pair(2)

        ab = ab + jnp.dot(xb[there, slot(3)], wv[0, slot(3), :], preferred_element_type=f32)
        xb[here, pl.ds(last * CW, CW)] = act(ab)
        o = jnp.dot(xb[here, hcols], wv[2, hcols, :], preferred_element_type=f32)
        xb[here, pl.ds(fq + 4 * CW, 2 * CW)] = o.astype(bf16)
        for m in range(2):
            send(xb.at[here, pl.ds(fq + (4 + m) * CW, CW)], r1i.at[0, m, here, :], s_rs.at[6], s_r1.at[0], to_y)
        return 0

    lax.fori_loop(0, 4, first_pair, 0)
    load_pair(0, 1, 1)
    for s in range(4):
        src = x.at[:, pl.ds(col(quarter[s] * dk), dk)]
        pltpu.make_async_copy(src, xb.at[block(1), slot(s)], s_loc).start()

    def early(i, _):
        k = i // 2
        r = i % 2
        p = 2 - k % 2
        part = rows // 2

        def place_of(i):
            return i // 2, pl.ds(col((i % 2) * part, part), part)

        def done_with(i):
            k, there = place_of(i)
            wait(xb.at[there, pl.ds(fq, 2 * CW)], s_pr.at[i % 2], "pr")
            for m in range(2):
                send(po.at[1, k, m, there, :], r1i.at[k, m, there, :], s_rs.at[1], s_r1.at[k], to_y)

        @pl.when((r == 0) & (k + 1 < ns))
        def _():
            load_pair(0, k + 1, 3 - p)

        @pl.when(r == 0)
        def _():
            wait_pair(p)

        here = place_of(i)[1]
        o = jnp.dot(xb[here, hcols], wv[p, hcols, :], preferred_element_type=f32)

        @pl.when(i > 2)
        def _():
            done_with(i - 1)

        xb[here, pl.ds(fq, 2 * CW)] = o.astype(bf16)
        for m in range(2):
            pltpu.make_async_copy(xb.at[here, pl.ds(fq + m * CW, CW)], po.at[1, k, m, here, :], s_pr.at[r]).start()

        @pl.when(i + 1 == 2 * ns)
        def _():
            done_with(i)

        return 0

    lax.fori_loop(2, 2 * ns, early, 0)

    done = last - 1 - first
    load_chunk(done, 1)
    wait(xb.at[block(1), :], s_loc, "loc")
    gate(2, last, 0, q, False)
    gate(1, last, 0, 1 - q, False, 0)
    hcopy(2, last, q).wait()
    hcopy(0, last, 1 - q).wait()
    wait(xb.at[block(2), :], s_xs.at[2], "xs")
    load_h(2, 2)
    load_h(0, 1)

    def diagonal(j, _):
        i = j - done
        p = jnp.where(j == last, 0, 1 + i % 2)

        @pl.when(j + 1 < last)
        def _():
            load_chunk(j + 1, 2 - i % 2)

        @pl.when(j < last)
        def _():
            wait(wv.at[p], s_wv.at[p], "wv")

        gate(3, j, p, 2)
        return 0

    lax.fori_loop(done, nch, diagonal, 0)
    load_pair(0, 0, 1)
    hcopy(3, last, 2).wait()
    load_h(3, 3)
    for b in (1, 2, 3):
        wait_h(b)

    u, v = ns - 1, 2 * ns - 1
    over, under = pl.ds(0, turned), pl.ds(turned, rows - turned)

    def own_half(k, _):
        p = 1 + k % 2

        @pl.when(k + 1 < ns)
        def _():
            load_pair(0, k + 1, 3 - p)

        wait_pair(p)

        def rows_of(n, _):
            b = 3 - n
            down(b, jnp.where(b == 1, 0, b), k, p)

            @pl.when((n == 0) & (k + 1 < ns))
            def _():
                ship_d(k)

            @pl.when((n == 0) & (k + 1 == ns))
            def _():
                for m in range(2):
                    send(po.at[3, u, m, over, :], bxi.at[m], s_rs.at[2], s_bx.at[m], to_x)
                    send(po.at[3, u, m, under, :], rdi.at[u, m, under, :], s_rs.at[4], s_rd.at[u], to_y)

            @pl.when((n == 1) & (k + 1 == ns))
            def _():
                for m in range(2):
                    send(po.at[2, u, m, over, :], yxi.at[v, m, over, :], s_rs.at[3], s_yx.at[v], to_x)

            return 0

        lax.fori_loop(0, 3, rows_of, 0)
        return 0

    def fetch_pair(k, p):
        wait(db.at[1, k], s_d2.at[k], "d2")
        send(db.at[1, k], db.at[2, k], s_ws.at[5], s_d3.at[k], to_mate)
        wait(db.at[2, k], s_d3.at[k], "d3")
        load_pair(1, k, p)

    lax.fori_loop(0, ns, own_half, 0)

    def total(tiles):
        o = xb[block(tiles[0][0]), pl.ds(fq + tiles[0][1] * CW, CW)].astype(f32)
        for b, c in tiles[1:]:
            o = o + xb[block(b), pl.ds(fq + c * CW, CW)].astype(f32)
        return o.astype(bf16)

    def relay(half, k, m, turn):
        u = half * ns + k
        pltpu.make_async_copy(po.at[2, u, m], tile(0, 2), s_ld.at[0]).start()
        if m == 0:
            wait(rdi.at[u], s_rd.at[u], "rd")
        pltpu.make_async_copy(rdi.at[u, m], tile(0, 3), s_ld.at[1]).start()
        ring = turn % 4

        @pl.when(turn >= 4)
        def _():
            wait(tile(ring, 4 + m), s_ys.at[2 * ring + m], "ys")

        wait(tile(0, 2), s_ld.at[0], "ld")
        wait(tile(0, 3), s_ld.at[1], "ld")
        xb[block(ring), pl.ds(fq + (4 + m) * CW, CW)] = total(((0, 2), (0, 3)))
        v = (1 - half) * ns + k
        sem = v if m == 0 else jnp.where(v == ns - 1, 2 * ns, v)
        send(tile(ring, 4 + m), yxi.at[v, m], s_ys.at[2 * ring + m], s_yx.at[sem], to_x)

    def other_half(k, _):
        p = k % 3
        u = ns + k
        wait_pair(p)

        def rows_of(n, _):
            b = jnp.where(n == 0, 3, jnp.where(n == 1, 0, jnp.where(n == 2, 2, 1)))
            out = jnp.where(n == 0, 3, jnp.where(n == 1, 1, jnp.where(n == 2, 2, 0)))
            down(b, out, u, p)

            @pl.when(n == 0)
            def _():
                ship_d(u)

            @pl.when((n == 1) & (k > 0))
            def _():
                ship_1(u - 1)

            @pl.when((n == 1) & (k + 1 < ns))
            def _():
                fetch_pair(k + 1, (k + 1) % 3)

            return 0

        lax.fori_loop(0, 4, rows_of, 0)

        @pl.when(k + 1 < ns)
        def _():
            for m in range(2):
                relay(0, k, m, k)

        return 0

    fetch_pair(0, 0)
    wait(tile(0, 4, 2), s_rs.at[6], "rs")
    lax.fori_loop(0, ns, other_half, 0)

    def rows_in(b, start, size):
        return pl.ds(b * rows + start, size)

    for m in range(2):
        one = xb.at[rows_in(1, 0, turned), pl.ds(fq + 2 * CW, CW)]
        two = xb.at[rows_in(1, 0, turned), pl.ds(fq + 3 * CW, CW)]
        pltpu.make_async_copy(po.at[1, v, m, over, :], one, s_ld.at[0]).start()
        wait(bxi.at[m], s_bx.at[m], "bx")
        pltpu.make_async_copy(bxi.at[m], two, s_ld.at[1]).start()
        wait(one, s_ld.at[0], "ld")
        wait(two, s_ld.at[1], "ld")
        here = rows_in(2, 0, turned), pl.ds(fq + m * CW, CW)
        xb[here] = (one[...].astype(f32) + two[...].astype(f32)).astype(bf16)
        send(xb.at[here], r1i.at[v, m, over, :], s_yb.at[m], s_r1.at[v + m], to_y)
        send(po.at[1, v, m, under, :], r1i.at[v, m, under, :], s_rs.at[5], s_r1.at[v + m], to_y)

    for m in range(2):
        one = xb.at[rows_in(1, 0, rows - turned), pl.ds(fq + 2 * CW, CW)]
        two = xb.at[rows_in(1, 0, rows - turned), pl.ds(fq + 3 * CW, CW)]
        pltpu.make_async_copy(po.at[2, u, m, under, :], one, s_ld.at[0]).start()
        if m == 0:
            wait(rdi.at[u, :, under, :], s_rd.at[u], "rd")
        pltpu.make_async_copy(rdi.at[u, m, under, :], two, s_ld.at[1]).start()
        wait(one, s_ld.at[0], "ld")
        wait(two, s_ld.at[1], "ld")
        here = rows_in(0, 0, rows - turned), pl.ds(fq + m * CW, CW)
        xb[here] = (one[...].astype(f32) + two[...].astype(f32)).astype(bf16)
        send(xb.at[here], yxi.at[v, m, under, :], s_xb.at[m], s_yx.at[v], to_x)

    parts = ((1, 2), (1, 3), (2, 2), (2, 3))

    def pair_here(ref, sem, u, apart, k):
        if not apart:
            wait(ref.at[u], sem.at[u])
            return

        @pl.when(k + 1 < ns)
        def _():
            wait(ref.at[u], sem.at[u])

        @pl.when(k + 1 == ns)
        def _():
            wait(ref.at[u, 0], sem.at[u])

    def finish(half, k, m, used):
        u = half * ns + k
        n = 2 * half + m
        cols = pl.ds(col(quarter[n] * dk + k * CW), CW)
        pltpu.make_async_copy(po.at[0, u, m], tile(*parts[0]), s_ld.at[0]).start()
        pltpu.make_async_copy(x.at[:, cols], tile(*parts[1]), s_ld.at[1]).start()
        if m == 0:
            pair_here(r1i, s_r1, u, half == 1, k)
        pltpu.make_async_copy(r1i.at[u, m], tile(*parts[2]), s_ld.at[2]).start()
        if m == 0:
            pair_here(yxi, s_yx, u, half == 0, k)
        pltpu.make_async_copy(yxi.at[u, m], tile(*parts[3]), s_ld.at[3]).start()
        for c in range(4):
            wait(tile(*parts[c]), s_ld.at[c], "ld")
        out = pltpu.make_async_copy(tile(3, n), y.at[:, cols], s_out.at[n])

        @pl.when(used)
        def _():
            out.wait()

        xb[block(3), pl.ds(fq + n * CW, CW)] = total(parts)
        out.start()

    def begin(half):
        w = half * ns + ns - 1
        n = 2 * half + 1
        src = (r1i, yxi)[half]
        cols = pl.ds(col(quarter[n] * dk + (ns - 1) * CW), CW)
        pltpu.make_async_copy(po.at[0, w, 1], tile(*parts[0]), s_ld.at[0]).start()
        pltpu.make_async_copy(src.at[w, 1], tile(*parts[1]), s_ld.at[1]).start()
        wait(tile(*parts[0]), s_ld.at[0], "ld")
        wait(tile(*parts[1]), s_ld.at[1], "ld")
        out = pltpu.make_async_copy(tile(3, n), y.at[:, cols], s_out.at[n])
        out.wait()
        xb[block(3), pl.ds(fq + n * CW, CW)] = total(parts[:2])
        out.start()

    def tail(k, _):
        @pl.when(k < ns)
        def _():
            for m in range(2):
                relay(1, k, m, ns - 1 + k)

        @pl.when(k > 0)
        def _():
            for half in (1, 0):
                finish(half, k - 1, 0, k > 1)

            @pl.when(k < ns)
            def _():
                for half in (1, 0):
                    finish(half, k - 1, 1, k > 1)

            @pl.when(k == ns)
            def _():
                for half in (1, 0):
                    begin(half)

        return 0

    lax.fori_loop(0, ns + 1, tail, 0)

    for n in range(4):
        wait(tile(3, n), s_out.at[n], "out")
    for m in range(2):
        wait(xb.at[rows_in(2, 0, turned), pl.ds(fq + m * CW, CW)], s_yb.at[m], "yb")
        wait(xb.at[rows_in(0, 0, rows - turned), pl.ds(fq + m * CW, CW)], s_xb.at[m], "xb")
        for ring in range(4):
            wait(tile(ring, 4 + m), s_ys.at[2 * ring + m], "ys")
    wait(x, s_xs.at[0], "xs")
    wait(x, s_xs.at[1], "xs")
    wait(w1, s_ws.at[0], "ws")
    wait(w2, s_ws.at[1], "ws")
    wait(db.at[0], s_ws.at[2], "ws")
    wait(db.at[1], s_ws.at[3], "ws")
    wait(w3, s_ws.at[4], "ws")
    wait(db.at[2], s_ws.at[5], "ws")
    wait(rdi.at[pl.ds(0, 2 * ns - 1)], s_rs.at[0], "rs")
    wait(r1i.at[pl.ds(0, 2 * ns - 2)], s_rs.at[1], "rs")
    wait(bxi, s_rs.at[2], "rs")
    wait(bxi, s_rs.at[3], "rs")
    wait(rdi.at[u, :, under, :], s_rs.at[4], "rs")
    wait(r1i.at[v, :, under, :], s_rs.at[5], "rs")
    wait(r1i.at[v, 1], s_r1.at[v + 1], "r1")
    wait(yxi.at[u, 1], s_yx.at[v + 1], "yx")


def write(x, part, r1i, yxi, y, buf, strip, s_strip, s_in, s_out):
    dk = x.shape[1] // 4
    ns = dk // CW
    n, size = buf.shape[:2]
    d = lax.axis_index("dp")
    mate = d + 1 - 2 * (d % 2)
    cols = [pl.ds(pl.multiple_of(q * dk + (ns - 1) * CW, 128), CW) for q in (mate, (mate + 2) % 4)]
    loads = []
    for half, late in enumerate((yxi.at[ns - 1, 1], r1i.at[2 * ns - 1, 1])):
        for i, src in enumerate((x.at[:, cols[half]], late)):
            loads.append(pltpu.make_async_copy(src, strip.at[half, i], s_strip.at[2 * half + i]))
    rows = [pl.ds(i * size, size) for i in range(n)]
    ins = [pltpu.make_async_copy(part.at[rows[i], :], buf.at[i], s_in.at[i]) for i in range(n)]
    outs = [pltpu.make_async_copy(buf.at[i], y.at[rows[i], :], s_out.at[i]) for i in range(n)]
    for copy in loads + ins:
        copy.start()
    for copy in loads:
        copy.wait()
    for i in range(n):
        ins[i].wait()
        for half in range(2):
            o = buf[i, :, cols[half]].astype(jnp.float32) + strip[half, 1, rows[i], :].astype(jnp.float32)
            o = o + strip[half, 0, rows[i], :].astype(jnp.float32)
            buf[i, :, cols[half]] = o.astype(buf.dtype)
        outs[i].start()
    for copy in outs:
        copy.wait()


def solution(mesh):
    def body(x, wg, wu, wd):
        rows, dim = x.shape
        dk = dim // 4
        fq = wg.shape[1] // 2
        nch = fq // CW
        ns = dk // CW
        bf16 = jnp.bfloat16
        dma = pltpu.SemaphoreType.DMA
        shapes = [
            (rows, dim),
            (nch, dk, 2 * CW), (nch, dk, 2 * CW), (nch, dk, 2 * CW),
            (3, ns, fq, CW),
            (4 * rows, fq),
            (4, 2 * ns, 2, rows, CW),
            (2 * ns, 2, rows, CW), (2 * ns, 2, rows, CW), (2 * ns, 2, rows, CW), (2, rows * 3 // 4, CW),
        ]
        outs = pl.pallas_call(
            kernel,
            out_shape=[jax.ShapeDtypeStruct(s, bf16) for s in shapes],
            in_specs=[pl.BlockSpec(memory_space=pl.ANY)] * 4,
            out_specs=[pl.BlockSpec(memory_space=pl.ANY)] * len(shapes),
            scratch_shapes=[
                pltpu.VMEM((4 * rows, dim), bf16),
                pltpu.VMEM((3, dim, 2 * CW), bf16),
                pltpu.VMEM((3, rows, CW), bf16),
                pltpu.VMEM((rows, 2 * CW), jnp.float32),
                dma, dma((3,)), dma((6,)), dma((4,)), dma, dma,
                dma, dma((nch,)), dma((nch,)), dma, dma((ns,)), dma((ns,)),
                dma((4,)), dma((3,)), dma, dma((2,)), dma((7,)),
                dma((2 * ns,)), dma((2 * ns + 1,)), dma((2 * ns + 1,)), dma((2,)), dma((8,)), dma((2,)), dma((2,)), dma((4,)), dma((4,)),
            ],
            compiler_params=pltpu.CompilerParams(
                collective_id=0, has_side_effects=True, vmem_limit_bytes=67043328),
            cost_estimate=pl.CostEstimate(
                flops=6 * rows * 4 * dim * fq, bytes_accessed=4 * rows * dim * 2, transcendentals=0),
        )(x, wg, wu, wd)
        part, r1i, yxi = outs[0], outs[8], outs[9]
        n = 8
        any_space = pl.BlockSpec(memory_space=pl.ANY)
        return pl.pallas_call(
            write,
            out_shape=jax.ShapeDtypeStruct((rows, dim), bf16),
            in_specs=[any_space] * 4,
            out_specs=any_space,
            scratch_shapes=[
                pltpu.VMEM((n, rows // n, dim), bf16),
                pltpu.VMEM((2, 2, rows, CW), bf16),
                dma((4,)), dma((n,)), dma((n,)),
            ],
            compiler_params=pltpu.CompilerParams(vmem_limit_bytes=67043328),
        )(x, part, r1i, yxi)

    return jax.shard_map(body, mesh=mesh, in_specs=(P(("dp", "tp"), None), P("dp", "tp"), P("dp", "tp"), P("tp", "dp")), out_specs=P(("dp", "tp"), None), check_vma=False)
```

```python
import jax
import jax.numpy as jnp
from jax import lax
from jax.experimental import pallas as pl
from jax.experimental.pallas import tpu as pltpu
from jax.sharding import PartitionSpec as P

CW = 256


def late_chunks(nch):
    return min(4, nch // 3)


def kernel(x, wg, wu, wd, y, w1, w2, w3, db, hb, po, rdi, r1i, yxi, hy, hx, wx,
           xb, wv, hst, s_loc, s_xs, s_ws, s_xx, s_xy, s_xd, s_w1, s_w2, s_w3, s_d1, s_d2, s_d3, s_wx, s_hx,
           s_wv, s_h, s_po, s_rs, s_rd, s_r1, s_yx, s_ys, s_ld, s_out):
    rows, dim = x.shape
    dk = dim // 4
    fq = wg.shape[1] // 2
    nch = fq // CW
    first = nch // 2
    nl = late_chunks(nch)
    ne = nch - nl
    last = nch - 1
    ns = dk // CW
    f32, bf16 = jnp.float32, jnp.bfloat16

    t = lax.axis_index("tp")
    d = lax.axis_index("dp")
    side = d // 2
    core = d % 2
    mate = d + 1 - 2 * core
    quarter = [d, mate, (d + 2) % 4, (mate + 2) % 4]
    to_mate = {"dp": mate}
    to_x = {"dp": (d + 2) % 4}
    to_y = {"tp": 1 - t}

    def col(v, size=128):
        return v if isinstance(v, int) else pl.multiple_of(v, size)

    def send(src, dst, send_sem, recv_sem, where):
        pltpu.make_async_remote_copy(
            src_ref=src, dst_ref=dst, send_sem=send_sem, recv_sem=recv_sem,
            device_id=where, device_id_type=pl.DeviceIdType.MESH).start()

    def load(src, dst, sem):
        pltpu.make_async_copy(src, dst, sem).start()

    def wait(ref, sem, name="w"):
        with jax.named_scope(name):
            pltpu.make_async_copy(ref, ref, sem).wait()

    def block(b):
        return pl.ds(col(b * rows, rows), rows)

    def slot(s):
        return pl.ds(s * dk, dk)

    def piece(k):
        return pl.ds(col(k * CW), CW)

    barrier = pltpu.get_barrier_semaphore()
    for where in (to_mate, to_x, to_y):
        pl.semaphore_signal(barrier, inc=1, device_id=where, device_id_type=pl.DeviceIdType.MESH)
    pl.semaphore_wait(barrier, 3)

    own_cols = [pl.ds(col(quarter[s] * dk), dk) for s in range(4)]
    for s in range(4):
        src = x.at[:, own_cols[s]]
        send(src, xb.at[block(2), slot(s ^ 2)], s_xs.at[0], s_xx.at[s ^ 2], to_x)
        send(src, xb.at[block(1), slot(s)], s_xs.at[1], s_xy, to_y)
    for s in range(4):
        load(x.at[:, own_cols[s]], xb.at[block(0), slot(s)], s_loc)

    def send_chunk(j, _):
        for m, w in enumerate((wg, wu)):
            away = w.at[:, pl.ds(col((1 - side) * fq + j * CW), CW)]
            here = w.at[:, pl.ds(col(side * fq + j * CW), CW)]
            send(away, w2.at[j, :, pl.ds(m * CW, CW)], s_ws.at[1], s_w2.at[j], to_x)
            send(here, w1.at[j, :, pl.ds(m * CW, CW)], s_ws.at[0], s_w1, to_mate)
        return 0

    lax.fori_loop(0, nch, send_chunk, 0)

    def send_strip(k, _):
        send(wd.at[pl.ds(col((1 - side) * fq), fq), piece(k)], db.at[1, k], s_ws.at[3], s_d2.at[k], to_x)
        send(wd.at[pl.ds(col(side * fq), fq), piece(k)], db.at[0, k], s_ws.at[2], s_d1, to_mate)
        return 0

    lax.fori_loop(0, ns, send_strip, 0)

    for s in (2, 3, 0, 1):
        part = xb.at[block(2), slot(s)]
        wait(part, s_xx.at[s], "xx")
        send(part, xb.at[block(3), slot(s)], s_xs.at[2], s_xd, to_y)

    def send_rest(k, _):
        send(wd.at[pl.ds(col(side * fq + ne * CW), nl * CW), piece(k)], wx.at[0, k], s_ws.at[6], s_wx.at[0], to_y)
        return 0

    lax.fori_loop(0, ns, send_rest, 0)

    at_hand, to_come = pl.ds(0, 2 * dk), pl.ds(2 * dk, 2 * dk)

    def load_here(j, p, sem):
        for m, w in enumerate((wg, wu)):
            here = w.at[:, pl.ds(col(side * fq + j * CW), CW)]
            load(here, wv.at[p, slot(0), pl.ds(m * CW, CW)], s_wv.at[sem])

    def load_slot(w, j, n, p, sem):
        load(w.at[j], wv.at[p, slot(n)], s_wv.at[sem])

    def load_chunk(j, p):
        load_here(j, p, p)
        for n, w in ((1, w1), (2, w2), (3, w3)):
            load_slot(w, j, n, p, p)

    def load_local(j):
        load_here(j, 0, 3)
        load_slot(w1, j, 1, 0, 3)

    def fetch_chunk(j):
        wait(w2.at[j], s_w2.at[j], "w2")
        send(w2.at[j], w3.at[j], s_ws.at[4], s_w3.at[j], to_mate)
        load_slot(w2, j, 2, 0, 0)
        wait(w3.at[j], s_w3.at[j], "w3")
        load_slot(w3, j, 3, 0, 0)

    def wait_chunk():
        wait(wv.at[0, at_hand, :], s_wv.at[3], "wv")
        wait(wv.at[0, to_come, :], s_wv.at[0], "wv")

    def hcopy(b, j, q):
        return pltpu.make_async_copy(hst.at[q], hb.at[block(b), piece(j)], s_h.at[q])

    def gated(b, p):
        ab = jnp.dot(xb[block(b), :], wv[p], preferred_element_type=f32)
        a = ab[:, :CW]
        return (a * jax.nn.sigmoid(a) * ab[:, CW:]).astype(bf16)

    def gate(b, j, p, q, used=True, to=None):
        to = b if to is None else to

        @pl.when(used)
        def _():
            hcopy(to, j, q).wait()

        hst[q] = gated(b, p)
        hcopy(to, j, q).start()

    wait(xb.at[block(0), :], s_loc, "loc")
    wait(xb.at[block(1), :], s_xy, "xy")
    wait(w1, s_w1, "w1")
    load_local(0)

    hcols = pl.ds(0, fq)
    ecols = pl.ds(0, ne * CW)
    both = pl.ds(fq, 2 * CW)

    def load_h(b, to):
        load(hb.at[block(b), :], xb.at[block(to), hcols], s_ld.at[to])

    def wait_h(to):
        wait(xb.at[block(to), hcols], s_ld.at[to], "ld")

    def tile(b, c, n=1):
        return xb.at[block(b), pl.ds(fq + c * CW, n * CW)]

    halves = (pl.ds(0, CW), pl.ds(CW, CW))

    def load_early(k, p):
        load(wd.at[pl.ds(col(side * fq), ne * CW), piece(k)], wv.at[p, ecols, halves[0]], s_wv.at[p])
        load(db.at[0, k, ecols, :], wv.at[p, ecols, halves[1]], s_wv.at[p])

    def load_pair(half, k, p):
        if half == 0:
            src = (wd.at[pl.ds(col(side * fq), fq), piece(k)], db.at[0, k])
        else:
            src = (db.at[1, k], db.at[2, k])
        for m in range(2):
            load(src[m], wv.at[p, hcols, halves[m]], s_wv.at[p])

    def wait_pair(p):
        wait(wv.at[p, hcols, :], s_wv.at[p], "wv")

    def put(b, out, u):
        for m in range(2):
            load(tile(b, m), po.at[out, u, m], s_po)
        wait(tile(b, 0, 2), s_po, "po")

    def down(b, out, u, p):
        o = jnp.dot(xb[block(b), hcols], wv[p, hcols, :], preferred_element_type=f32)
        xb[block(b), both] = o.astype(bf16)
        put(b, out, u)

    def ship_d(u):
        for m in range(2):
            send(po.at[3, u, m], rdi.at[u, m], s_rs.at[0], s_rd.at[u], to_y)

    def ship_1(u):
        for m in range(2):
            send(po.at[1, u, m], r1i.at[u, m], s_rs.at[1], s_r1.at[u], to_y)

    def chunk(j, _):
        fetch_chunk(j)

        @pl.when(j == first)
        def _():
            wait(xb.at[block(3), :], s_xd, "xd")

        @pl.when(j >= first)
        def _():
            load_chunk(j - first, 1)

        wait_chunk()

        def rows_of(n, _):
            g = 3 * j + n
            gate((n + 1) % 3, j, 0, g % 2, g >= 2)
            return 0

        lax.fori_loop(0, 3, rows_of, 0)
        load_local(j + 1)

        @pl.when(j + 1 == ne)
        def _():
            for n in range(2):
                hcopy(0, 0, n).wait()
            load(hb.at[block(1), ecols], xb.at[block(0), ecols], s_ld.at[0])
            wait(db.at[0], s_d1, "d1")
            load_early(0, 2)

        @pl.when(j >= first)
        def _():
            wait(wv.at[1], s_wv.at[1], "wv")
            gate(3, j - first, 1, 2, j > first)

        return 0

    lax.fori_loop(0, ne, chunk, 0)

    wait(xb.at[block(0), ecols], s_ld.at[0], "ld")

    def early(k, _):
        p = 2 - k % 2

        @pl.when(k + 1 < ns)
        def _():
            load_early(k + 1, 3 - p)

        wait(wv.at[p, ecols, :], s_wv.at[p], "wv")
        o = jnp.dot(xb[block(0), ecols], wv[p, ecols, :], preferred_element_type=f32)
        xb[block(0), both] = o.astype(bf16)
        put(0, 1, k)
        ship_1(k)
        return 0

    lax.fori_loop(0, ns, early, 0)

    def late(j, _):
        fetch_chunk(j)
        two = (j > ne) & (j < last)
        base = ne - first + 2 * (j - ne - 1)

        @pl.when(two)
        def _():
            for i in range(2):
                load_chunk(base + i, 1 + i)

        wait_chunk()
        hst[0] = gated(1, 0)
        load(hst.at[0], hy.at[j - ne], s_h.at[0])
        gate(2, j, 0, 1, j > ne)
        wait(hst.at[0], s_h.at[0], "h")
        send(hy.at[j - ne], hx.at[j - ne], s_rs.at[2], s_hx, to_y)

        @pl.when(j < last)
        def _():
            load_local(j + 1)

        @pl.when(two)
        def _():
            def old(i, _):
                wait(wv.at[1 + i], s_wv.at[1 + i], "wv")
                gate(3, base + i, 1 + i, 2)
                return 0

            lax.fori_loop(0, 2, old, 0)

        return 0

    lax.fori_loop(ne, nch, late, 0)
    for s in range(4):
        load(x.at[:, own_cols[s]], xb.at[block(1), slot(s)], s_loc)
    for j in range(nl):
        load(hy.at[j], xb.at[block(0), pl.ds((ne + j) * CW, CW)], s_ld.at[0])
    hcopy(2, last, 1).wait()
    wait(xb.at[block(2), :], s_xs.at[2], "xs")
    load_h(2, 2)
    wait(wx.at[0], s_wx.at[0], "wx")
    send(wx.at[0], wx.at[1], s_ws.at[7], s_wx.at[1], to_mate)

    done = ne - first + 2 * (nl - 2)
    load_chunk(done, 1)

    def diagonal(j, _):
        i = j - done
        p = jnp.where(j == last, 0, 1 + i % 2)

        @pl.when(j + 1 < last)
        def _():
            load_chunk(j + 1, 2 - i % 2)

        @pl.when(j < last)
        def _():
            wait(wv.at[p], s_wv.at[p], "wv")

        gate(3, j, p, 2)
        return 0

    lax.fori_loop(done, nch, diagonal, 0)
    load_pair(0, 0, 1)
    hcopy(3, last, 2).wait()
    load_h(3, 3)
    wait(xb.at[block(0), pl.ds(ne * CW, nl * CW)], s_ld.at[0], "ld")
    wait_h(2)
    wait_h(3)

    def own_half(k, _):
        p = 1 + k % 2

        @pl.when(k + 1 < ns)
        def _():
            load_pair(0, k + 1, 3 - p)

        wait_pair(p)

        def rows_of(n, _):
            down(3 - n, 3 - n, k, p)

            @pl.when(n == 0)
            def _():
                ship_d(k)

            return 0

        lax.fori_loop(0, 2, rows_of, 0)
        return 0

    lax.fori_loop(0, ns, own_half, 0)

    load_chunk(ne, 1)
    wait(xb.at[block(1), :], s_loc, "loc")

    def own_late(j, _):
        i = j - ne
        p = jnp.where(j == last, 0, 1 + i % 2)

        @pl.when(j + 1 < last)
        def _():
            load_chunk(j + 1, 2 - i % 2)

        @pl.when(j < last)
        def _():
            wait(wv.at[p], s_wv.at[p], "wv")

        gate(1, j, p, 0, i > 0, 0)
        return 0

    lax.fori_loop(ne, nch, own_late, 0)

    long = pl.ds(0, fq + nl * CW)
    rest = pl.ds(fq, nl * CW)

    def load_long(k, p):
        load_pair(0, k, p)
        for m in range(2):
            load(wx.at[m, k], wv.at[p, rest, halves[m]], s_wv.at[p])

    hcopy(0, last, 0).wait()
    load_h(0, 1)
    wait(hx, s_hx, "hx")
    for j in range(nl):
        load(hx.at[j], xb.at[block(1), pl.ds(fq + j * CW, CW)], s_ld.at[3])
    wait(wx.at[1], s_wx.at[1], "wx")
    load_long(0, 1)
    wait_h(1)
    wait(xb.at[block(1), rest], s_ld.at[3], "ld")

    def total(tiles):
        o = xb[block(tiles[0][0]), pl.ds(fq + tiles[0][1] * CW, CW)].astype(f32)
        for b, c in tiles[1:]:
            o = o + xb[block(b), pl.ds(fq + c * CW, CW)].astype(f32)
        return o.astype(bf16)

    def relay(half, k, m, turn):
        u = half * ns + k
        load(po.at[2, u, m], tile(0, 2), s_ld.at[0])
        if m == 0:
            wait(rdi.at[u], s_rd.at[u], "rd")
        load(rdi.at[u, m], tile(0, 3), s_ld.at[1])
        ring = turn % 4

        @pl.when(turn >= 4)
        def _():
            wait(tile(ring, 4 + m), s_ys.at[2 * ring + m], "ys")

        wait(tile(0, 2), s_ld.at[0], "ld")
        wait(tile(0, 3), s_ld.at[1], "ld")
        xb[block(ring), pl.ds(fq + (4 + m) * CW, CW)] = total(((0, 2), (0, 3)))
        v = (1 - half) * ns + k
        sem = v if m == 0 else jnp.where(v == ns - 1, 2 * ns, v)
        send(tile(ring, 4 + m), yxi.at[v, m], s_ys.at[2 * ring + m], s_yx.at[sem], to_x)

    def forward_strip(k):
        wait(db.at[1, k], s_d2.at[k], "d2")
        send(db.at[1, k], db.at[2, k], s_ws.at[5], s_d3.at[k], to_mate)

    def own_rows(k, _):
        p = 1 + k % 2

        @pl.when(k + 1 < ns)
        def _():
            load_long(k + 1, 3 - p)
            forward_strip(k)

        wait(wv.at[p, long, :], s_wv.at[p], "wv")
        o = jnp.dot(xb[block(1), long], wv[p, long, :], preferred_element_type=f32)
        xb[block(0), both] = o.astype(bf16)
        put(0, 0, k)

        @pl.when(k < 4)
        def _():
            for m in range(2):
                relay(0, k, m, k)

        return 0

    lax.fori_loop(0, ns, own_rows, 0)

    def fetch_pair(k, p):
        @pl.when(k + 1 == ns)
        def _():
            forward_strip(k)

        wait(db.at[2, k], s_d3.at[k], "d3")
        load_pair(1, k, p)

    def other_half(k, _):
        p = k % 3
        u = ns + k
        wait_pair(p)

        def rows_of(n, _):
            b = jnp.where(n == 0, 3, jnp.where(n == 1, 0, jnp.where(n == 2, 2, 1)))
            out = jnp.where(n == 0, 3, jnp.where(n == 1, 1, jnp.where(n == 2, 2, 0)))
            down(b, out, u, p)

            @pl.when(n == 0)
            def _():
                ship_d(u)

            @pl.when((n == 1) & (k > 0))
            def _():
                ship_1(u - 1)

            @pl.when((n == 1) & (k + 1 < ns))
            def _():
                fetch_pair(k + 1, (k + 1) % 3)

            return 0

        lax.fori_loop(0, 4, rows_of, 0)

        if ns > 4:
            @pl.when(k == 1)
            def _():
                for m in range(2):
                    relay(0, 4, m, 4)

        return 0

    fetch_pair(0, 0)
    lax.fori_loop(0, ns, other_half, 0)
    ship_1(2 * ns - 1)

    parts = ((1, 2), (1, 3), (2, 2), (2, 3))

    def finish(half, k, m, used):
        u = half * ns + k
        n = 2 * half + m
        cols = pl.ds(col(quarter[n] * dk + k * CW), CW)
        load(po.at[0, u, m], tile(*parts[0]), s_ld.at[0])
        load(x.at[:, cols], tile(*parts[1]), s_ld.at[1])
        if m == 0:
            wait(r1i.at[u], s_r1.at[u], "r1")
        load(r1i.at[u, m], tile(*parts[2]), s_ld.at[2])
        if m == 0 and half == 1:
            wait(yxi.at[u], s_yx.at[u], "yx")
        if m == 0 and half == 0:
            @pl.when(k + 1 < ns)
            def _():
                wait(yxi.at[u], s_yx.at[u], "yx")

            @pl.when(k + 1 == ns)
            def _():
                wait(yxi.at[u, 0], s_yx.at[u], "yx")
        load(yxi.at[u, m], tile(*parts[3]), s_ld.at[3])
        for c in range(4):
            wait(tile(*parts[c]), s_ld.at[c], "ld")
        out = pltpu.make_async_copy(tile(3, n), y.at[:, cols], s_out.at[n])

        @pl.when(used)
        def _():
            out.wait()

        xb[block(3), pl.ds(fq + n * CW, CW)] = total(parts)
        out.start()

    def begin():
        cols = pl.ds(col(quarter[1] * dk + (ns - 1) * CW), CW)
        load(po.at[0, ns - 1, 1], tile(*parts[0]), s_ld.at[0])
        load(r1i.at[ns - 1, 1], tile(*parts[1]), s_ld.at[1])
        wait(tile(*parts[0]), s_ld.at[0], "ld")
        wait(tile(*parts[1]), s_ld.at[1], "ld")
        out = pltpu.make_async_copy(tile(3, 1), y.at[:, cols], s_out.at[1])
        out.wait()
        xb[block(3), pl.ds(fq + CW, CW)] = total(parts[:2])
        out.start()

    def tail(k, _):
        @pl.when(k < ns)
        def _():
            for m in range(2):
                relay(1, k, m, ns + k)

        @pl.when(k > 0)
        def _():
            for m in range(2):
                finish(1, k - 1, m, k > 1)
            finish(0, k - 1, 0, k > 1)

            @pl.when(k < ns)
            def _():
                finish(0, k - 1, 1, k > 1)

            @pl.when(k == ns)
            def _():
                begin()

        return 0

    lax.fori_loop(0, ns + 1, tail, 0)

    for n in range(4):
        wait(tile(3, n), s_out.at[n], "out")
    for m in range(2):
        for ring in range(4):
            wait(tile(ring, 4 + m), s_ys.at[2 * ring + m], "ys")
    wait(x, s_xs.at[0], "xs")
    wait(x, s_xs.at[1], "xs")
    wait(w1, s_ws.at[0], "ws")
    wait(w2, s_ws.at[1], "ws")
    wait(db.at[0], s_ws.at[2], "ws")
    wait(db.at[1], s_ws.at[3], "ws")
    wait(w3, s_ws.at[4], "ws")
    wait(db.at[2], s_ws.at[5], "ws")
    wait(wx.at[0], s_ws.at[6], "ws")
    wait(wx.at[1], s_ws.at[7], "ws")
    wait(rdi, s_rs.at[0], "rs")
    wait(r1i, s_rs.at[1], "rs")
    wait(hx, s_rs.at[2], "rs")
    wait(yxi.at[ns - 1, 1], s_yx.at[2 * ns], "yx")


def write(x, part, yxi, y, buf, strip, s_strip, s_in, s_out):
    dk = x.shape[1] // 4
    ns = dk // CW
    n, size = buf.shape[:2]
    d = lax.axis_index("dp")
    mate = d + 1 - 2 * (d % 2)
    cols = pl.ds(pl.multiple_of(mate * dk + (ns - 1) * CW, 128), CW)
    loads = [pltpu.make_async_copy(src, strip.at[i], s_strip.at[i])
             for i, src in enumerate((x.at[:, cols], yxi.at[ns - 1, 1]))]
    rows = [pl.ds(i * size, size) for i in range(n)]
    ins = [pltpu.make_async_copy(part.at[rows[i], :], buf.at[i], s_in.at[i]) for i in range(n)]
    outs = [pltpu.make_async_copy(buf.at[i], y.at[rows[i], :], s_out.at[i]) for i in range(n)]
    for copy in loads + ins:
        copy.start()
    for copy in loads:
        copy.wait()
    for i in range(n):
        ins[i].wait()
        o = buf[i, :, cols].astype(jnp.float32) + strip[1, rows[i], :].astype(jnp.float32)
        o = o + strip[0, rows[i], :].astype(jnp.float32)
        buf[i, :, cols] = o.astype(buf.dtype)
        outs[i].start()
    for copy in outs:
        copy.wait()


def solution(mesh):
    def body(x, wg, wu, wd):
        rows, dim = x.shape
        dk = dim // 4
        fq = wg.shape[1] // 2
        nch = fq // CW
        nl = late_chunks(nch)
        ns = dk // CW
        bf16 = jnp.bfloat16
        dma = pltpu.SemaphoreType.DMA
        pairs = (2 * ns, 2, rows, CW)
        shapes = [
            (rows, dim),
            (nch, dk, 2 * CW), (nch, dk, 2 * CW), (nch, dk, 2 * CW),
            (3, ns, fq, CW),
            (4 * rows, fq),
            (4,) + pairs, pairs, pairs, pairs,
            (nl, rows, CW), (nl, rows, CW),
            (2, ns, nl * CW, CW),
        ]
        any_space = pl.BlockSpec(memory_space=pl.ANY)
        outs = pl.pallas_call(
            kernel,
            out_shape=[jax.ShapeDtypeStruct(s, bf16) for s in shapes],
            in_specs=[any_space] * 4,
            out_specs=[any_space] * len(shapes),
            scratch_shapes=[
                pltpu.VMEM((4 * rows, dim), bf16),
                pltpu.VMEM((3, dim, 2 * CW), bf16),
                pltpu.VMEM((3, rows, CW), bf16),
                dma, dma((3,)), dma((8,)), dma((4,)), dma, dma,
                dma, dma((nch,)), dma((nch,)), dma, dma((ns,)), dma((ns,)), dma((2,)), dma,
                dma((4,)), dma((3,)), dma, dma((3,)),
                dma((2 * ns,)), dma((2 * ns,)), dma((2 * ns + 1,)), dma((8,)), dma((4,)), dma((4,)),
            ],
            compiler_params=pltpu.CompilerParams(
                collective_id=0, has_side_effects=True, vmem_limit_bytes=67043328),
            cost_estimate=pl.CostEstimate(
                flops=6 * rows * 4 * dim * fq, bytes_accessed=4 * rows * dim * 2, transcendentals=0),
        )(x, wg, wu, wd)
        n = 8
        return pl.pallas_call(
            write,
            out_shape=jax.ShapeDtypeStruct((rows, dim), bf16),
            in_specs=[any_space] * 3,
            out_specs=any_space,
            scratch_shapes=[
                pltpu.VMEM((n, rows // n, dim), bf16),
                pltpu.VMEM((2, rows, CW), bf16),
                dma((2,)), dma((n,)), dma((n,)),
            ],
            compiler_params=pltpu.CompilerParams(vmem_limit_bytes=67043328),
        )(x, outs[0], outs[9])

    return jax.shard_map(body, mesh=mesh, in_specs=(P(("dp", "tp"), None), P("dp", "tp"), P("dp", "tp"), P("tp", "dp")), out_specs=P(("dp", "tp"), None), check_vma=False)
```

```python
import jax
import jax.numpy as jnp
from jax import lax
from jax.experimental import pallas as pl
from jax.experimental.pallas import tpu as pltpu
from jax.sharding import PartitionSpec as P

CW = 256


def late_chunks(nch):
    return min(4, nch // 3)


def kernel(x, wg, wu, wd, y, w1, w2, w3, db, hb, po, rdi, r1i, yxi, hy, hx, wx,
           xb, wv, hst, s_loc, s_xs, s_ws, s_xx, s_xy, s_xd, s_w1, s_w2, s_w3, s_d1, s_d2, s_d3, s_wx, s_hx,
           s_wv, s_h, s_po, s_rs, s_rd, s_r1, s_yx, s_ys, s_ld, s_out):
    rows, dim = x.shape
    dk = dim // 4
    fq = wg.shape[1] // 2
    nch = fq // CW
    first = nch // 2
    nl = late_chunks(nch)
    ne = nch - nl
    last = nch - 1
    ns = dk // CW
    f32, bf16 = jnp.float32, jnp.bfloat16

    t = lax.axis_index("tp")
    d = lax.axis_index("dp")
    side = d // 2
    core = d % 2
    mate = d + 1 - 2 * core
    quarter = [d, mate, (d + 2) % 4, (mate + 2) % 4]
    to_mate = {"dp": mate}
    to_x = {"dp": (d + 2) % 4}
    to_y = {"tp": 1 - t}

    def col(v, size=128):
        return v if isinstance(v, int) else pl.multiple_of(v, size)

    def send(src, dst, send_sem, recv_sem, where):
        pltpu.make_async_remote_copy(
            src_ref=src, dst_ref=dst, send_sem=send_sem, recv_sem=recv_sem,
            device_id=where, device_id_type=pl.DeviceIdType.MESH).start()

    def load(src, dst, sem):
        pltpu.make_async_copy(src, dst, sem).start()

    def wait(ref, sem, name="w"):
        with jax.named_scope(name):
            pltpu.make_async_copy(ref, ref, sem).wait()

    def block(b):
        return pl.ds(col(b * rows, rows), rows)

    def slot(s):
        return pl.ds(s * dk, dk)

    def piece(k):
        return pl.ds(col(k * CW), CW)

    barrier = pltpu.get_barrier_semaphore()
    for where in (to_mate, to_x, to_y):
        pl.semaphore_signal(barrier, inc=1, device_id=where, device_id_type=pl.DeviceIdType.MESH)
    pl.semaphore_wait(barrier, 3)

    own_cols = [pl.ds(col(quarter[s] * dk), dk) for s in range(4)]
    for s in range(4):
        src = x.at[:, own_cols[s]]
        send(src, xb.at[block(2), slot(s ^ 2)], s_xs.at[0], s_xx.at[s ^ 2], to_x)
        send(src, xb.at[block(1), slot(s)], s_xs.at[1], s_xy, to_y)
    for s in range(4):
        load(x.at[:, own_cols[s]], xb.at[block(0), slot(s)], s_loc)

    def send_chunk(j, _):
        for m, w in enumerate((wg, wu)):
            away = w.at[:, pl.ds(col((1 - side) * fq + j * CW), CW)]
            here = w.at[:, pl.ds(col(side * fq + j * CW), CW)]
            send(away, w2.at[j, :, pl.ds(m * CW, CW)], s_ws.at[1], s_w2.at[j], to_x)
            send(here, w1.at[j, :, pl.ds(m * CW, CW)], s_ws.at[0], s_w1, to_mate)
        return 0

    lax.fori_loop(0, nch, send_chunk, 0)

    def send_strip(k, _):
        send(wd.at[pl.ds(col((1 - side) * fq), fq), piece(k)], db.at[1, k], s_ws.at[3], s_d2.at[k], to_x)
        send(wd.at[pl.ds(col(side * fq), fq), piece(k)], db.at[0, k], s_ws.at[2], s_d1, to_mate)
        return 0

    lax.fori_loop(0, ns, send_strip, 0)

    for s in (2, 3, 0, 1):
        part = xb.at[block(2), slot(s)]
        wait(part, s_xx.at[s], "xx")
        send(part, xb.at[block(3), slot(s)], s_xs.at[2], s_xd, to_y)

    def send_rest(k, _):
        send(wd.at[pl.ds(col(side * fq + ne * CW), nl * CW), piece(k)], wx.at[0, k], s_ws.at[6], s_wx.at[0], to_y)
        return 0

    lax.fori_loop(0, ns, send_rest, 0)

    at_hand, to_come = pl.ds(0, 2 * dk), pl.ds(2 * dk, 2 * dk)

    def load_here(j, p, sem):
        for m, w in enumerate((wg, wu)):
            here = w.at[:, pl.ds(col(side * fq + j * CW), CW)]
            load(here, wv.at[p, slot(0), pl.ds(m * CW, CW)], s_wv.at[sem])

    def load_slot(w, j, n, p, sem):
        load(w.at[j], wv.at[p, slot(n)], s_wv.at[sem])

    def load_chunk(j, p):
        load_here(j, p, p)
        for n, w in ((1, w1), (2, w2), (3, w3)):
            load_slot(w, j, n, p, p)

    def load_local(j):
        load_here(j, 0, 3)
        load_slot(w1, j, 1, 0, 3)

    def fetch_chunk(j):
        wait(w2.at[j], s_w2.at[j], "w2")
        send(w2.at[j], w3.at[j], s_ws.at[4], s_w3.at[j], to_mate)
        load_slot(w2, j, 2, 0, 0)
        wait(w3.at[j], s_w3.at[j], "w3")
        load_slot(w3, j, 3, 0, 0)

    def wait_chunk():
        wait(wv.at[0, at_hand, :], s_wv.at[3], "wv")
        wait(wv.at[0, to_come, :], s_wv.at[0], "wv")

    def hcopy(b, j, q):
        return pltpu.make_async_copy(hst.at[q], hb.at[block(b), piece(j)], s_h.at[q])

    def gated(b, p):
        ab = jnp.dot(xb[block(b), :], wv[p], preferred_element_type=f32)
        a = ab[:, :CW]
        return (a * jax.nn.sigmoid(a) * ab[:, CW:]).astype(bf16)

    def gate(b, j, p, q, used=True, to=None):
        to = b if to is None else to

        @pl.when(used)
        def _():
            hcopy(to, j, q).wait()

        hst[q] = gated(b, p)
        hcopy(to, j, q).start()

    wait(xb.at[block(0), :], s_loc, "loc")
    wait(xb.at[block(1), :], s_xy, "xy")
    wait(w1, s_w1, "w1")
    load_local(0)

    hcols = pl.ds(0, fq)
    ecols = pl.ds(0, ne * CW)
    both = pl.ds(fq, 2 * CW)

    def load_h(b, to):
        load(hb.at[block(b), :], xb.at[block(to), hcols], s_ld.at[to])

    def wait_h(to):
        wait(xb.at[block(to), hcols], s_ld.at[to], "ld")

    def tile(b, c, n=1):
        return xb.at[block(b), pl.ds(fq + c * CW, n * CW)]

    halves = (pl.ds(0, CW), pl.ds(CW, CW))

    def load_early(k, p):
        load(wd.at[pl.ds(col(side * fq), ne * CW), piece(k)], wv.at[p, ecols, halves[0]], s_wv.at[p])
        load(db.at[0, k, ecols, :], wv.at[p, ecols, halves[1]], s_wv.at[p])

    def load_pair(half, k, p):
        if half == 0:
            src = (wd.at[pl.ds(col(side * fq), fq), piece(k)], db.at[0, k])
        else:
            src = (db.at[1, k], db.at[2, k])
        for m in range(2):
            load(src[m], wv.at[p, hcols, halves[m]], s_wv.at[p])

    def wait_pair(p):
        wait(wv.at[p, hcols, :], s_wv.at[p], "wv")

    def put(b, out, u):
        for m in range(2):
            load(tile(b, m), po.at[out, u, m], s_po)
        wait(tile(b, 0, 2), s_po, "po")

    def down(b, out, u, p):
        o = jnp.dot(xb[block(b), hcols], wv[p, hcols, :], preferred_element_type=f32)
        xb[block(b), both] = o.astype(bf16)
        put(b, out, u)

    def ship_d(u):
        for m in range(2):
            send(po.at[3, u, m], rdi.at[u, m], s_rs.at[0], s_rd.at[u], to_y)

    def ship_1(u):
        for m in range(2):
            send(po.at[1, u, m], r1i.at[u, m], s_rs.at[1], s_r1.at[u], to_y)

    def chunk(j, _):
        fetch_chunk(j)

        @pl.when(j == first)
        def _():
            wait(xb.at[block(3), :], s_xd, "xd")

        @pl.when(j >= first)
        def _():
            load_chunk(j - first, 1)

        wait_chunk()

        def rows_of(n, _):
            g = 3 * j + n
            gate((n + 1) % 3, j, 0, g % 2, g >= 2)
            return 0

        lax.fori_loop(0, 3, rows_of, 0)
        load_local(j + 1)

        @pl.when(j + 1 == ne)
        def _():
            for n in range(2):
                hcopy(0, 0, n).wait()
            load(hb.at[block(1), ecols], xb.at[block(0), ecols], s_ld.at[0])
            wait(db.at[0], s_d1, "d1")
            load_early(0, 2)

        @pl.when(j >= first)
        def _():
            wait(wv.at[1], s_wv.at[1], "wv")
            gate(3, j - first, 1, 2, j > first)

        return 0

    lax.fori_loop(0, ne, chunk, 0)

    wait(xb.at[block(0), ecols], s_ld.at[0], "ld")

    def early(k, _):
        p = 2 - k % 2

        @pl.when(k + 1 < ns)
        def _():
            load_early(k + 1, 3 - p)

        wait(wv.at[p, ecols, :], s_wv.at[p], "wv")
        o = jnp.dot(xb[block(0), ecols], wv[p, ecols, :], preferred_element_type=f32)
        xb[block(0), both] = o.astype(bf16)
        put(0, 1, k)
        ship_1(k)
        return 0

    lax.fori_loop(0, ns, early, 0)

    done = ne - first + 2 * (nl - 2)

    def late(j, _):
        fetch_chunk(j)
        two = (j > ne) & (j < last)
        base = ne - first + 2 * (j - ne - 1)

        @pl.when(two)
        def _():
            for i in range(2):
                load_chunk(base + i, 1 + i)

        @pl.when(j == last)
        def _():
            load_chunk(done, 1)

        wait_chunk()
        hst[0] = gated(1, 0)
        load(hst.at[0], hy.at[j - ne], s_h.at[0])
        gate(2, j, 0, 1, j > ne)
        wait(hst.at[0], s_h.at[0], "h")
        send(hy.at[j - ne], hx.at[j - ne], s_rs.at[2], s_hx, to_y)

        @pl.when(j < last)
        def _():
            load_local(j + 1)

        @pl.when(two)
        def _():
            def old(i, _):
                wait(wv.at[1 + i], s_wv.at[1 + i], "wv")
                gate(3, base + i, 1 + i, 2)
                return 0

            lax.fori_loop(0, 2, old, 0)

        return 0

    lax.fori_loop(ne, nch, late, 0)
    for j in range(nl):
        load(hy.at[j], xb.at[block(0), pl.ds((ne + j) * CW, CW)], s_ld.at[0])
    hcopy(2, last, 1).wait()
    wait(xb.at[block(2), :], s_xs.at[2], "xs")
    load_h(2, 2)
    wait(wx.at[0], s_wx.at[0], "wx")
    send(wx.at[0], wx.at[1], s_ws.at[7], s_wx.at[1], to_mate)

    def diagonal(j, _):
        i = j - done
        p = jnp.where(j == last, 0, 1 + i % 2)

        @pl.when(j + 1 < last)
        def _():
            load_chunk(j + 1, 2 - i % 2)

        @pl.when(j < last)
        def _():
            wait(wv.at[p], s_wv.at[p], "wv")

        gate(3, j, p, 2 - i % 2, i != 1)
        return 0

    lax.fori_loop(done, nch, diagonal, 0)
    load_pair(0, 0, 1)
    for q in (1, 2):
        hcopy(3, last, q).wait()
    load_h(3, 3)
    wait(xb.at[block(0), pl.ds(ne * CW, nl * CW)], s_ld.at[0], "ld")
    wait_h(2)
    wait_h(3)
    for s in range(4):
        load(x.at[:, own_cols[s]], xb.at[block(1), slot(s)], s_loc)

    def forward_strip(k):
        wait(db.at[1, k], s_d2.at[k], "d2")
        send(db.at[1, k], db.at[2, k], s_ws.at[5], s_d3.at[k], to_mate)

    def own_half(k, _):
        p = 1 + k % 2

        @pl.when(k + 1 < ns)
        def _():
            load_pair(0, k + 1, 3 - p)

        wait_pair(p)

        def rows_of(n, _):
            down(3 - n, 3 - n, k, p)

            @pl.when(n == 0)
            def _():
                ship_d(k)

            return 0

        lax.fori_loop(0, 2, rows_of, 0)

        @pl.when(k == 1)
        def _():
            forward_strip(0)

        @pl.when(k + 1 == ns)
        def _():
            forward_strip(1)

        return 0

    lax.fori_loop(0, ns, own_half, 0)

    def total(tiles):
        o = xb[block(tiles[0][0]), pl.ds(fq + tiles[0][1] * CW, CW)].astype(f32)
        for b, c in tiles[1:]:
            o = o + xb[block(b), pl.ds(fq + c * CW, CW)].astype(f32)
        return o.astype(bf16)

    def ring_at(ring, m):
        b = jnp.where(ring == 0, 0, jnp.where(ring == 3, 3, 2))
        c = jnp.where(ring == 1, 2, 4)
        return block(b), pl.ds(col(fq + (c + m) * CW), CW)

    def ring_tile(ring, m):
        return xb.at[ring_at(ring, m)]

    def relay(half, k, m, turn):
        u = half * ns + k
        load(po.at[2, u, m], tile(0, 2), s_ld.at[0])
        if m == 0:
            wait(rdi.at[u], s_rd.at[u], "rd")
        load(rdi.at[u, m], tile(0, 3), s_ld.at[1])
        ring = turn % 4

        @pl.when(turn >= 4)
        def _():
            wait(ring_tile(ring, m), s_ys.at[2 * ring + m], "ys")

        wait(tile(0, 2), s_ld.at[0], "ld")
        wait(tile(0, 3), s_ld.at[1], "ld")
        xb[ring_at(ring, m)] = total(((0, 2), (0, 3)))
        v = (1 - half) * ns + k
        sem = v if m == 0 else jnp.where(v == ns - 1, 2 * ns, v)
        send(ring_tile(ring, m), yxi.at[v, m], s_ys.at[2 * ring + m], s_yx.at[sem], to_x)

    def fetch_pair(k):
        @pl.when(k >= 3)
        def _():
            forward_strip(k)

        wait(db.at[2, k], s_d3.at[k], "d3")
        load_pair(1, k, 1 + k % 2)

    def other_half(k, _):
        p = 1 + k % 2
        u = ns + k
        wait_pair(p)

        def rows_of(n, _):
            b = jnp.where(n == 0, 3, jnp.where(n == 1, 0, 2))
            down(b, jnp.where(n == 1, 1, b), u, p)

            @pl.when(n == 0)
            def _():
                ship_d(u)

            @pl.when((n == 1) & (k > 0))
            def _():
                ship_1(u - 1)

            return 0

        lax.fori_loop(0, 3, rows_of, 0)
        for m in range(2):
            relay(0, k, m, k)

        @pl.when(k == 0)
        def _():
            forward_strip(2)

        @pl.when(k + 1 < ns)
        def _():
            fetch_pair(k + 1)

        return 0

    fetch_pair(0)
    lax.fori_loop(0, ns, other_half, 0)
    ship_1(2 * ns - 1)

    load_chunk(ne, 1)
    wait(xb.at[block(1), :], s_loc, "loc")

    def own_late(j, _):
        i = j - ne
        p = jnp.where(j == last, 0, 1 + i % 2)

        @pl.when(j + 1 < last)
        def _():
            load_chunk(j + 1, 2 - i % 2)

        @pl.when(j < last)
        def _():
            wait(wv.at[p], s_wv.at[p], "wv")

        gate(1, j, p, i % 2, i > 1, 0)
        return 0

    lax.fori_loop(ne, nch, own_late, 0)

    long = pl.ds(0, fq + nl * CW)
    rest = pl.ds(fq, nl * CW)

    def load_long(k, p):
        load_pair(0, k, p)
        for m in range(2):
            load(wx.at[m, k], wv.at[p, rest, halves[m]], s_wv.at[p])

    for q in range(2):
        hcopy(0, last, q).wait()
    load_h(0, 1)
    wait(hx, s_hx, "hx")
    for j in range(nl):
        load(hx.at[j], xb.at[block(1), pl.ds(fq + j * CW, CW)], s_ld.at[3])
    wait(wx.at[1], s_wx.at[1], "wx")
    load_long(0, 1)
    wait_h(1)
    wait(xb.at[block(1), rest], s_ld.at[3], "ld")

    for m in range(2):
        relay(1, 0, m, ns)

    def own_rows(k, _):
        p = 1 + k % 2

        @pl.when(k + 1 < ns)
        def _():
            load_long(k + 1, 3 - p)

        wait(wv.at[p, long, :], s_wv.at[p], "wv")
        o = jnp.dot(xb[block(1), long], wv[p, long, :], preferred_element_type=f32)
        xb[block(0), both] = o.astype(bf16)
        put(0, 0, k)
        return 0

    lax.fori_loop(0, ns, own_rows, 0)
    load_pair(1, 0, 1)
    for m in range(2):
        relay(1, 1, m, ns + 1)

    def own_rows_too(k, _):
        p = 1 + k % 2

        @pl.when(k + 1 < ns)
        def _():
            load_pair(1, k + 1, 3 - p)

        wait_pair(p)
        down(1, 0, ns + k, p)
        return 0

    lax.fori_loop(0, ns, own_rows_too, 0)
    for m in range(2):
        relay(1, 2, m, ns + 2)

    parts = ((1, 2), (1, 3), (1, 4), (1, 5))

    def finish(half, k, m, used):
        u = half * ns + k
        n = 2 * half + m
        cols = pl.ds(col(quarter[n] * dk + k * CW), CW)
        load(po.at[0, u, m], tile(*parts[0]), s_ld.at[0])
        load(x.at[:, cols], tile(*parts[1]), s_ld.at[1])
        if m == 0:
            wait(r1i.at[u], s_r1.at[u], "r1")
        load(r1i.at[u, m], tile(*parts[2]), s_ld.at[2])
        if m == 0 and half == 1:
            wait(yxi.at[u], s_yx.at[u], "yx")
        if m == 0 and half == 0:
            @pl.when(k + 1 < ns)
            def _():
                wait(yxi.at[u], s_yx.at[u], "yx")

            @pl.when(k + 1 == ns)
            def _():
                wait(yxi.at[u, 0], s_yx.at[u], "yx")
        load(yxi.at[u, m], tile(*parts[3]), s_ld.at[3])
        for c in range(4):
            wait(tile(*parts[c]), s_ld.at[c], "ld")
        out = pltpu.make_async_copy(tile(3, n), y.at[:, cols], s_out.at[n])

        @pl.when(used)
        def _():
            out.wait()

        xb[block(3), pl.ds(fq + n * CW, CW)] = total(parts)
        out.start()

    def begin():
        cols = pl.ds(col(quarter[1] * dk + (ns - 1) * CW), CW)
        load(po.at[0, ns - 1, 1], tile(*parts[0]), s_ld.at[0])
        load(r1i.at[ns - 1, 1], tile(*parts[1]), s_ld.at[1])
        wait(tile(*parts[0]), s_ld.at[0], "ld")
        wait(tile(*parts[1]), s_ld.at[1], "ld")
        out = pltpu.make_async_copy(tile(3, 1), y.at[:, cols], s_out.at[1])
        out.wait()
        xb[block(3), pl.ds(fq + CW, CW)] = total(parts[:2])
        out.start()

    def tail(k, _):
        @pl.when((k > 2) & (k < ns))
        def _():
            for m in range(2):
                relay(1, k, m, ns + k)

        @pl.when(k > 0)
        def _():
            finish(0, k - 1, 0, k > 1)

            @pl.when(k < ns)
            def _():
                finish(0, k - 1, 1, k > 1)

            @pl.when(k == ns)
            def _():
                begin()

            for m in range(2):
                finish(1, k - 1, m, k > 1)

        return 0

    lax.fori_loop(0, ns + 1, tail, 0)

    for n in range(4):
        wait(tile(3, n), s_out.at[n], "out")
    for m in range(2):
        for ring in range(4):
            wait(ring_tile(ring, m), s_ys.at[2 * ring + m], "ys")
    wait(x, s_xs.at[0], "xs")
    wait(x, s_xs.at[1], "xs")
    wait(w1, s_ws.at[0], "ws")
    wait(w2, s_ws.at[1], "ws")
    wait(db.at[0], s_ws.at[2], "ws")
    wait(db.at[1], s_ws.at[3], "ws")
    wait(w3, s_ws.at[4], "ws")
    wait(db.at[2], s_ws.at[5], "ws")
    wait(wx.at[0], s_ws.at[6], "ws")
    wait(wx.at[1], s_ws.at[7], "ws")
    wait(rdi, s_rs.at[0], "rs")
    wait(r1i, s_rs.at[1], "rs")
    wait(hx, s_rs.at[2], "rs")
    wait(yxi.at[ns - 1, 1], s_yx.at[2 * ns], "yx")


def write(x, part, yxi, y, buf, strip, s_strip, s_in, s_out):
    dk = x.shape[1] // 4
    ns = dk // CW
    n, size = buf.shape[:2]
    d = lax.axis_index("dp")
    mate = d + 1 - 2 * (d % 2)
    cols = pl.ds(pl.multiple_of(mate * dk + (ns - 1) * CW, 128), CW)
    loads = [pltpu.make_async_copy(src, strip.at[i], s_strip.at[i])
             for i, src in enumerate((x.at[:, cols], yxi.at[ns - 1, 1]))]
    rows = [pl.ds(i * size, size) for i in range(n)]
    ins = [pltpu.make_async_copy(part.at[rows[i], :], buf.at[i], s_in.at[i]) for i in range(n)]
    outs = [pltpu.make_async_copy(buf.at[i], y.at[rows[i], :], s_out.at[i]) for i in range(n)]
    for copy in loads + ins:
        copy.start()
    for copy in loads:
        copy.wait()
    for i in range(n):
        ins[i].wait()
        o = buf[i, :, cols].astype(jnp.float32) + strip[1, rows[i], :].astype(jnp.float32)
        o = o + strip[0, rows[i], :].astype(jnp.float32)
        buf[i, :, cols] = o.astype(buf.dtype)
        outs[i].start()
    for copy in outs:
        copy.wait()


def solution(mesh):
    def body(x, wg, wu, wd):
        rows, dim = x.shape
        dk = dim // 4
        fq = wg.shape[1] // 2
        nch = fq // CW
        nl = late_chunks(nch)
        ns = dk // CW
        bf16 = jnp.bfloat16
        dma = pltpu.SemaphoreType.DMA
        pairs = (2 * ns, 2, rows, CW)
        shapes = [
            (rows, dim),
            (nch, dk, 2 * CW), (nch, dk, 2 * CW), (nch, dk, 2 * CW),
            (3, ns, fq, CW),
            (4 * rows, fq),
            (4,) + pairs, pairs, pairs, pairs,
            (nl, rows, CW), (nl, rows, CW),
            (2, ns, nl * CW, CW),
        ]
        any_space = pl.BlockSpec(memory_space=pl.ANY)
        outs = pl.pallas_call(
            kernel,
            out_shape=[jax.ShapeDtypeStruct(s, bf16) for s in shapes],
            in_specs=[any_space] * 4,
            out_specs=[any_space] * len(shapes),
            scratch_shapes=[
                pltpu.VMEM((4 * rows, dim), bf16),
                pltpu.VMEM((3, dim, 2 * CW), bf16),
                pltpu.VMEM((3, rows, CW), bf16),
                dma, dma((3,)), dma((8,)), dma((4,)), dma, dma,
                dma, dma((nch,)), dma((nch,)), dma, dma((ns,)), dma((ns,)), dma((2,)), dma,
                dma((4,)), dma((3,)), dma, dma((3,)),
                dma((2 * ns,)), dma((2 * ns,)), dma((2 * ns + 1,)), dma((8,)), dma((4,)), dma((4,)),
            ],
            compiler_params=pltpu.CompilerParams(
                collective_id=0, has_side_effects=True, vmem_limit_bytes=67043328),
            cost_estimate=pl.CostEstimate(
                flops=6 * rows * 4 * dim * fq, bytes_accessed=4 * rows * dim * 2, transcendentals=0),
        )(x, wg, wu, wd)
        n = 8
        return pl.pallas_call(
            write,
            out_shape=jax.ShapeDtypeStruct((rows, dim), bf16),
            in_specs=[any_space] * 3,
            out_specs=any_space,
            scratch_shapes=[
                pltpu.VMEM((n, rows // n, dim), bf16),
                pltpu.VMEM((2, rows, CW), bf16),
                dma((2,)), dma((n,)), dma((n,)),
            ],
            compiler_params=pltpu.CompilerParams(vmem_limit_bytes=67043328),
        )(x, outs[0], outs[9])

    return jax.shard_map(body, mesh=mesh, in_specs=(P(("dp", "tp"), None), P("dp", "tp"), P("dp", "tp"), P("tp", "dp")), out_specs=P(("dp", "tp"), None), check_vma=False)
```

```python
import jax
import jax.numpy as jnp
from jax import lax
from jax.experimental import pallas as pl
from jax.experimental.pallas import tpu as pltpu
from jax.sharding import PartitionSpec as P

CW = 256


def late_chunks(nch):
    return min(4, nch // 3)


def kernel(x, wg, wu, wd, wv, w1, w2, w3, db, hb, po, rdi, r1i, yxi, hy, hx, wx,
           xb, hst, s_loc, s_xs, s_ws, s_xx, s_xy, s_xd, s_w1, s_w2, s_w3, s_d1, s_d2, s_d3, s_wx, s_hx,
           s_wv, s_h, s_po, s_rs, s_rd, s_r1, s_yx, s_ys, s_ld):
    rows, dim = x.shape
    dk = dim // 4
    fq = wg.shape[1] // 2
    nch = fq // CW
    first = nch // 2
    nl = late_chunks(nch)
    ne = nch - nl
    last = nch - 1
    ns = dk // CW
    f32, bf16 = jnp.float32, jnp.bfloat16

    t = lax.axis_index("tp")
    d = lax.axis_index("dp")
    side = d // 2
    core = d % 2
    mate = d + 1 - 2 * core
    quarter = [d, mate, (d + 2) % 4, (mate + 2) % 4]
    to_mate = {"dp": mate}
    to_x = {"dp": (d + 2) % 4}
    to_y = {"tp": 1 - t}

    def col(v, size=128):
        return v if isinstance(v, int) else pl.multiple_of(v, size)

    def send(src, dst, send_sem, recv_sem, where):
        pltpu.make_async_remote_copy(
            src_ref=src, dst_ref=dst, send_sem=send_sem, recv_sem=recv_sem,
            device_id=where, device_id_type=pl.DeviceIdType.MESH).start()

    def load(src, dst, sem):
        pltpu.make_async_copy(src, dst, sem).start()

    def wait(ref, sem, name="w"):
        with jax.named_scope(name):
            pltpu.make_async_copy(ref, ref, sem).wait()

    def block(b):
        return pl.ds(col(b * rows, rows), rows)

    def slot(s):
        return pl.ds(s * dk, dk)

    def piece(k):
        return pl.ds(col(k * CW), CW)

    barrier = pltpu.get_barrier_semaphore()
    for where in (to_mate, to_x, to_y):
        pl.semaphore_signal(barrier, inc=1, device_id=where, device_id_type=pl.DeviceIdType.MESH)
    pl.semaphore_wait(barrier, 3)

    own_cols = [pl.ds(col(quarter[s] * dk), dk) for s in range(4)]
    for s in range(4):
        src = x.at[:, own_cols[s]]
        send(src, xb.at[block(2), slot(s ^ 2)], s_xs.at[0], s_xx.at[s ^ 2], to_x)
        send(src, xb.at[block(1), slot(s)], s_xs.at[1], s_xy, to_y)
    for s in range(4):
        load(x.at[:, own_cols[s]], xb.at[block(0), slot(s)], s_loc)

    def send_chunk(j, _):
        for m, w in enumerate((wg, wu)):
            away = w.at[:, pl.ds(col((1 - side) * fq + j * CW), CW)]
            here = w.at[:, pl.ds(col(side * fq + j * CW), CW)]
            send(away, w2.at[j, :, pl.ds(m * CW, CW)], s_ws.at[1], s_w2.at[j], to_x)
            send(here, w1.at[j, :, pl.ds(m * CW, CW)], s_ws.at[0], s_w1, to_mate)
        return 0

    lax.fori_loop(0, nch, send_chunk, 0)

    def send_strip(k, _):
        send(wd.at[pl.ds(col((1 - side) * fq), fq), piece(k)], db.at[1, k], s_ws.at[3], s_d2.at[k], to_x)
        send(wd.at[pl.ds(col(side * fq), fq), piece(k)], db.at[0, k], s_ws.at[2], s_d1, to_mate)
        return 0

    lax.fori_loop(0, ns, send_strip, 0)

    for s in (2, 3, 0, 1):
        part = xb.at[block(2), slot(s)]
        wait(part, s_xx.at[s], "xx")
        send(part, xb.at[block(3), slot(s)], s_xs.at[2], s_xd, to_y)

    def send_rest(k, _):
        send(wd.at[pl.ds(col(side * fq + ne * CW), nl * CW), piece(k)], wx.at[0, k], s_ws.at[6], s_wx.at[0], to_y)
        return 0

    lax.fori_loop(0, ns, send_rest, 0)

    at_hand, to_come = pl.ds(0, 2 * dk), pl.ds(2 * dk, 2 * dk)

    def load_here(j, p, sem):
        for m, w in enumerate((wg, wu)):
            here = w.at[:, pl.ds(col(side * fq + j * CW), CW)]
            load(here, wv.at[p, slot(0), pl.ds(m * CW, CW)], s_wv.at[sem])

    def load_slot(w, j, n, p, sem):
        load(w.at[j], wv.at[p, slot(n)], s_wv.at[sem])

    def load_chunk(j, p):
        load_here(j, p, p)
        for n, w in ((1, w1), (2, w2), (3, w3)):
            load_slot(w, j, n, p, p)

    def load_local(j):
        load_here(j, 0, 3)
        load_slot(w1, j, 1, 0, 3)

    def fetch_chunk(j):
        wait(w2.at[j], s_w2.at[j], "w2")
        send(w2.at[j], w3.at[j], s_ws.at[4], s_w3.at[j], to_mate)
        load_slot(w2, j, 2, 0, 0)
        wait(w3.at[j], s_w3.at[j], "w3")
        load_slot(w3, j, 3, 0, 0)

    def wait_chunk():
        wait(wv.at[0, at_hand, :], s_wv.at[3], "wv")
        wait(wv.at[0, to_come, :], s_wv.at[0], "wv")

    def hcopy(b, j, q):
        return pltpu.make_async_copy(hst.at[q], hb.at[block(b), piece(j)], s_h.at[q])

    def gated(b, p):
        ab = jnp.dot(xb[block(b), :], wv[p], preferred_element_type=f32)
        a = ab[:, :CW]
        return (a * jax.nn.sigmoid(a) * ab[:, CW:]).astype(bf16)

    def gate(b, j, p, q, used=True, to=None):
        to = b if to is None else to

        @pl.when(used)
        def _():
            hcopy(to, j, q).wait()

        hst[q] = gated(b, p)
        hcopy(to, j, q).start()

    wait(xb.at[block(0), :], s_loc, "loc")
    wait(xb.at[block(1), :], s_xy, "xy")
    wait(w1, s_w1, "w1")
    load_local(0)

    hcols = pl.ds(0, fq)
    ecols = pl.ds(0, ne * CW)
    both = pl.ds(fq, 2 * CW)

    def load_h(b, to):
        load(hb.at[block(b), :], xb.at[block(to), hcols], s_ld.at[to])

    def wait_h(to):
        wait(xb.at[block(to), hcols], s_ld.at[to], "ld")

    def tile(b, c, n=1):
        return xb.at[block(b), pl.ds(fq + c * CW, n * CW)]

    halves = (pl.ds(0, CW), pl.ds(CW, CW))

    def load_early(k, p):
        load(wd.at[pl.ds(col(side * fq), ne * CW), piece(k)], wv.at[p, ecols, halves[0]], s_wv.at[p])
        load(db.at[0, k, ecols, :], wv.at[p, ecols, halves[1]], s_wv.at[p])

    def load_pair(half, k, p):
        if half == 0:
            src = (wd.at[pl.ds(col(side * fq), fq), piece(k)], db.at[0, k])
        else:
            src = (db.at[1, k], db.at[2, k])
        for m in range(2):
            load(src[m], wv.at[p, hcols, halves[m]], s_wv.at[p])

    def wait_pair(p):
        wait(wv.at[p, hcols, :], s_wv.at[p], "wv")

    def put(b, out, u):
        for m in range(2):
            load(tile(b, m), po.at[out, u, m], s_po)
        wait(tile(b, 0, 2), s_po, "po")

    def down(b, out, u, p):
        o = jnp.dot(xb[block(b), hcols], wv[p, hcols, :], preferred_element_type=f32)
        xb[block(b), both] = o.astype(bf16)
        put(b, out, u)

    def ship_d(u):
        for m in range(2):
            send(po.at[3, u, m], rdi.at[u, m], s_rs.at[0], s_rd.at[u], to_y)

    def ship_1(u):
        for m in range(2):
            send(po.at[1, u, m], r1i.at[u, m], s_rs.at[1], s_r1.at[u], to_y)

    def chunk(j, _):
        fetch_chunk(j)

        @pl.when(j == first)
        def _():
            wait(xb.at[block(3), :], s_xd, "xd")

        @pl.when(j >= first)
        def _():
            load_chunk(j - first, 1)

        wait_chunk()

        def rows_of(n, _):
            g = 3 * j + n
            gate((n + 1) % 3, j, 0, g % 2, g >= 2)
            return 0

        lax.fori_loop(0, 3, rows_of, 0)
        load_local(j + 1)

        @pl.when(j + 1 == ne)
        def _():
            for n in range(2):
                hcopy(0, 0, n).wait()
            load(hb.at[block(1), ecols], xb.at[block(0), ecols], s_ld.at[0])
            wait(db.at[0], s_d1, "d1")
            load_early(0, 2)

        @pl.when(j >= first)
        def _():
            wait(wv.at[1], s_wv.at[1], "wv")
            gate(3, j - first, 1, 2, j > first)

        return 0

    lax.fori_loop(0, ne, chunk, 0)

    wait(xb.at[block(0), ecols], s_ld.at[0], "ld")

    def early(k, _):
        p = 2 - k % 2

        @pl.when(k + 1 < ns)
        def _():
            load_early(k + 1, 3 - p)

        wait(wv.at[p, ecols, :], s_wv.at[p], "wv")
        o = jnp.dot(xb[block(0), ecols], wv[p, ecols, :], preferred_element_type=f32)
        xb[block(0), both] = o.astype(bf16)
        put(0, 1, k)
        ship_1(k)
        return 0

    lax.fori_loop(0, ns, early, 0)

    done = ne - first + 2 * (nl - 2)

    def late(j, _):
        fetch_chunk(j)
        two = (j > ne) & (j < last)
        base = ne - first + 2 * (j - ne - 1)

        @pl.when(two)
        def _():
            for i in range(2):
                load_chunk(base + i, 1 + i)

        @pl.when(j == last)
        def _():
            load_chunk(done, 1)

        wait_chunk()
        hst[0] = gated(1, 0)
        load(hst.at[0], hy.at[j - ne], s_h.at[0])
        gate(2, j, 0, 1, j > ne)
        wait(hst.at[0], s_h.at[0], "h")
        send(hy.at[j - ne], hx.at[j - ne], s_rs.at[2], s_hx, to_y)

        @pl.when(j < last)
        def _():
            load_local(j + 1)

        @pl.when(two)
        def _():
            def old(i, _):
                wait(wv.at[1 + i], s_wv.at[1 + i], "wv")
                gate(3, base + i, 1 + i, 2)
                return 0

            lax.fori_loop(0, 2, old, 0)

        return 0

    lax.fori_loop(ne, nch, late, 0)
    for j in range(nl):
        load(hy.at[j], xb.at[block(0), pl.ds((ne + j) * CW, CW)], s_ld.at[0])
    hcopy(2, last, 1).wait()
    wait(xb.at[block(2), :], s_xs.at[2], "xs")
    load_h(2, 2)
    wait(wx.at[0], s_wx.at[0], "wx")
    send(wx.at[0], wx.at[1], s_ws.at[7], s_wx.at[1], to_mate)

    def diagonal(j, _):
        i = j - done
        p = jnp.where(j == last, 0, 1 + i % 2)

        @pl.when(j + 1 < last)
        def _():
            load_chunk(j + 1, 2 - i % 2)

        @pl.when(j < last)
        def _():
            wait(wv.at[p], s_wv.at[p], "wv")

        gate(3, j, p, 2 - i % 2, i != 1)
        return 0

    lax.fori_loop(done, nch, diagonal, 0)
    load_pair(0, 0, 1)
    for q in (1, 2):
        hcopy(3, last, q).wait()
    load_h(3, 3)
    wait(xb.at[block(0), pl.ds(ne * CW, nl * CW)], s_ld.at[0], "ld")
    wait_h(2)
    wait_h(3)
    for s in range(4):
        load(x.at[:, own_cols[s]], xb.at[block(1), slot(s)], s_loc)

    def forward_strip(k):
        wait(db.at[1, k], s_d2.at[k], "d2")
        send(db.at[1, k], db.at[2, k], s_ws.at[5], s_d3.at[k], to_mate)

    def own_half(k, _):
        p = 1 + k % 2

        @pl.when(k + 1 < ns)
        def _():
            load_pair(0, k + 1, 3 - p)

        wait_pair(p)

        def rows_of(n, _):
            down(3 - n, 3 - n, k, p)

            @pl.when(n == 0)
            def _():
                ship_d(k)

            return 0

        lax.fori_loop(0, 2, rows_of, 0)

        @pl.when(k == 1)
        def _():
            forward_strip(0)

        @pl.when(k + 1 == ns)
        def _():
            forward_strip(1)

        return 0

    lax.fori_loop(0, ns, own_half, 0)

    def total(tiles):
        o = xb[block(tiles[0][0]), pl.ds(fq + tiles[0][1] * CW, CW)].astype(f32)
        for b, c in tiles[1:]:
            o = o + xb[block(b), pl.ds(fq + c * CW, CW)].astype(f32)
        return o.astype(bf16)

    def ring_at(ring, m):
        b = jnp.where(ring == 0, 0, jnp.where(ring == 3, 3, 2))
        c = jnp.where(ring == 1, 2, 4)
        return block(b), pl.ds(col(fq + (c + m) * CW), CW)

    def ring_tile(ring, m):
        return xb.at[ring_at(ring, m)]

    def relay(half, k, m, turn):
        u = half * ns + k
        load(po.at[2, u, m], tile(0, 2), s_ld.at[0])
        if m == 0:
            wait(rdi.at[u], s_rd.at[u], "rd")
        load(rdi.at[u, m], tile(0, 3), s_ld.at[1])
        ring = turn % 4

        @pl.when(turn >= 4)
        def _():
            wait(ring_tile(ring, m), s_ys.at[2 * ring + m], "ys")

        wait(tile(0, 2), s_ld.at[0], "ld")
        wait(tile(0, 3), s_ld.at[1], "ld")
        xb[ring_at(ring, m)] = total(((0, 2), (0, 3)))
        v = (1 - half) * ns + k
        sem = v if m == 0 else jnp.where(v == ns - 1, 2 * ns, v)
        send(ring_tile(ring, m), yxi.at[v, m], s_ys.at[2 * ring + m], s_yx.at[sem], to_x)

    def fetch_pair(k):
        @pl.when(k >= 3)
        def _():
            forward_strip(k)

        wait(db.at[2, k], s_d3.at[k], "d3")
        load_pair(1, k, 1 + k % 2)

    def other_half(k, _):
        p = 1 + k % 2
        u = ns + k
        wait_pair(p)

        def rows_of(n, _):
            b = jnp.where(n == 0, 3, jnp.where(n == 1, 0, 2))
            down(b, jnp.where(n == 1, 1, b), u, p)

            @pl.when(n == 0)
            def _():
                ship_d(u)

            @pl.when((n == 1) & (k > 0))
            def _():
                ship_1(u - 1)

            return 0

        lax.fori_loop(0, 3, rows_of, 0)
        for m in range(2):
            relay(0, k, m, k)

        @pl.when(k == 0)
        def _():
            forward_strip(2)

        @pl.when(k + 1 < ns)
        def _():
            fetch_pair(k + 1)

        return 0

    fetch_pair(0)
    lax.fori_loop(0, ns, other_half, 0)
    ship_1(2 * ns - 1)

    load_chunk(ne, 1)
    wait(xb.at[block(1), :], s_loc, "loc")

    def own_late(j, _):
        i = j - ne
        p = jnp.where(j == last, 0, 1 + i % 2)

        @pl.when(j + 1 < last)
        def _():
            load_chunk(j + 1, 2 - i % 2)

        @pl.when(j < last)
        def _():
            wait(wv.at[p], s_wv.at[p], "wv")

        gate(1, j, p, i % 2, i > 1, 0)
        return 0

    lax.fori_loop(ne, nch, own_late, 0)

    long = pl.ds(0, fq + nl * CW)
    rest = pl.ds(fq, nl * CW)

    def load_long(k, p):
        load_pair(0, k, p)
        for m in range(2):
            load(wx.at[m, k], wv.at[p, rest, halves[m]], s_wv.at[p])

    for q in range(2):
        hcopy(0, last, q).wait()
    load_h(0, 1)
    wait(hx, s_hx, "hx")
    for j in range(nl):
        load(hx.at[j], xb.at[block(1), pl.ds(fq + j * CW, CW)], s_ld.at[3])
    wait(wx.at[1], s_wx.at[1], "wx")
    load_long(0, 1)
    wait_h(1)
    wait(xb.at[block(1), rest], s_ld.at[3], "ld")

    for m in range(2):
        relay(1, 0, m, ns)

    def own_rows(k, _):
        p = 1 + k % 2

        @pl.when(k + 1 < ns)
        def _():
            load_long(k + 1, 3 - p)

        wait(wv.at[p, long, :], s_wv.at[p], "wv")
        o = jnp.dot(xb[block(1), long], wv[p, long, :], preferred_element_type=f32)
        xb[block(0), both] = o.astype(bf16)
        put(0, 0, k)
        return 0

    lax.fori_loop(0, ns, own_rows, 0)
    load_pair(1, 0, 1)
    for m in range(2):
        relay(1, 1, m, ns + 1)

    def own_rows_too(k, _):
        p = 1 + k % 2

        @pl.when(k + 1 < ns)
        def _():
            load_pair(1, k + 1, 3 - p)

        wait_pair(p)
        down(1, 0, ns + k, p)
        return 0

    lax.fori_loop(0, ns, own_rows_too, 0)
    for m in range(2):
        relay(1, 2, m, ns + 2)

    parts = ((1, 2), (1, 3), (1, 4), (1, 5))

    def keep(half, k, m, o):
        wv[half, pl.ds(col(k * rows, rows), rows), halves[m]] = o

    def finish(half, k, m):
        u = half * ns + k
        n = 2 * half + m
        cols = pl.ds(col(quarter[n] * dk + k * CW), CW)
        load(po.at[0, u, m], tile(*parts[0]), s_ld.at[0])
        load(x.at[:, cols], tile(*parts[1]), s_ld.at[1])
        if m == 0:
            wait(r1i.at[u], s_r1.at[u], "r1")
        load(r1i.at[u, m], tile(*parts[2]), s_ld.at[2])
        if m == 0 and half == 1:
            wait(yxi.at[u], s_yx.at[u], "yx")
        if m == 0 and half == 0:
            @pl.when(k + 1 < ns)
            def _():
                wait(yxi.at[u], s_yx.at[u], "yx")

            @pl.when(k + 1 == ns)
            def _():
                wait(yxi.at[u, 0], s_yx.at[u], "yx")
        load(yxi.at[u, m], tile(*parts[3]), s_ld.at[3])
        for c in range(4):
            wait(tile(*parts[c]), s_ld.at[c], "ld")
        keep(half, k, m, total(parts))

    def begin():
        load(po.at[0, ns - 1, 1], tile(*parts[0]), s_ld.at[0])
        load(r1i.at[ns - 1, 1], tile(*parts[1]), s_ld.at[1])
        wait(tile(*parts[0]), s_ld.at[0], "ld")
        wait(tile(*parts[1]), s_ld.at[1], "ld")
        keep(0, ns - 1, 1, total(parts[:2]))

    def tail(k, _):
        @pl.when((k > 2) & (k < ns))
        def _():
            for m in range(2):
                relay(1, k, m, ns + k)

        @pl.when(k > 0)
        def _():
            finish(0, k - 1, 0)

            @pl.when(k < ns)
            def _():
                finish(0, k - 1, 1)

            @pl.when(k == ns)
            def _():
                begin()

            for m in range(2):
                finish(1, k - 1, m)

        return 0

    lax.fori_loop(0, ns + 1, tail, 0)

    for m in range(2):
        for ring in range(4):
            wait(ring_tile(ring, m), s_ys.at[2 * ring + m], "ys")
    wait(x, s_xs.at[0], "xs")
    wait(x, s_xs.at[1], "xs")
    wait(w1, s_ws.at[0], "ws")
    wait(w2, s_ws.at[1], "ws")
    wait(db.at[0], s_ws.at[2], "ws")
    wait(db.at[1], s_ws.at[3], "ws")
    wait(w3, s_ws.at[4], "ws")
    wait(db.at[2], s_ws.at[5], "ws")
    wait(wx.at[0], s_ws.at[6], "ws")
    wait(wx.at[1], s_ws.at[7], "ws")
    wait(rdi, s_rs.at[0], "rs")
    wait(r1i, s_rs.at[1], "rs")
    wait(hx, s_rs.at[2], "rs")
    wait(yxi.at[ns - 1, 1], s_yx.at[2 * ns], "yx")


def write(x, done, yxi, y, strip, s_in, s_out):
    rows, dim = x.shape
    dk = dim // 4
    ns = dk // CW
    d = lax.axis_index("dp")
    mate = d + 1 - 2 * (d % 2)
    quarter = [d, mate, (d + 2) % 4, (mate + 2) % 4]

    def cols(half, k, m):
        return pl.ds(pl.multiple_of(quarter[2 * half + m] * dk + k * CW, 128), CW)

    def kept(half, k, m):
        return done.at[half, pl.ds(k * rows, rows), pl.ds(m * CW, CW)]

    end = (0, ns - 1, 1)
    loads = [pltpu.make_async_copy(src, strip.at[i], s_in.at[i])
             for i, src in enumerate((x.at[:, cols(*end)], yxi.at[ns - 1, 1]))]
    for copy in loads:
        copy.start()
    strips = [(half, k, m) for k in range(ns) for half in range(2) for m in range(2)]
    strips.remove(end)
    outs = [pltpu.make_async_copy(kept(*i), y.at[:, cols(*i)], s_out.at[n]) for n, i in enumerate(strips)]
    for copy in outs:
        copy.start()
    for copy in loads:
        copy.wait()
    o = kept(*end)[...].astype(jnp.float32) + strip[1].astype(jnp.float32) + strip[0].astype(jnp.float32)
    strip[2] = o.astype(strip.dtype)
    outs.append(pltpu.make_async_copy(strip.at[2], y.at[:, cols(*end)], s_out.at[len(strips)]))
    outs[-1].start()
    for copy in outs:
        copy.wait()


def solution(mesh):
    def body(x, wg, wu, wd):
        rows, dim = x.shape
        dk = dim // 4
        fq = wg.shape[1] // 2
        nch = fq // CW
        nl = late_chunks(nch)
        ns = dk // CW
        bf16 = jnp.bfloat16
        dma = pltpu.SemaphoreType.DMA
        pairs = (2 * ns, 2, rows, CW)
        shapes = [
            (nch, dk, 2 * CW), (nch, dk, 2 * CW), (nch, dk, 2 * CW),
            (3, ns, fq, CW),
            (4 * rows, fq),
            (4,) + pairs, pairs, pairs, pairs,
            (nl, rows, CW), (nl, rows, CW),
            (2, ns, nl * CW, CW),
        ]
        any_space = pl.BlockSpec(memory_space=pl.ANY)
        in_vmem = pl.BlockSpec(memory_space=pltpu.VMEM)
        outs = pl.pallas_call(
            kernel,
            out_shape=[pltpu.VMEM((3, dim, 2 * CW), bf16)] + [jax.ShapeDtypeStruct(s, bf16) for s in shapes],
            in_specs=[any_space] * 4,
            out_specs=[in_vmem] + [any_space] * len(shapes),
            scratch_shapes=[
                pltpu.VMEM((4 * rows, dim), bf16),
                pltpu.VMEM((3, rows, CW), bf16),
                dma, dma((3,)), dma((8,)), dma((4,)), dma, dma,
                dma, dma((nch,)), dma((nch,)), dma, dma((ns,)), dma((ns,)), dma((2,)), dma,
                dma((4,)), dma((3,)), dma, dma((3,)),
                dma((2 * ns,)), dma((2 * ns,)), dma((2 * ns + 1,)), dma((8,)), dma((4,)),
            ],
            compiler_params=pltpu.CompilerParams(
                collective_id=0, has_side_effects=True, vmem_limit_bytes=48 * 2**20),
            cost_estimate=pl.CostEstimate(
                flops=6 * rows * 4 * dim * fq, bytes_accessed=4 * rows * dim * 2, transcendentals=0),
        )(x, wg, wu, wd)
        return pl.pallas_call(
            write,
            out_shape=jax.ShapeDtypeStruct((rows, dim), bf16),
            in_specs=[any_space, in_vmem, any_space],
            out_specs=any_space,
            scratch_shapes=[pltpu.VMEM((3, rows, CW), bf16), dma((2,)), dma((4 * ns,))],
            compiler_params=pltpu.CompilerParams(vmem_limit_bytes=48 * 2**20),
        )(x, pltpu.with_memory_space_constraint(outs[0], pltpu.VMEM), outs[9])

    return jax.shard_map(body, mesh=mesh, in_specs=(P(("dp", "tp"), None), P("dp", "tp"), P("dp", "tp"), P("tp", "dp")), out_specs=P(("dp", "tp"), None), check_vma=False)
```

```python
import jax
import jax.numpy as jnp
from jax import lax
from jax.experimental import pallas as pl
from jax.experimental.pallas import tpu as pltpu
from jax.sharding import PartitionSpec as P

CW = 256


def late_chunks(nch):
    return min(4, nch // 3)


def kernel(x, wg, wu, wd, wv, w1, w2, w3, db, hb, po, rdi, r1i, yxi, hy, hx, wx,
           xb, hst, s_loc, s_xs, s_ws, s_xx, s_xy, s_xd, s_w1, s_w2, s_w3, s_d1, s_d2, s_d3, s_wx, s_hx,
           s_wv, s_h, s_po, s_rs, s_rd, s_r1, s_yx, s_ys, s_ld):
    rows, dim = x.shape
    dk = dim // 4
    fq = wg.shape[1] // 2
    nch = fq // CW
    first = nch // 2
    nl = late_chunks(nch)
    ne = nch - nl
    last = nch - 1
    ns = dk // CW
    f32, bf16 = jnp.float32, jnp.bfloat16

    t = lax.axis_index("tp")
    d = lax.axis_index("dp")
    side = d // 2
    core = d % 2
    mate = d + 1 - 2 * core
    quarter = [d, mate, (d + 2) % 4, (mate + 2) % 4]
    to_mate = {"dp": mate}
    to_x = {"dp": (d + 2) % 4}
    to_y = {"tp": 1 - t}

    def col(v, size=128):
        return v if isinstance(v, int) else pl.multiple_of(v, size)

    def send(src, dst, send_sem, recv_sem, where):
        pltpu.make_async_remote_copy(
            src_ref=src, dst_ref=dst, send_sem=send_sem, recv_sem=recv_sem,
            device_id=where, device_id_type=pl.DeviceIdType.MESH).start()

    def load(src, dst, sem):
        pltpu.make_async_copy(src, dst, sem).start()

    def wait(ref, sem):
        pltpu.make_async_copy(ref, ref, sem).wait()

    def block(b):
        return pl.ds(col(b * rows, rows), rows)

    def slot(s):
        return pl.ds(s * dk, dk)

    def piece(k):
        return pl.ds(col(k * CW), CW)

    barrier = pltpu.get_barrier_semaphore()
    for where in (to_mate, to_x, to_y):
        pl.semaphore_signal(barrier, inc=1, device_id=where, device_id_type=pl.DeviceIdType.MESH)
    pl.semaphore_wait(barrier, 3)

    own_cols = [pl.ds(col(quarter[s] * dk), dk) for s in range(4)]
    for s in range(4):
        src = x.at[:, own_cols[s]]
        send(src, xb.at[block(2), slot(s ^ 2)], s_xs.at[0], s_xx.at[s ^ 2], to_x)
        send(src, xb.at[block(1), slot(s)], s_xs.at[1], s_xy, to_y)
    for s in range(4):
        load(x.at[:, own_cols[s]], xb.at[block(0), slot(s)], s_loc)

    def send_chunk(j, _):
        for m, w in enumerate((wg, wu)):
            away = w.at[:, pl.ds(col((1 - side) * fq + j * CW), CW)]
            here = w.at[:, pl.ds(col(side * fq + j * CW), CW)]
            send(away, w2.at[j, :, pl.ds(m * CW, CW)], s_ws.at[1], s_w2.at[j], to_x)
            send(here, w1.at[j, :, pl.ds(m * CW, CW)], s_ws.at[0], s_w1, to_mate)
        return 0

    lax.fori_loop(0, nch, send_chunk, 0)

    def send_strip(k, _):
        send(wd.at[pl.ds(col((1 - side) * fq), fq), piece(k)], db.at[1, k], s_ws.at[3], s_d2.at[k], to_x)
        send(wd.at[pl.ds(col(side * fq), fq), piece(k)], db.at[0, k], s_ws.at[2], s_d1, to_mate)
        return 0

    lax.fori_loop(0, ns, send_strip, 0)

    for s in (2, 3, 0, 1):
        part = xb.at[block(2), slot(s)]
        wait(part, s_xx.at[s])
        send(part, xb.at[block(3), slot(s)], s_xs.at[2], s_xd, to_y)

    def send_rest(k, _):
        send(wd.at[pl.ds(col(side * fq + ne * CW), nl * CW), piece(k)], wx.at[0, k], s_ws.at[6], s_wx.at[0], to_y)
        return 0

    lax.fori_loop(0, ns, send_rest, 0)

    at_hand, to_come = pl.ds(0, 2 * dk), pl.ds(2 * dk, 2 * dk)

    def load_here(j, p, sem):
        for m, w in enumerate((wg, wu)):
            here = w.at[:, pl.ds(col(side * fq + j * CW), CW)]
            load(here, wv.at[p, slot(0), pl.ds(m * CW, CW)], s_wv.at[sem])

    def load_slot(w, j, n, p, sem):
        load(w.at[j], wv.at[p, slot(n)], s_wv.at[sem])

    def load_chunk(j, p):
        load_here(j, p, p)
        for n, w in ((1, w1), (2, w2), (3, w3)):
            load_slot(w, j, n, p, p)

    def load_local(j):
        load_here(j, 0, 3)
        load_slot(w1, j, 1, 0, 3)

    def fetch_chunk(j):
        wait(w2.at[j], s_w2.at[j])
        send(w2.at[j], w3.at[j], s_ws.at[4], s_w3.at[j], to_mate)
        load_slot(w2, j, 2, 0, 0)
        wait(w3.at[j], s_w3.at[j])
        load_slot(w3, j, 3, 0, 0)

    def wait_chunk():
        wait(wv.at[0, at_hand, :], s_wv.at[3])
        wait(wv.at[0, to_come, :], s_wv.at[0])

    def hcopy(b, j, q):
        return pltpu.make_async_copy(hst.at[q], hb.at[block(b), piece(j)], s_h.at[q])

    def gated(b, p):
        ab = jnp.dot(xb[block(b), :], wv[p], preferred_element_type=f32)
        a = ab[:, :CW]
        return (a * jax.nn.sigmoid(a) * ab[:, CW:]).astype(bf16)

    def gate(b, j, p, q, used=True, to=None):
        to = b if to is None else to

        @pl.when(used)
        def _():
            hcopy(to, j, q).wait()

        hst[q] = gated(b, p)
        hcopy(to, j, q).start()

    wait(xb.at[block(0), :], s_loc)
    wait(xb.at[block(1), :], s_xy)
    wait(w1, s_w1)
    load_local(0)

    hcols = pl.ds(0, fq)
    ecols = pl.ds(0, ne * CW)
    both = pl.ds(fq, 2 * CW)

    def load_h(b, to):
        load(hb.at[block(b), :], xb.at[block(to), hcols], s_ld.at[to])

    def wait_h(to):
        wait(xb.at[block(to), hcols], s_ld.at[to])

    def tile(b, c, n=1):
        return xb.at[block(b), pl.ds(fq + c * CW, n * CW)]

    halves = (pl.ds(0, CW), pl.ds(CW, CW))

    def load_early(k, p):
        load(wd.at[pl.ds(col(side * fq), ne * CW), piece(k)], wv.at[p, ecols, halves[0]], s_wv.at[p])
        load(db.at[0, k, ecols, :], wv.at[p, ecols, halves[1]], s_wv.at[p])

    def load_pair(half, k, p):
        if half == 0:
            src = (wd.at[pl.ds(col(side * fq), fq), piece(k)], db.at[0, k])
        else:
            src = (db.at[1, k], db.at[2, k])
        for m in range(2):
            load(src[m], wv.at[p, hcols, halves[m]], s_wv.at[p])

    def wait_pair(p):
        wait(wv.at[p, hcols, :], s_wv.at[p])

    def put(b, out, u):
        for m in range(2):
            load(tile(b, m), po.at[out, u, m], s_po)
        wait(tile(b, 0, 2), s_po)

    def down(b, out, u, p):
        o = jnp.dot(xb[block(b), hcols], wv[p, hcols, :], preferred_element_type=f32)
        xb[block(b), both] = o.astype(bf16)
        put(b, out, u)

    def ship_d(u):
        for m in range(2):
            send(po.at[3, u, m], rdi.at[u, m], s_rs.at[0], s_rd.at[u], to_y)

    def ship_1(u):
        for m in range(2):
            send(po.at[1, u, m], r1i.at[u, m], s_rs.at[1], s_r1.at[u], to_y)

    def chunk(j, _):
        fetch_chunk(j)

        @pl.when(j == first)
        def _():
            wait(xb.at[block(3), :], s_xd)

        @pl.when(j >= first)
        def _():
            load_chunk(j - first, 1)

        wait_chunk()

        def rows_of(n, _):
            g = 3 * j + n
            gate((n + 1) % 3, j, 0, g % 2, g >= 2)
            return 0

        lax.fori_loop(0, 3, rows_of, 0)
        load_local(j + 1)

        @pl.when(j + 1 == ne)
        def _():
            for n in range(2):
                hcopy(0, 0, n).wait()
            load(hb.at[block(1), ecols], xb.at[block(0), ecols], s_ld.at[0])
            wait(db.at[0], s_d1)
            load_early(0, 2)

        @pl.when(j >= first)
        def _():
            wait(wv.at[1], s_wv.at[1])
            gate(3, j - first, 1, 2, j > first)

        return 0

    lax.fori_loop(0, ne, chunk, 0)

    wait(xb.at[block(0), ecols], s_ld.at[0])

    def early(k, _):
        p = 2 - k % 2

        @pl.when(k + 1 < ns)
        def _():
            load_early(k + 1, 3 - p)

        wait(wv.at[p, ecols, :], s_wv.at[p])
        o = jnp.dot(xb[block(0), ecols], wv[p, ecols, :], preferred_element_type=f32)
        xb[block(0), both] = o.astype(bf16)
        put(0, 1, k)
        ship_1(k)
        return 0

    lax.fori_loop(0, ns, early, 0)

    done = ne - first + 2 * (nl - 2)

    def late(j, _):
        fetch_chunk(j)
        two = (j > ne) & (j < last)
        base = ne - first + 2 * (j - ne - 1)

        @pl.when(two)
        def _():
            for i in range(2):
                load_chunk(base + i, 1 + i)

        @pl.when(j == last)
        def _():
            load_chunk(done, 1)

        wait_chunk()
        hst[0] = gated(1, 0)
        load(hst.at[0], hy.at[j - ne], s_h.at[0])
        gate(2, j, 0, 1, j > ne)
        wait(hst.at[0], s_h.at[0])
        send(hy.at[j - ne], hx.at[j - ne], s_rs.at[2], s_hx, to_y)

        @pl.when(j < last)
        def _():
            load_local(j + 1)

        @pl.when(two)
        def _():
            def old(i, _):
                wait(wv.at[1 + i], s_wv.at[1 + i])
                gate(3, base + i, 1 + i, 2)
                return 0

            lax.fori_loop(0, 2, old, 0)

        return 0

    lax.fori_loop(ne, nch, late, 0)
    for j in range(nl):
        load(hy.at[j], xb.at[block(0), pl.ds((ne + j) * CW, CW)], s_ld.at[0])
    hcopy(2, last, 1).wait()
    wait(xb.at[block(2), :], s_xs.at[2])
    load_h(2, 2)
    wait(wx.at[0], s_wx.at[0])
    send(wx.at[0], wx.at[1], s_ws.at[7], s_wx.at[1], to_mate)

    def diagonal(j, _):
        i = j - done
        p = jnp.where(j == last, 0, 1 + i % 2)

        @pl.when(j + 1 < last)
        def _():
            load_chunk(j + 1, 2 - i % 2)

        @pl.when(j < last)
        def _():
            wait(wv.at[p], s_wv.at[p])

        gate(3, j, p, 2 - i % 2, i != 1)
        return 0

    lax.fori_loop(done, nch, diagonal, 0)
    load_pair(0, 0, 1)
    for q in (1, 2):
        hcopy(3, last, q).wait()
    load_h(3, 3)
    wait(xb.at[block(0), pl.ds(ne * CW, nl * CW)], s_ld.at[0])
    wait_h(2)
    wait_h(3)
    for s in range(4):
        load(x.at[:, own_cols[s]], xb.at[block(1), slot(s)], s_loc)

    def forward_strip(k):
        wait(db.at[1, k], s_d2.at[k])
        send(db.at[1, k], db.at[2, k], s_ws.at[5], s_d3.at[k], to_mate)

    def own_half(k, _):
        p = 1 + k % 2

        @pl.when(k + 1 < ns)
        def _():
            load_pair(0, k + 1, 3 - p)

        wait_pair(p)

        def rows_of(n, _):
            down(3 - n, 3 - n, k, p)

            @pl.when(n == 0)
            def _():
                ship_d(k)

            return 0

        lax.fori_loop(0, 2, rows_of, 0)

        @pl.when(k == 1)
        def _():
            forward_strip(0)

        @pl.when(k + 1 == ns)
        def _():
            forward_strip(1)

        return 0

    lax.fori_loop(0, ns, own_half, 0)

    def total(tiles):
        o = xb[block(tiles[0][0]), pl.ds(fq + tiles[0][1] * CW, CW)].astype(f32)
        for b, c in tiles[1:]:
            o = o + xb[block(b), pl.ds(fq + c * CW, CW)].astype(f32)
        return o.astype(bf16)

    def ring_at(ring, m):
        b = jnp.where(ring == 0, 0, jnp.where(ring == 3, 3, 2))
        c = jnp.where(ring == 1, 2, 4)
        return block(b), pl.ds(col(fq + (c + m) * CW), CW)

    def ring_tile(ring, m):
        return xb.at[ring_at(ring, m)]

    def relay(half, k, m, turn):
        u = half * ns + k
        load(po.at[2, u, m], tile(0, 2), s_ld.at[0])
        if m == 0:
            wait(rdi.at[u], s_rd.at[u])
        load(rdi.at[u, m], tile(0, 3), s_ld.at[1])
        ring = turn % 4

        @pl.when(turn >= 4)
        def _():
            wait(ring_tile(ring, m), s_ys.at[2 * ring + m])

        wait(tile(0, 2), s_ld.at[0])
        wait(tile(0, 3), s_ld.at[1])
        xb[ring_at(ring, m)] = total(((0, 2), (0, 3)))
        v = (1 - half) * ns + k
        sem = v if m == 0 else jnp.where(v == ns - 1, 2 * ns, v)
        send(ring_tile(ring, m), yxi.at[v, m], s_ys.at[2 * ring + m], s_yx.at[sem], to_x)

    def fetch_pair(k):
        @pl.when(k >= 3)
        def _():
            forward_strip(k)

        wait(db.at[2, k], s_d3.at[k])
        load_pair(1, k, 1 + k % 2)

    def other_half(k, _):
        p = 1 + k % 2
        u = ns + k
        wait_pair(p)

        def rows_of(n, _):
            b = jnp.where(n == 0, 3, jnp.where(n == 1, 0, 2))
            down(b, jnp.where(n == 1, 1, b), u, p)

            @pl.when(n == 0)
            def _():
                ship_d(u)

            @pl.when((n == 1) & (k > 0))
            def _():
                ship_1(u - 1)

            return 0

        lax.fori_loop(0, 3, rows_of, 0)
        for m in range(2):
            relay(0, k, m, k)

        @pl.when(k == 0)
        def _():
            forward_strip(2)

        @pl.when(k + 1 < ns)
        def _():
            fetch_pair(k + 1)

        return 0

    fetch_pair(0)
    lax.fori_loop(0, ns, other_half, 0)
    ship_1(2 * ns - 1)

    load_chunk(ne, 1)
    wait(xb.at[block(1), :], s_loc)

    def own_late(j, _):
        i = j - ne
        p = jnp.where(j == last, 0, 1 + i % 2)

        @pl.when(j + 1 < last)
        def _():
            load_chunk(j + 1, 2 - i % 2)

        @pl.when(j < last)
        def _():
            wait(wv.at[p], s_wv.at[p])

        gate(1, j, p, i % 2, i > 1, 0)
        return 0

    lax.fori_loop(ne, nch, own_late, 0)

    long = pl.ds(0, fq + nl * CW)
    rest = pl.ds(fq, nl * CW)

    def load_long(k, p):
        load_pair(0, k, p)
        for m in range(2):
            load(wx.at[m, k], wv.at[p, rest, halves[m]], s_wv.at[p])

    for q in range(2):
        hcopy(0, last, q).wait()
    load_h(0, 1)
    wait(hx, s_hx)
    for j in range(nl):
        load(hx.at[j], xb.at[block(1), pl.ds(fq + j * CW, CW)], s_ld.at[3])
    wait(wx.at[1], s_wx.at[1])
    load_long(0, 1)
    wait_h(1)
    wait(xb.at[block(1), rest], s_ld.at[3])

    for m in range(2):
        relay(1, 0, m, ns)

    def own_rows(k, _):
        p = 1 + k % 2

        @pl.when(k + 1 < ns)
        def _():
            load_long(k + 1, 3 - p)

        wait(wv.at[p, long, :], s_wv.at[p])
        o = jnp.dot(xb[block(1), long], wv[p, long, :], preferred_element_type=f32)
        xb[block(0), both] = o.astype(bf16)
        put(0, 0, k)
        return 0

    lax.fori_loop(0, ns, own_rows, 0)
    load_pair(1, 0, 1)
    for m in range(2):
        relay(1, 1, m, ns + 1)

    def own_rows_too(k, _):
        p = 1 + k % 2

        @pl.when(k + 1 < ns)
        def _():
            load_pair(1, k + 1, 3 - p)

        wait_pair(p)
        down(1, 0, ns + k, p)
        return 0

    lax.fori_loop(0, ns, own_rows_too, 0)
    for m in range(2):
        relay(1, 2, m, ns + 2)

    parts = ((1, 2), (1, 3), (1, 4), (1, 5))

    def keep(half, k, m, o):
        wv[half, pl.ds(col(k * rows, rows), rows), halves[m]] = o

    def finish(half, k, m):
        u = half * ns + k
        n = 2 * half + m
        cols = pl.ds(col(quarter[n] * dk + k * CW), CW)
        load(po.at[0, u, m], tile(*parts[0]), s_ld.at[0])
        load(x.at[:, cols], tile(*parts[1]), s_ld.at[1])
        if m == 0:
            wait(r1i.at[u], s_r1.at[u])
        load(r1i.at[u, m], tile(*parts[2]), s_ld.at[2])
        if m == 0 and half == 1:
            wait(yxi.at[u], s_yx.at[u])
        if m == 0 and half == 0:
            @pl.when(k + 1 < ns)
            def _():
                wait(yxi.at[u], s_yx.at[u])

            @pl.when(k + 1 == ns)
            def _():
                wait(yxi.at[u, 0], s_yx.at[u])
        load(yxi.at[u, m], tile(*parts[3]), s_ld.at[3])
        for c in range(4):
            wait(tile(*parts[c]), s_ld.at[c])
        keep(half, k, m, total(parts))

    def begin():
        load(po.at[0, ns - 1, 1], tile(*parts[0]), s_ld.at[0])
        load(r1i.at[ns - 1, 1], tile(*parts[1]), s_ld.at[1])
        wait(tile(*parts[0]), s_ld.at[0])
        wait(tile(*parts[1]), s_ld.at[1])
        keep(0, ns - 1, 1, total(parts[:2]))

    def tail(k, _):
        @pl.when((k > 2) & (k < ns))
        def _():
            for m in range(2):
                relay(1, k, m, ns + k)

        @pl.when(k > 0)
        def _():
            finish(0, k - 1, 0)

            @pl.when(k < ns)
            def _():
                finish(0, k - 1, 1)

            @pl.when(k == ns)
            def _():
                begin()

            for m in range(2):
                finish(1, k - 1, m)

        return 0

    lax.fori_loop(0, ns + 1, tail, 0)

    for m in range(2):
        for ring in range(4):
            wait(ring_tile(ring, m), s_ys.at[2 * ring + m])
    wait(x, s_xs.at[0])
    wait(x, s_xs.at[1])
    wait(w1, s_ws.at[0])
    wait(w2, s_ws.at[1])
    wait(db.at[0], s_ws.at[2])
    wait(db.at[1], s_ws.at[3])
    wait(w3, s_ws.at[4])
    wait(db.at[2], s_ws.at[5])
    wait(wx.at[0], s_ws.at[6])
    wait(wx.at[1], s_ws.at[7])
    wait(rdi, s_rs.at[0])
    wait(r1i, s_rs.at[1])
    wait(hx, s_rs.at[2])
    wait(yxi.at[ns - 1, 1], s_yx.at[2 * ns])


def write(x, done, yxi, y, strip, s_in, s_out):
    rows, dim = x.shape
    dk = dim // 4
    ns = dk // CW
    d = lax.axis_index("dp")
    mate = d + 1 - 2 * (d % 2)
    quarter = [d, mate, (d + 2) % 4, (mate + 2) % 4]

    def cols(half, k, m):
        return pl.ds(pl.multiple_of(quarter[2 * half + m] * dk + k * CW, 128), CW)

    def kept(half, k, m):
        return done.at[half, pl.ds(k * rows, rows), pl.ds(m * CW, CW)]

    end = (0, ns - 1, 1)
    loads = [pltpu.make_async_copy(src, strip.at[i], s_in.at[i])
             for i, src in enumerate((x.at[:, cols(*end)], yxi.at[ns - 1, 1]))]
    for copy in loads:
        copy.start()
    strips = [(half, k, m) for k in range(ns) for half in range(2) for m in range(2)]
    strips.remove(end)
    outs = [pltpu.make_async_copy(kept(*i), y.at[:, cols(*i)], s_out.at[n]) for n, i in enumerate(strips)]
    for copy in outs:
        copy.start()
    for copy in loads:
        copy.wait()
    o = kept(*end)[...].astype(jnp.float32) + strip[1].astype(jnp.float32) + strip[0].astype(jnp.float32)
    strip[2] = o.astype(strip.dtype)
    outs.append(pltpu.make_async_copy(strip.at[2], y.at[:, cols(*end)], s_out.at[len(strips)]))
    outs[-1].start()
    for copy in outs:
        copy.wait()


def solution(mesh):
    def body(x, wg, wu, wd):
        rows, dim = x.shape
        dk = dim // 4
        fq = wg.shape[1] // 2
        nch = fq // CW
        nl = late_chunks(nch)
        ns = dk // CW
        bf16 = jnp.bfloat16
        dma = pltpu.SemaphoreType.DMA
        pairs = (2 * ns, 2, rows, CW)
        shapes = [
            (nch, dk, 2 * CW), (nch, dk, 2 * CW), (nch, dk, 2 * CW),
            (3, ns, fq, CW),
            (4 * rows, fq),
            (4,) + pairs, pairs, pairs, pairs,
            (nl, rows, CW), (nl, rows, CW),
            (2, ns, nl * CW, CW),
        ]
        any_space = pl.BlockSpec(memory_space=pl.ANY)
        in_vmem = pl.BlockSpec(memory_space=pltpu.VMEM)
        outs = pl.pallas_call(
            kernel,
            out_shape=[pltpu.VMEM((3, dim, 2 * CW), bf16)] + [jax.ShapeDtypeStruct(s, bf16) for s in shapes],
            in_specs=[any_space] * 4,
            out_specs=[in_vmem] + [any_space] * len(shapes),
            scratch_shapes=[
                pltpu.VMEM((4 * rows, dim), bf16),
                pltpu.VMEM((3, rows, CW), bf16),
                dma, dma((3,)), dma((8,)), dma((4,)), dma, dma,
                dma, dma((nch,)), dma((nch,)), dma, dma((ns,)), dma((ns,)), dma((2,)), dma,
                dma((4,)), dma((3,)), dma, dma((3,)),
                dma((2 * ns,)), dma((2 * ns,)), dma((2 * ns + 1,)), dma((8,)), dma((4,)),
            ],
            compiler_params=pltpu.CompilerParams(
                collective_id=0, has_side_effects=True, vmem_limit_bytes=48 * 2**20),
            cost_estimate=pl.CostEstimate(
                flops=6 * rows * 4 * dim * fq, bytes_accessed=4 * rows * dim * 2, transcendentals=0),
        )(x, wg, wu, wd)
        return pl.pallas_call(
            write,
            out_shape=jax.ShapeDtypeStruct((rows, dim), bf16),
            in_specs=[any_space, in_vmem, any_space],
            out_specs=any_space,
            scratch_shapes=[pltpu.VMEM((3, rows, CW), bf16), dma((2,)), dma((4 * ns,))],
            compiler_params=pltpu.CompilerParams(vmem_limit_bytes=48 * 2**20),
        )(x, pltpu.with_memory_space_constraint(outs[0], pltpu.VMEM), outs[9])

    return jax.shard_map(body, mesh=mesh, in_specs=(P(("dp", "tp"), None), P("dp", "tp"), P("dp", "tp"), P("tp", "dp")), out_specs=P(("dp", "tp"), None), check_vma=False)
```

```python
import jax
import jax.numpy as jnp
from jax import lax
from jax.experimental import pallas as pl
from jax.experimental.pallas import tpu as pltpu
from jax.sharding import PartitionSpec as P

CW = 256


def late_chunks(nch):
    return min(4, nch // 3)


def kernel(x, wg, wu, wd, wv, w1, w2, w3, db, hb, po, rdi, r1i, yxi, hy, hx, wx,
           xb, hst, s_loc, s_xs, s_ws, s_xx, s_xy, s_xd, s_w1, s_w2, s_w3, s_d1, s_d2, s_d3, s_wx, s_hx,
           s_wv, s_h, s_po, s_rs, s_rd, s_r1, s_yx, s_ys, s_ld):
    rows, dim = x.shape
    dk = dim // 4
    fq = wg.shape[1] // 2
    nch = fq // CW
    first = nch // 2
    nl = late_chunks(nch)
    ne = nch - nl
    last = nch - 1
    ns = dk // CW
    f32, bf16 = jnp.float32, jnp.bfloat16

    t = lax.axis_index("tp")
    d = lax.axis_index("dp")
    side = d // 2
    core = d % 2
    mate = d + 1 - 2 * core
    quarter = [d, mate, (d + 2) % 4, (mate + 2) % 4]
    to_mate = {"dp": mate}
    to_x = {"dp": (d + 2) % 4}
    to_y = {"tp": 1 - t}

    def col(v, size=128):
        return v if isinstance(v, int) else pl.multiple_of(v, size)

    def send(src, dst, send_sem, recv_sem, where):
        pltpu.make_async_remote_copy(
            src_ref=src, dst_ref=dst, send_sem=send_sem, recv_sem=recv_sem,
            device_id=where, device_id_type=pl.DeviceIdType.MESH).start()

    def load(src, dst, sem):
        pltpu.make_async_copy(src, dst, sem).start()

    def wait(ref, sem):
        pltpu.make_async_copy(ref, ref, sem).wait()

    def block(b):
        return pl.ds(col(b * rows, rows), rows)

    def slot(s):
        return pl.ds(s * dk, dk)

    def piece(k):
        return pl.ds(col(k * CW), CW)

    barrier = pltpu.get_barrier_semaphore()
    for where in (to_mate, to_x, to_y):
        pl.semaphore_signal(barrier, inc=1, device_id=where, device_id_type=pl.DeviceIdType.MESH)
    pl.semaphore_wait(barrier, 3)

    own_cols = [pl.ds(col(quarter[s] * dk), dk) for s in range(4)]
    for s in range(4):
        src = x.at[:, own_cols[s]]
        send(src, xb.at[block(2), slot(s ^ 2)], s_xs.at[0], s_xx.at[s ^ 2], to_x)
        send(src, xb.at[block(1), slot(s)], s_xs.at[1], s_xy, to_y)
    for s in range(4):
        load(x.at[:, own_cols[s]], xb.at[block(0), slot(s)], s_loc)

    def send_chunk(j, _):
        for m, w in enumerate((wg, wu)):
            away = w.at[:, pl.ds(col((1 - side) * fq + j * CW), CW)]
            here = w.at[:, pl.ds(col(side * fq + j * CW), CW)]
            send(away, w2.at[j, :, pl.ds(m * CW, CW)], s_ws.at[1], s_w2.at[j], to_x)
            send(here, w1.at[j, :, pl.ds(m * CW, CW)], s_ws.at[0], s_w1, to_mate)
        return 0

    lax.fori_loop(0, nch, send_chunk, 0)

    def send_strip(k, _):
        send(wd.at[pl.ds(col((1 - side) * fq), fq), piece(k)], db.at[1, k], s_ws.at[3], s_d2.at[k], to_x)
        send(wd.at[pl.ds(col(side * fq), fq), piece(k)], db.at[0, k], s_ws.at[2], s_d1, to_mate)
        return 0

    lax.fori_loop(0, ns, send_strip, 0)

    for s in (2, 3, 0, 1):
        part = xb.at[block(2), slot(s)]
        wait(part, s_xx.at[s])
        send(part, xb.at[block(3), slot(s)], s_xs.at[2], s_xd, to_y)

    def send_rest(k, _):
        send(wd.at[pl.ds(col(side * fq + ne * CW), nl * CW), piece(k)], wx.at[0, k], s_ws.at[6], s_wx.at[0], to_y)
        return 0

    lax.fori_loop(0, ns, send_rest, 0)

    at_hand, to_come = pl.ds(0, 2 * dk), pl.ds(2 * dk, 2 * dk)

    def load_here(j, p, sem):
        for m, w in enumerate((wg, wu)):
            here = w.at[:, pl.ds(col(side * fq + j * CW), CW)]
            load(here, wv.at[p, slot(0), pl.ds(m * CW, CW)], s_wv.at[sem])

    def load_slot(w, j, n, p, sem):
        load(w.at[j], wv.at[p, slot(n)], s_wv.at[sem])

    def load_chunk(j, p):
        load_here(j, p, p)
        for n, w in ((1, w1), (2, w2), (3, w3)):
            load_slot(w, j, n, p, p)

    def load_local(j):
        load_here(j, 0, 3)
        load_slot(w1, j, 1, 0, 3)

    def fetch_chunk(j):
        wait(w2.at[j], s_w2.at[j])
        send(w2.at[j], w3.at[j], s_ws.at[4], s_w3.at[j], to_mate)
        load_slot(w2, j, 2, 0, 0)
        wait(w3.at[j], s_w3.at[j])
        load_slot(w3, j, 3, 0, 0)

    def wait_chunk():
        wait(wv.at[0, at_hand, :], s_wv.at[3])
        wait(wv.at[0, to_come, :], s_wv.at[0])

    def hcopy(b, j, q):
        return pltpu.make_async_copy(hst.at[q], hb.at[block(b), piece(j)], s_h.at[q])

    def gated(b, p):
        ab = jnp.dot(xb[block(b), :], wv[p], preferred_element_type=f32)
        a = ab[:, :CW]
        return (a * jax.nn.sigmoid(a) * ab[:, CW:]).astype(bf16)

    def gate(b, j, p, q, used=True, to=None):
        to = b if to is None else to

        @pl.when(used)
        def _():
            hcopy(to, j, q).wait()

        hst[q] = gated(b, p)
        hcopy(to, j, q).start()

    wait(xb.at[block(0), :], s_loc)
    wait(xb.at[block(1), :], s_xy)
    wait(w1, s_w1)
    load_local(0)

    hcols = pl.ds(0, fq)
    ecols = pl.ds(0, ne * CW)
    both = pl.ds(fq, 2 * CW)

    def load_h(b, to):
        load(hb.at[block(b), :], xb.at[block(to), hcols], s_ld.at[to])

    def wait_h(to):
        wait(xb.at[block(to), hcols], s_ld.at[to])

    def tile(b, c, n=1):
        return xb.at[block(b), pl.ds(fq + c * CW, n * CW)]

    halves = (pl.ds(0, CW), pl.ds(CW, CW))

    def load_early(k, p):
        load(wd.at[pl.ds(col(side * fq), ne * CW), piece(k)], wv.at[p, ecols, halves[0]], s_wv.at[p])
        load(db.at[0, k, ecols, :], wv.at[p, ecols, halves[1]], s_wv.at[p])

    def load_pair(half, k, p):
        if half == 0:
            src = (wd.at[pl.ds(col(side * fq), fq), piece(k)], db.at[0, k])
        else:
            src = (db.at[1, k], db.at[2, k])
        for m in range(2):
            load(src[m], wv.at[p, hcols, halves[m]], s_wv.at[p])

    def wait_pair(p):
        wait(wv.at[p, hcols, :], s_wv.at[p])

    def put(b, out, u):
        for m in range(2):
            load(tile(b, m), po.at[out, u, m], s_po)
        wait(tile(b, 0, 2), s_po)

    def down(b, out, u, p):
        o = jnp.dot(xb[block(b), hcols], wv[p, hcols, :], preferred_element_type=f32)
        xb[block(b), both] = o.astype(bf16)
        put(b, out, u)

    def ship_d(u):
        for m in range(2):
            send(po.at[3, u, m], rdi.at[u, m], s_rs.at[0], s_rd.at[u], to_y)

    def ship_1(u, n):
        for m in range(2):
            send(po.at[1, u, m], r1i.at[u, m], s_rs.at[1], s_r1.at[n], to_y)

    def chunk(j, _):
        fetch_chunk(j)

        @pl.when(j == first)
        def _():
            wait(xb.at[block(3), :], s_xd)

        @pl.when(j >= first)
        def _():
            load_chunk(j - first, 1)

        wait_chunk()

        def rows_of(n, _):
            g = 3 * j + n
            gate((n + 1) % 3, j, 0, g % 2, g >= 2)
            return 0

        lax.fori_loop(0, 3, rows_of, 0)
        load_local(j + 1)

        @pl.when(j + 1 == ne)
        def _():
            for n in range(2):
                hcopy(0, 0, n).wait()
            load(hb.at[block(1), ecols], xb.at[block(0), ecols], s_ld.at[0])
            wait(db.at[0], s_d1)
            load_early(0, 2)

        @pl.when(j >= first)
        def _():
            wait(wv.at[1], s_wv.at[1])
            gate(3, j - first, 1, 2, j > first)

        return 0

    lax.fori_loop(0, ne, chunk, 0)

    wait(xb.at[block(0), ecols], s_ld.at[0])

    def early(k, _):
        p = 2 - k % 2

        @pl.when(k + 1 < ns)
        def _():
            load_early(k + 1, 3 - p)

        wait(wv.at[p, ecols, :], s_wv.at[p])
        o = jnp.dot(xb[block(0), ecols], wv[p, ecols, :], preferred_element_type=f32)
        xb[block(0), both] = o.astype(bf16)
        put(0, 1, k)
        ship_1(k, 0)
        return 0

    lax.fori_loop(0, ns, early, 0)

    done = ne - first + 2 * (nl - 2)

    def late(j, _):
        fetch_chunk(j)
        two = (j > ne) & (j < last)
        base = ne - first + 2 * (j - ne - 1)

        @pl.when(two)
        def _():
            for i in range(2):
                load_chunk(base + i, 1 + i)

        @pl.when(j == last)
        def _():
            load_chunk(done, 1)

        wait_chunk()
        hst[0] = gated(1, 0)
        load(hst.at[0], hy.at[j - ne], s_h.at[0])
        gate(2, j, 0, 1, j > ne)
        wait(hst.at[0], s_h.at[0])
        send(hy.at[j - ne], hx.at[j - ne], s_rs.at[2], s_hx, to_y)

        @pl.when(j < last)
        def _():
            load_local(j + 1)

        @pl.when(two)
        def _():
            def old(i, _):
                wait(wv.at[1 + i], s_wv.at[1 + i])
                gate(3, base + i, 1 + i, 2)
                return 0

            lax.fori_loop(0, 2, old, 0)

        return 0

    lax.fori_loop(ne, nch, late, 0)
    for j in range(nl):
        load(hy.at[j], xb.at[block(0), pl.ds((ne + j) * CW, CW)], s_ld.at[0])
    hcopy(2, last, 1).wait()
    wait(xb.at[block(2), :], s_xs.at[2])
    load_h(2, 2)
    wait(wx.at[0], s_wx.at[0])
    send(wx.at[0], wx.at[1], s_ws.at[7], s_wx.at[1], to_mate)

    def diagonal(j, _):
        i = j - done
        p = jnp.where(j == last, 0, 1 + i % 2)

        @pl.when(j + 1 < last)
        def _():
            load_chunk(j + 1, 2 - i % 2)

        @pl.when(j < last)
        def _():
            wait(wv.at[p], s_wv.at[p])

        gate(3, j, p, 2 - i % 2, i != 1)
        return 0

    lax.fori_loop(done, nch, diagonal, 0)
    load_pair(0, 0, 1)
    for q in (1, 2):
        hcopy(3, last, q).wait()
    load_h(3, 3)
    wait(xb.at[block(0), pl.ds(ne * CW, nl * CW)], s_ld.at[0])
    wait_h(2)
    wait_h(3)
    for s in range(4):
        load(x.at[:, own_cols[s]], xb.at[block(1), slot(s)], s_loc)

    def forward_strip(k):
        wait(db.at[1, k], s_d2.at[k])
        send(db.at[1, k], db.at[2, k], s_ws.at[5], s_d3.at[k], to_mate)

    def own_half(k, _):
        p = 1 + k % 2

        @pl.when(k + 1 < ns)
        def _():
            load_pair(0, k + 1, 3 - p)

        wait_pair(p)

        def rows_of(n, _):
            down(3 - n, 3 - n, k, p)

            @pl.when(n == 0)
            def _():
                ship_d(k)

            return 0

        lax.fori_loop(0, 2, rows_of, 0)

        @pl.when(k == 1)
        def _():
            forward_strip(0)

        @pl.when(k + 1 == ns)
        def _():
            forward_strip(1)

        return 0

    lax.fori_loop(0, ns, own_half, 0)

    def total(tiles):
        o = xb[block(tiles[0][0]), pl.ds(fq + tiles[0][1] * CW, CW)].astype(f32)
        for b, c in tiles[1:]:
            o = o + xb[block(b), pl.ds(fq + c * CW, CW)].astype(f32)
        return o.astype(bf16)

    def ring_at(ring, m, n=1):
        b = jnp.where(ring == 0, 0, jnp.where(ring == 3, 3, 2))
        c = jnp.where(ring == 1, 2, 4)
        return block(b), pl.ds(col(fq + (c + m) * CW), n * CW)

    def ring_tile(ring, m, n=1):
        return xb.at[ring_at(ring, m, n)]

    def relay(half, k, m, turn):
        u = half * ns + k
        load(po.at[2, u, m], tile(0, 2), s_ld.at[0])
        if m == 0:
            wait(rdi.at[u], s_rd.at[u])
        load(rdi.at[u, m], tile(0, 3), s_ld.at[1])
        ring = turn % 4

        @pl.when((turn >= 4) & (m == 0))
        def _():
            wait(ring_tile(ring, 0, 2), s_ys.at[ring])

        wait(tile(0, 2), s_ld.at[0])
        wait(tile(0, 3), s_ld.at[1])
        xb[ring_at(ring, m)] = total(((0, 2), (0, 3)))
        v = (1 - half) * ns + k
        sem = 0 if half == 0 else k + 1 if m == 0 else jnp.where(k + 1 == ns, ns + 1, k + 1)
        send(ring_tile(ring, m), yxi.at[v, m], s_ys.at[ring], s_yx.at[sem], to_x)

    def fetch_pair(k):
        @pl.when(k >= 3)
        def _():
            forward_strip(k)

        wait(db.at[2, k], s_d3.at[k])
        load_pair(1, k, 1 + k % 2)

    def other_half(k, _):
        p = 1 + k % 2
        u = ns + k
        wait_pair(p)

        def rows_of(n, _):
            b = jnp.where(n == 0, 3, jnp.where(n == 1, 0, 2))
            down(b, jnp.where(n == 1, 1, b), u, p)

            @pl.when(n == 0)
            def _():
                ship_d(u)

            @pl.when((n == 1) & (k > 0))
            def _():
                ship_1(u - 1, k)

            return 0

        lax.fori_loop(0, 3, rows_of, 0)
        for m in range(2):
            relay(0, k, m, k)

        @pl.when(k == 0)
        def _():
            forward_strip(2)

        @pl.when(k + 1 < ns)
        def _():
            fetch_pair(k + 1)

        return 0

    fetch_pair(0)
    lax.fori_loop(0, ns, other_half, 0)
    ship_1(2 * ns - 1, ns)

    load_chunk(ne, 1)
    wait(xb.at[block(1), :], s_loc)

    def own_late(j, _):
        i = j - ne
        p = jnp.where(j == last, 0, 1 + i % 2)

        @pl.when(j + 1 < last)
        def _():
            load_chunk(j + 1, 2 - i % 2)

        @pl.when(j < last)
        def _():
            wait(wv.at[p], s_wv.at[p])

        gate(1, j, p, i % 2, i > 1, 0)
        return 0

    lax.fori_loop(ne, nch, own_late, 0)

    long = pl.ds(0, fq + nl * CW)
    rest = pl.ds(fq, nl * CW)

    def load_long(k, p):
        load_pair(0, k, p)
        for m in range(2):
            load(wx.at[m, k], wv.at[p, rest, halves[m]], s_wv.at[p])

    for q in range(2):
        hcopy(0, last, q).wait()
    load_h(0, 1)
    wait(hx, s_hx)
    for j in range(nl):
        load(hx.at[j], xb.at[block(1), pl.ds(fq + j * CW, CW)], s_ld.at[3])
    wait(wx.at[1], s_wx.at[1])
    load_long(0, 1)
    wait_h(1)
    wait(xb.at[block(1), rest], s_ld.at[3])

    for m in range(2):
        relay(1, 0, m, ns)

    def own_rows(k, _):
        p = 1 + k % 2

        @pl.when(k + 1 < ns)
        def _():
            load_long(k + 1, 3 - p)

        wait(wv.at[p, long, :], s_wv.at[p])
        o = jnp.dot(xb[block(1), long], wv[p, long, :], preferred_element_type=f32)
        xb[block(0), both] = o.astype(bf16)
        put(0, 0, k)
        return 0

    lax.fori_loop(0, ns, own_rows, 0)
    load_pair(1, 0, 1)
    for m in range(2):
        relay(1, 1, m, ns + 1)

    def own_rows_too(k, _):
        p = 1 + k % 2

        @pl.when(k + 1 < ns)
        def _():
            load_pair(1, k + 1, 3 - p)

        wait_pair(p)
        down(1, 0, ns + k, p)
        return 0

    lax.fori_loop(0, ns, own_rows_too, 0)
    for m in range(2):
        relay(1, 2, m, ns + 2)

    parts = ((1, 2), (1, 3), (1, 4), (1, 5))

    def keep(half, k, m, o):
        wv[half, pl.ds(col(k * rows, rows), rows), halves[m]] = o

    def finish(half, k, m):
        u = half * ns + k
        n = 2 * half + m
        cols = pl.ds(col(quarter[n] * dk + k * CW), CW)
        load(po.at[0, u, m], tile(*parts[0]), s_ld.at[0])
        load(x.at[:, cols], tile(*parts[1]), s_ld.at[1])
        if m == 0 and half == 1:
            wait(r1i.at[u], s_r1.at[k + 1])
        load(r1i.at[u, m], tile(*parts[2]), s_ld.at[2])
        if m == 0 and half == 0:
            @pl.when(k + 1 < ns)
            def _():
                wait(yxi.at[u], s_yx.at[k + 1])

            @pl.when(k + 1 == ns)
            def _():
                wait(yxi.at[u, 0], s_yx.at[k + 1])
        load(yxi.at[u, m], tile(*parts[3]), s_ld.at[3])
        for c in range(4):
            wait(tile(*parts[c]), s_ld.at[c])
        keep(half, k, m, total(parts))

    def begin():
        load(po.at[0, ns - 1, 1], tile(*parts[0]), s_ld.at[0])
        load(r1i.at[ns - 1, 1], tile(*parts[1]), s_ld.at[1])
        wait(tile(*parts[0]), s_ld.at[0])
        wait(tile(*parts[1]), s_ld.at[1])
        keep(0, ns - 1, 1, total(parts[:2]))

    wait(r1i.at[pl.ds(0, ns)], s_r1.at[0])
    wait(yxi.at[pl.ds(ns, ns)], s_yx.at[0])

    def tail(k, _):
        @pl.when((k > 2) & (k < ns))
        def _():
            for m in range(2):
                relay(1, k, m, ns + k)

        @pl.when(k > 0)
        def _():
            finish(0, k - 1, 0)

            @pl.when(k < ns)
            def _():
                finish(0, k - 1, 1)

            @pl.when(k == ns)
            def _():
                begin()

            for m in range(2):
                finish(1, k - 1, m)

        return 0

    lax.fori_loop(0, ns + 1, tail, 0)

    for ring in range(4):
        wait(ring_tile(ring, 0, 2), s_ys.at[ring])
    wait(x, s_xs.at[0])
    wait(x, s_xs.at[1])
    wait(w1, s_ws.at[0])
    wait(w2, s_ws.at[1])
    wait(db.at[0], s_ws.at[2])
    wait(db.at[1], s_ws.at[3])
    wait(w3, s_ws.at[4])
    wait(db.at[2], s_ws.at[5])
    wait(wx.at[0], s_ws.at[6])
    wait(wx.at[1], s_ws.at[7])
    wait(rdi, s_rs.at[0])
    wait(r1i, s_rs.at[1])
    wait(hx, s_rs.at[2])
    wait(yxi.at[ns - 1, 1], s_yx.at[ns + 1])


def write(x, done, yxi, y, strip, s_in, s_out):
    rows, dim = x.shape
    dk = dim // 4
    ns = dk // CW
    d = lax.axis_index("dp")
    mate = d + 1 - 2 * (d % 2)
    quarter = [d, mate, (d + 2) % 4, (mate + 2) % 4]

    def cols(half, k, m):
        return pl.ds(pl.multiple_of(quarter[2 * half + m] * dk + k * CW, 128), CW)

    def kept(half, k, m):
        return done.at[half, pl.ds(k * rows, rows), pl.ds(m * CW, CW)]

    end = (0, ns - 1, 1)
    loads = [pltpu.make_async_copy(src, strip.at[i], s_in.at[i])
             for i, src in enumerate((x.at[:, cols(*end)], yxi.at[ns - 1, 1]))]
    for copy in loads:
        copy.start()
    strips = [(half, k, m) for k in range(ns) for half in range(2) for m in range(2)]
    strips.remove(end)
    outs = [pltpu.make_async_copy(kept(*i), y.at[:, cols(*i)], s_out) for i in strips]
    for copy in outs:
        copy.start()
    for copy in loads:
        copy.wait()
    o = kept(*end)[...].astype(jnp.float32) + strip[1].astype(jnp.float32) + strip[0].astype(jnp.float32)
    strip[2] = o.astype(strip.dtype)
    pltpu.make_async_copy(strip.at[2], y.at[:, cols(*end)], s_out).start()
    pltpu.make_async_copy(y, y, s_out).wait()


def solution(mesh):
    def body(x, wg, wu, wd):
        rows, dim = x.shape
        dk = dim // 4
        fq = wg.shape[1] // 2
        nch = fq // CW
        nl = late_chunks(nch)
        ns = dk // CW
        bf16 = jnp.bfloat16
        dma = pltpu.SemaphoreType.DMA
        pairs = (2 * ns, 2, rows, CW)
        shapes = [
            (nch, dk, 2 * CW), (nch, dk, 2 * CW), (nch, dk, 2 * CW),
            (3, ns, fq, CW),
            (4 * rows, fq),
            (4,) + pairs, pairs, pairs, pairs,
            (nl, rows, CW), (nl, rows, CW),
            (2, ns, nl * CW, CW),
        ]
        any_space = pl.BlockSpec(memory_space=pl.ANY)
        in_vmem = pl.BlockSpec(memory_space=pltpu.VMEM)
        outs = pl.pallas_call(
            kernel,
            out_shape=[pltpu.VMEM((3, dim, 2 * CW), bf16)] + [jax.ShapeDtypeStruct(s, bf16) for s in shapes],
            in_specs=[any_space] * 4,
            out_specs=[in_vmem] + [any_space] * len(shapes),
            scratch_shapes=[
                pltpu.VMEM((4 * rows, dim), bf16),
                pltpu.VMEM((3, rows, CW), bf16),
                dma, dma((3,)), dma((8,)), dma((4,)), dma, dma,
                dma, dma((nch,)), dma((nch,)), dma, dma((ns,)), dma((ns,)), dma((2,)), dma,
                dma((4,)), dma((3,)), dma, dma((3,)),
                dma((2 * ns,)), dma((ns + 1,)), dma((ns + 2,)), dma((4,)), dma((4,)),
            ],
            compiler_params=pltpu.CompilerParams(
                collective_id=0, has_side_effects=True, vmem_limit_bytes=48 * 2**20),
            cost_estimate=pl.CostEstimate(
                flops=6 * rows * 4 * dim * fq, bytes_accessed=4 * rows * dim * 2, transcendentals=0),
        )(x, wg, wu, wd)
        return pl.pallas_call(
            write,
            out_shape=jax.ShapeDtypeStruct((rows, dim), bf16),
            in_specs=[any_space, in_vmem, any_space],
            out_specs=any_space,
            scratch_shapes=[pltpu.VMEM((3, rows, CW), bf16), dma((2,)), dma],
            compiler_params=pltpu.CompilerParams(vmem_limit_bytes=48 * 2**20),
        )(x, pltpu.with_memory_space_constraint(outs[0], pltpu.VMEM), outs[9])

    return jax.shard_map(body, mesh=mesh, in_specs=(P(("dp", "tp"), None), P("dp", "tp"), P("dp", "tp"), P("tp", "dp")), out_specs=P(("dp", "tp"), None), check_vma=False)
```

```python
import jax
import jax.numpy as jnp
from jax import lax
from jax.experimental import pallas as pl
from jax.experimental.pallas import tpu as pltpu
from jax.sharding import PartitionSpec as P

CW = 256


def late_chunks(nch):
    return min(4, nch // 3)


def kernel(x, wg, wu, wd, wv, w1, w2, w3, db, hb, po, rdi, r1i, yxi, hy, hx, wx,
           xb, hst, s_loc, s_xs, s_ws, s_xx, s_xy, s_xd, s_w1, s_w2, s_w3, s_d1, s_d2, s_d3, s_wx, s_hx,
           s_wv, s_h, s_po, s_rs, s_rd, s_r1, s_yx, s_ys, s_ld):
    rows, dim = x.shape
    dk = dim // 4
    fq = wg.shape[1] // 2
    nch = fq // CW
    first = nch // 2
    nl = late_chunks(nch)
    ne = nch - nl
    last = nch - 1
    ns = dk // CW
    f32, bf16 = jnp.float32, jnp.bfloat16

    t = lax.axis_index("tp")
    d = lax.axis_index("dp")
    side = d // 2
    core = d % 2
    mate = d + 1 - 2 * core
    quarter = [d, mate, (d + 2) % 4, (mate + 2) % 4]
    to_mate = {"dp": mate}
    to_x = {"dp": (d + 2) % 4}
    to_y = {"tp": 1 - t}

    def col(v, size=128):
        return v if isinstance(v, int) else pl.multiple_of(v, size)

    def send(src, dst, send_sem, recv_sem, where):
        pltpu.make_async_remote_copy(
            src_ref=src, dst_ref=dst, send_sem=send_sem, recv_sem=recv_sem,
            device_id=where, device_id_type=pl.DeviceIdType.MESH).start()

    def load(src, dst, sem):
        pltpu.make_async_copy(src, dst, sem).start()

    def wait(ref, sem):
        pltpu.make_async_copy(ref, ref, sem).wait()

    def block(b):
        return pl.ds(col(b * rows, rows), rows)

    def slot(s):
        return pl.ds(s * dk, dk)

    def piece(k):
        return pl.ds(col(k * CW), CW)

    barrier = pltpu.get_barrier_semaphore()
    for where in (to_mate, to_x, to_y):
        pl.semaphore_signal(barrier, inc=1, device_id=where, device_id_type=pl.DeviceIdType.MESH)
    pl.semaphore_wait(barrier, 3)

    own_cols = [pl.ds(col(quarter[s] * dk), dk) for s in range(4)]
    for s in range(4):
        src = x.at[:, own_cols[s]]
        send(src, xb.at[block(2), slot(s ^ 2)], s_xs.at[0], s_xx.at[s ^ 2], to_x)
        send(src, xb.at[block(1), slot(s)], s_xs.at[1], s_xy, to_y)
    for s in range(4):
        load(x.at[:, own_cols[s]], xb.at[block(0), slot(s)], s_loc)

    def send_chunk(j, _):
        for m, w in enumerate((wg, wu)):
            away = w.at[:, pl.ds(col((1 - side) * fq + j * CW), CW)]
            here = w.at[:, pl.ds(col(side * fq + j * CW), CW)]
            send(away, w2.at[j, :, pl.ds(m * CW, CW)], s_ws.at[1], s_w2.at[j], to_x)
            send(here, w1.at[j, :, pl.ds(m * CW, CW)], s_ws.at[0], s_w1, to_mate)
        return 0

    lax.fori_loop(0, nch, send_chunk, 0)

    def send_strip(k, _):
        send(wd.at[pl.ds(col((1 - side) * fq), fq), piece(k)], db.at[1, k], s_ws.at[3], s_d2.at[k], to_x)
        send(wd.at[pl.ds(col(side * fq), fq), piece(k)], db.at[0, k], s_ws.at[2], s_d1, to_mate)
        return 0

    lax.fori_loop(0, ns, send_strip, 0)

    for s in (2, 3, 0, 1):
        part = xb.at[block(2), slot(s)]
        wait(part, s_xx.at[s])
        send(part, xb.at[block(3), slot(s)], s_xs.at[2], s_xd, to_y)

    def send_rest(k, _):
        send(wd.at[pl.ds(col(side * fq + ne * CW), nl * CW), piece(k)], wx.at[0, k], s_ws.at[6], s_wx.at[0], to_y)
        return 0

    lax.fori_loop(0, ns, send_rest, 0)

    at_hand, to_come = pl.ds(0, 2 * dk), pl.ds(2 * dk, 2 * dk)

    def load_here(j, p, sem):
        for m, w in enumerate((wg, wu)):
            here = w.at[:, pl.ds(col(side * fq + j * CW), CW)]
            load(here, wv.at[p, slot(0), pl.ds(m * CW, CW)], s_wv.at[sem])

    def load_slot(w, j, n, p, sem):
        load(w.at[j], wv.at[p, slot(n)], s_wv.at[sem])

    def load_chunk(j, p):
        load_here(j, p, p)
        for n, w in ((1, w1), (2, w2), (3, w3)):
            load_slot(w, j, n, p, p)

    def load_local(j):
        load_here(j, 0, 3)
        load_slot(w1, j, 1, 0, 3)

    def fetch_chunk(j):
        wait(w2.at[j], s_w2.at[j])
        send(w2.at[j], w3.at[j], s_ws.at[4], s_w3.at[j % 2], to_mate)
        load_slot(w2, j, 2, 0, 0)
        wait(w3.at[j], s_w3.at[j % 2])
        load_slot(w3, j, 3, 0, 0)

    def wait_chunk():
        wait(wv.at[0, at_hand, :], s_wv.at[3])
        wait(wv.at[0, to_come, :], s_wv.at[0])

    def hcopy(b, j, q):
        return pltpu.make_async_copy(hst.at[q], hb.at[block(b), piece(j)], s_h.at[q])

    def gated(b, p):
        ab = jnp.dot(xb[block(b), :], wv[p], preferred_element_type=f32)
        a = ab[:, :CW]
        return (a * jax.nn.sigmoid(a) * ab[:, CW:]).astype(bf16)

    def gate(b, j, p, q, used=True, to=None):
        to = b if to is None else to

        @pl.when(used)
        def _():
            hcopy(to, j, q).wait()

        hst[q] = gated(b, p)
        hcopy(to, j, q).start()

    wait(xb.at[block(0), :], s_loc)
    wait(xb.at[block(1), :], s_xy)
    wait(w1, s_w1)
    load_local(0)

    hcols = pl.ds(0, fq)
    ecols = pl.ds(0, ne * CW)
    both = pl.ds(fq, 2 * CW)

    def load_h(b, to):
        load(hb.at[block(b), :], xb.at[block(to), hcols], s_ld.at[to])

    def wait_h(to):
        wait(xb.at[block(to), hcols], s_ld.at[to])

    def tile(b, c, n=1):
        return xb.at[block(b), pl.ds(fq + c * CW, n * CW)]

    halves = (pl.ds(0, CW), pl.ds(CW, CW))

    def load_early(k, p):
        load(wd.at[pl.ds(col(side * fq), ne * CW), piece(k)], wv.at[p, ecols, halves[0]], s_wv.at[p])
        load(db.at[0, k, ecols, :], wv.at[p, ecols, halves[1]], s_wv.at[p])

    def load_pair(half, k, p):
        if half == 0:
            src = (wd.at[pl.ds(col(side * fq), fq), piece(k)], db.at[0, k])
        else:
            src = (db.at[1, k], db.at[2, k])
        for m in range(2):
            load(src[m], wv.at[p, hcols, halves[m]], s_wv.at[p])

    def wait_pair(p):
        wait(wv.at[p, hcols, :], s_wv.at[p])

    def put(b, out, u):
        for m in range(2):
            load(tile(b, m), po.at[out, u, m], s_po)
        wait(tile(b, 0, 2), s_po)

    def down(b, out, u, p):
        o = jnp.dot(xb[block(b), hcols], wv[p, hcols, :], preferred_element_type=f32)
        xb[block(b), both] = o.astype(bf16)
        put(b, out, u)

    def ship_d(u):
        for m in range(2):
            send(po.at[3, u, m], rdi.at[u, m], s_rs.at[0], s_rd.at[u], to_y)

    def ship_1(u, n):
        for m in range(2):
            send(po.at[1, u, m], r1i.at[u, m], s_rs.at[1], s_r1.at[n], to_y)

    def chunk(j, _):
        fetch_chunk(j)

        @pl.when(j == first)
        def _():
            wait(xb.at[block(3), :], s_xd)

        @pl.when(j >= first)
        def _():
            load_chunk(j - first, 1)

        wait_chunk()

        def rows_of(n, _):
            g = 3 * j + n
            gate((n + 1) % 3, j, 0, g % 2, g >= 2)
            return 0

        lax.fori_loop(0, 3, rows_of, 0)
        load_local(j + 1)

        @pl.when(j + 1 == ne)
        def _():
            for n in range(2):
                hcopy(0, 0, n).wait()
            load(hb.at[block(1), ecols], xb.at[block(0), ecols], s_ld.at[0])
            wait(db.at[0], s_d1)
            load_early(0, 2)

        @pl.when(j >= first)
        def _():
            wait(wv.at[1], s_wv.at[1])
            gate(3, j - first, 1, 2, j > first)

        return 0

    lax.fori_loop(0, ne, chunk, 0)

    wait(xb.at[block(0), ecols], s_ld.at[0])

    def early(k, _):
        p = 2 - k % 2

        @pl.when(k + 1 < ns)
        def _():
            load_early(k + 1, 3 - p)

        wait(wv.at[p, ecols, :], s_wv.at[p])
        o = jnp.dot(xb[block(0), ecols], wv[p, ecols, :], preferred_element_type=f32)
        xb[block(0), both] = o.astype(bf16)
        put(0, 1, k)
        ship_1(k, 0)
        return 0

    lax.fori_loop(0, ns, early, 0)

    done = ne - first + 2 * (nl - 2)

    def late(j, _):
        fetch_chunk(j)
        two = (j > ne) & (j < last)
        base = ne - first + 2 * (j - ne - 1)

        @pl.when(two)
        def _():
            for i in range(2):
                load_chunk(base + i, 1 + i)

        @pl.when(j == last)
        def _():
            load_chunk(done, 1)

        wait_chunk()
        hst[0] = gated(1, 0)
        load(hst.at[0], hy.at[j - ne], s_h.at[0])
        gate(2, j, 0, 1, j > ne)
        wait(hst.at[0], s_h.at[0])
        send(hy.at[j - ne], hx.at[j - ne], s_rs.at[2], s_hx, to_y)

        @pl.when(j < last)
        def _():
            load_local(j + 1)

        @pl.when(two)
        def _():
            def old(i, _):
                wait(wv.at[1 + i], s_wv.at[1 + i])
                gate(3, base + i, 1 + i, 2)
                return 0

            lax.fori_loop(0, 2, old, 0)

        return 0

    lax.fori_loop(ne, nch, late, 0)
    for j in range(nl):
        load(hy.at[j], xb.at[block(0), pl.ds((ne + j) * CW, CW)], s_ld.at[0])
    hcopy(2, last, 1).wait()
    wait(xb.at[block(2), :], s_xs.at[2])
    load_h(2, 2)
    wait(wx.at[0], s_wx.at[0])
    send(wx.at[0], wx.at[1], s_ws.at[7], s_wx.at[1], to_mate)

    def diagonal(j, _):
        i = j - done
        p = jnp.where(j == last, 0, 1 + i % 2)

        @pl.when(j + 1 < last)
        def _():
            load_chunk(j + 1, 2 - i % 2)

        @pl.when(j < last)
        def _():
            wait(wv.at[p], s_wv.at[p])

        gate(3, j, p, 2 - i % 2, i != 1)
        return 0

    lax.fori_loop(done, nch, diagonal, 0)
    load_pair(0, 0, 1)
    for q in (1, 2):
        hcopy(3, last, q).wait()
    load_h(3, 3)
    wait(xb.at[block(0), pl.ds(ne * CW, nl * CW)], s_ld.at[0])
    wait_h(2)
    wait_h(3)
    for s in range(4):
        load(x.at[:, own_cols[s]], xb.at[block(1), slot(s)], s_loc)

    def forward_strip(k):
        wait(db.at[1, k], s_d2.at[k])
        send(db.at[1, k], db.at[2, k], s_ws.at[5], s_d3.at[k % 3], to_mate)

    def own_half(k, _):
        p = 1 + k % 2

        @pl.when(k + 1 < ns)
        def _():
            load_pair(0, k + 1, 3 - p)

        wait_pair(p)

        def rows_of(n, _):
            down(3 - n, 3 - n, k, p)

            @pl.when(n == 0)
            def _():
                ship_d(k)

            return 0

        lax.fori_loop(0, 2, rows_of, 0)

        @pl.when(k == 1)
        def _():
            forward_strip(0)

        @pl.when(k + 1 == ns)
        def _():
            forward_strip(1)

        return 0

    lax.fori_loop(0, ns, own_half, 0)

    def total(tiles):
        o = xb[block(tiles[0][0]), pl.ds(fq + tiles[0][1] * CW, CW)].astype(f32)
        for b, c in tiles[1:]:
            o = o + xb[block(b), pl.ds(fq + c * CW, CW)].astype(f32)
        return o.astype(bf16)

    def ring_at(ring, m, n=1):
        b = jnp.where(ring == 0, 0, jnp.where(ring == 3, 3, 2))
        c = jnp.where(ring == 1, 2, 4)
        return block(b), pl.ds(col(fq + (c + m) * CW), n * CW)

    def ring_tile(ring, m, n=1):
        return xb.at[ring_at(ring, m, n)]

    def relay(half, k, m, turn):
        u = half * ns + k
        load(po.at[2, u, m], tile(0, 2), s_ld.at[0])
        if m == 0:
            wait(rdi.at[u], s_rd.at[u])
        load(rdi.at[u, m], tile(0, 3), s_ld.at[1])
        ring = turn % 4

        @pl.when((turn >= 4) & (m == 0))
        def _():
            wait(ring_tile(ring, 0, 2), s_ys.at[ring])

        wait(tile(0, 2), s_ld.at[0])
        wait(tile(0, 3), s_ld.at[1])
        xb[ring_at(ring, m)] = total(((0, 2), (0, 3)))
        v = (1 - half) * ns + k
        sem = 0 if half == 0 else k + 1 if m == 0 else jnp.where(k + 1 == ns, ns + 1, k + 1)
        send(ring_tile(ring, m), yxi.at[v, m], s_ys.at[ring], s_yx.at[sem], to_x)

    def fetch_pair(k):
        @pl.when(k >= 3)
        def _():
            forward_strip(k)

        wait(db.at[2, k], s_d3.at[k % 3])
        load_pair(1, k, 1 + k % 2)

    def other_half(k, _):
        p = 1 + k % 2
        u = ns + k
        wait_pair(p)

        def rows_of(n, _):
            b = jnp.where(n == 0, 3, jnp.where(n == 1, 0, 2))
            down(b, jnp.where(n == 1, 1, b), u, p)

            @pl.when(n == 0)
            def _():
                ship_d(u)

            @pl.when((n == 1) & (k > 0))
            def _():
                ship_1(u - 1, k)

            return 0

        lax.fori_loop(0, 3, rows_of, 0)
        for m in range(2):
            relay(0, k, m, k)

        @pl.when(k == 0)
        def _():
            forward_strip(2)

        @pl.when(k + 1 < ns)
        def _():
            fetch_pair(k + 1)

        return 0

    fetch_pair(0)
    lax.fori_loop(0, ns, other_half, 0)
    ship_1(2 * ns - 1, ns)

    load_chunk(ne, 1)
    wait(xb.at[block(1), :], s_loc)

    def own_late(j, _):
        i = j - ne
        p = jnp.where(j == last, 0, 1 + i % 2)

        @pl.when(j + 1 < last)
        def _():
            load_chunk(j + 1, 2 - i % 2)

        @pl.when(j < last)
        def _():
            wait(wv.at[p], s_wv.at[p])

        gate(1, j, p, i % 2, i > 1, 0)
        return 0

    lax.fori_loop(ne, nch, own_late, 0)

    long = pl.ds(0, fq + nl * CW)
    rest = pl.ds(fq, nl * CW)

    def load_long(k, p):
        load_pair(0, k, p)
        for m in range(2):
            load(wx.at[m, k], wv.at[p, rest, halves[m]], s_wv.at[p])

    for q in range(2):
        hcopy(0, last, q).wait()
    load_h(0, 1)
    wait(hx, s_hx)
    for j in range(nl):
        load(hx.at[j], xb.at[block(1), pl.ds(fq + j * CW, CW)], s_ld.at[3])
    wait(wx.at[1], s_wx.at[1])
    load_long(0, 1)
    wait_h(1)
    wait(xb.at[block(1), rest], s_ld.at[3])

    for m in range(2):
        relay(1, 0, m, ns)

    def own_rows(k, _):
        p = 1 + k % 2

        @pl.when(k + 1 < ns)
        def _():
            load_long(k + 1, 3 - p)

        wait(wv.at[p, long, :], s_wv.at[p])
        o = jnp.dot(xb[block(1), long], wv[p, long, :], preferred_element_type=f32)
        xb[block(0), both] = o.astype(bf16)
        put(0, 0, k)
        return 0

    lax.fori_loop(0, ns, own_rows, 0)
    load_pair(1, 0, 1)
    for m in range(2):
        relay(1, 1, m, ns + 1)

    def own_rows_too(k, _):
        p = 1 + k % 2

        @pl.when(k + 1 < ns)
        def _():
            load_pair(1, k + 1, 3 - p)

        wait_pair(p)
        down(1, 0, ns + k, p)
        return 0

    lax.fori_loop(0, ns, own_rows_too, 0)
    for m in range(2):
        relay(1, 2, m, ns + 2)

    parts = ((1, 2), (1, 3), (1, 4), (1, 5))

    def keep(half, k, m, o):
        wv[half, pl.ds(col(k * rows, rows), rows), halves[m]] = o

    def finish(half, k, m):
        u = half * ns + k
        n = 2 * half + m
        cols = pl.ds(col(quarter[n] * dk + k * CW), CW)
        load(po.at[0, u, m], tile(*parts[0]), s_ld.at[0])
        load(x.at[:, cols], tile(*parts[1]), s_ld.at[1])
        if m == 0 and half == 1:
            wait(r1i.at[u], s_r1.at[k + 1])
        load(r1i.at[u, m], tile(*parts[2]), s_ld.at[2])
        if m == 0 and half == 0:
            @pl.when(k + 1 < ns)
            def _():
                wait(yxi.at[u], s_yx.at[k + 1])

            @pl.when(k + 1 == ns)
            def _():
                wait(yxi.at[u, 0], s_yx.at[k + 1])
        load(yxi.at[u, m], tile(*parts[3]), s_ld.at[3])
        for c in range(4):
            wait(tile(*parts[c]), s_ld.at[c])
        keep(half, k, m, total(parts))

    def begin():
        spare_x = wv.at[2, pl.ds(0, rows), halves[0]]
        load(x.at[:, pl.ds(col(quarter[1] * dk + (ns - 1) * CW), CW)], spare_x, s_ld.at[2])
        load(po.at[0, ns - 1, 1], tile(*parts[0]), s_ld.at[0])
        load(r1i.at[ns - 1, 1], tile(*parts[1]), s_ld.at[1])
        wait(tile(*parts[0]), s_ld.at[0])
        wait(tile(*parts[1]), s_ld.at[1])
        keep(0, ns - 1, 1, total(parts[:2]))
        wait(spare_x, s_ld.at[2])

    wait(r1i.at[pl.ds(0, ns)], s_r1.at[0])
    wait(yxi.at[pl.ds(ns, ns)], s_yx.at[0])

    def tail(k, _):
        @pl.when((k > 2) & (k < ns))
        def _():
            for m in range(2):
                relay(1, k, m, ns + k)

        @pl.when(k > 0)
        def _():
            finish(0, k - 1, 0)

            @pl.when(k < ns)
            def _():
                finish(0, k - 1, 1)

            @pl.when(k == ns)
            def _():
                begin()

            for m in range(2):
                finish(1, k - 1, m)

        return 0

    lax.fori_loop(0, ns + 1, tail, 0)

    for ring in range(4):
        wait(ring_tile(ring, 0, 2), s_ys.at[ring])
    wait(x, s_xs.at[0])
    wait(x, s_xs.at[1])
    wait(w1, s_ws.at[0])
    wait(w2, s_ws.at[1])
    wait(db.at[0], s_ws.at[2])
    wait(db.at[1], s_ws.at[3])
    wait(w3, s_ws.at[4])
    wait(db.at[2], s_ws.at[5])
    wait(wx.at[0], s_ws.at[6])
    wait(wx.at[1], s_ws.at[7])
    wait(rdi, s_rs.at[0])
    wait(r1i, s_rs.at[1])
    wait(hx, s_rs.at[2])
    wait(yxi.at[ns - 1, 1], s_yx.at[ns + 1])


def write(done, yxi, y, strip, s_in, s_out):
    rows, dim = y.shape
    dk = dim // 4
    ns = dk // CW
    d = lax.axis_index("dp")
    mate = d + 1 - 2 * (d % 2)
    quarter = [d, mate, (d + 2) % 4, (mate + 2) % 4]

    def cols(half, k, m):
        return pl.ds(pl.multiple_of(quarter[2 * half + m] * dk + k * CW, 128), CW)

    def kept(half, k, m):
        return done.at[half, pl.ds(k * rows, rows), pl.ds(m * CW, CW)]

    end = (0, ns - 1, 1)
    late = pltpu.make_async_copy(yxi.at[ns - 1, 1], strip.at[0], s_in)
    late.start()
    strips = [(half, k, m) for k in range(ns) for half in range(2) for m in range(2)]
    strips.remove(end)
    outs = [pltpu.make_async_copy(kept(*i), y.at[:, cols(*i)], s_out) for i in strips]
    for copy in outs:
        copy.start()
    late.wait()
    o = kept(*end)[...].astype(jnp.float32) + strip[0].astype(jnp.float32)
    o = o + done[2, pl.ds(0, rows), pl.ds(0, CW)].astype(jnp.float32)
    strip[1] = o.astype(strip.dtype)
    pltpu.make_async_copy(strip.at[1], y.at[:, cols(*end)], s_out).start()
    pltpu.make_async_copy(y, y, s_out).wait()


def solution(mesh):
    def body(x, wg, wu, wd):
        rows, dim = x.shape
        dk = dim // 4
        fq = wg.shape[1] // 2
        nch = fq // CW
        nl = late_chunks(nch)
        ns = dk // CW
        bf16 = jnp.bfloat16
        dma = pltpu.SemaphoreType.DMA
        pairs = (2 * ns, 2, rows, CW)
        shapes = [
            (nch, dk, 2 * CW), (nch, dk, 2 * CW), (nch, dk, 2 * CW),
            (3, ns, fq, CW),
            (4 * rows, fq),
            (4,) + pairs, pairs, pairs, pairs,
            (nl, rows, CW), (nl, rows, CW),
            (2, ns, nl * CW, CW),
        ]
        any_space = pl.BlockSpec(memory_space=pl.ANY)
        in_vmem = pl.BlockSpec(memory_space=pltpu.VMEM)
        outs = pl.pallas_call(
            kernel,
            out_shape=[pltpu.VMEM((3, dim, 2 * CW), bf16)] + [jax.ShapeDtypeStruct(s, bf16) for s in shapes],
            in_specs=[any_space] * 4,
            out_specs=[in_vmem] + [any_space] * len(shapes),
            scratch_shapes=[
                pltpu.VMEM((4 * rows, dim), bf16),
                pltpu.VMEM((3, rows, CW), bf16),
                dma, dma((3,)), dma((8,)), dma((4,)), dma, dma,
                dma, dma((nch,)), dma((2,)), dma, dma((ns,)), dma((3,)), dma((2,)), dma,
                dma((4,)), dma((3,)), dma, dma((3,)),
                dma((2 * ns,)), dma((ns + 1,)), dma((ns + 2,)), dma((4,)), dma((4,)),
            ],
            compiler_params=pltpu.CompilerParams(
                collective_id=0, has_side_effects=True, vmem_limit_bytes=48 * 2**20),
            cost_estimate=pl.CostEstimate(
                flops=6 * rows * 4 * dim * fq, bytes_accessed=4 * rows * dim * 2, transcendentals=0),
        )(x, wg, wu, wd)
        return pl.pallas_call(
            write,
            out_shape=jax.ShapeDtypeStruct((rows, dim), bf16),
            in_specs=[in_vmem, any_space],
            out_specs=any_space,
            scratch_shapes=[pltpu.VMEM((2, rows, CW), bf16), dma, dma],
            compiler_params=pltpu.CompilerParams(vmem_limit_bytes=48 * 2**20),
        )(pltpu.with_memory_space_constraint(outs[0], pltpu.VMEM), outs[9])

    return jax.shard_map(body, mesh=mesh, in_specs=(P(("dp", "tp"), None), P("dp", "tp"), P("dp", "tp"), P("tp", "dp")), out_specs=P(("dp", "tp"), None), check_vma=False)
```
